128 devices in a mesh: gx: 16 (over y, x), gy: 4 (over z), gz: 2 (over core).
Axes of the slice: x: 4, y: 4, z: 4, core: 2. Of those that a mesh axis runs over, the one named last changes fastest.
Arguments:
- load: float32 [1024, 256, 256], P('gx', 'gy', 'gz'), may hold values from -12 to 12
- stiffness: float32 [1024, 256, 256], P('gx', 'gy', 'gz'), may hold values from 0.02 to 2
- prestress: float32 [1024, 256], P(('gx', 'gy'), 'gz'), may hold values from -3 to 3
- state_var: float32 [1024, 256], P(('gx', 'gy'), 'gz'), may hold values from -1 to 1
- normal_a: float32 [1024, 256], P(('gx', 'gy'), 'gz'), may hold values from 1 to 3
Outputs:
- displacement: float32 [1024, 256, 256], P('gx', 'gy', 'gz')
- slip_rate: float32 [1024, 256], P(('gx', 'gy'), 'gz')
The draws below stay inside these ranges and needn't reach their ends.
All inputs are finite; a program needn't handle non-finite values.
Results may differ from the reference program's by a relative error of at most 0.0003.
Values sent between devices are 32-bit elements; how exact they have to be, the bound alone decides.
A program may use at most 128 MiB of HBM per device.

```python
import math
import jax
import jax.numpy as jnp

ITERS = 3
NX = 1024
NY = 256
NZ = 256


def draw_load(key, part):
    subkeys = jax.random.split(key, 4)
    along_x = ((jnp.arange(NX, dtype=jnp.float32) + 0.5) / NX)[:, None, None]
    along_y = ((jnp.arange(NY, dtype=jnp.float32) + 0.5) / NY)[None, :, None]
    along_z = ((jnp.arange(NZ, dtype=jnp.float32) + 0.5) / NZ)[None, None, :]
    waves_x = jax.random.randint(subkeys[0], (4,), 1, 4).astype(jnp.float32)
    waves_z = jax.random.randint(subkeys[1], (4,), 0, 2).astype(jnp.float32)
    phases = jax.random.uniform(subkeys[2], (7,), jnp.float32, 0.0, 2.0 * math.pi)
    smooth = jnp.zeros((NX, NY, NZ), jnp.float32)
    for mode_num in range(4):
        smooth = smooth + jnp.cos(2.0 * math.pi * (waves_x[mode_num] * along_x + along_y + waves_z[mode_num] * along_z) + phases[mode_num])
    smooth = smooth * 0.7071
    exponent = 0.5 + 0.25 * jnp.sin(2.0 * math.pi * along_x + phases[4]) + 0.25 * jnp.sin(2.0 * math.pi * along_y + phases[5])
    rough_scale = 0.3 * jnp.exp(exponent * math.log(5.0))
    smooth_scale = 0.4 + 0.4 * (1.0 + jnp.cos(2.0 * math.pi * along_z + phases[6]))
    white_noise = jax.random.truncated_normal(subkeys[3], -4.0, 4.0, (NX, NY, NZ), jnp.float32)
    return (smooth_scale * smooth + rough_scale * white_noise).astype(jnp.float32)


def level_of(rng, shape, cuts, smallest, top_value):
    factor_of = 1.0
    for dim, blocks in cuts:
        steps = jax.random.uniform(jax.random.fold_in(jax.random.fold_in(rng, 6), dim), (blocks,), jnp.float32, smallest / len(cuts), top_value / len(cuts))
        factor_of = factor_of * jnp.repeat(jnp.exp(steps), shape[dim] // blocks).reshape((-1,) + (1,) * (len(shape) - 1 - dim))
    return factor_of


def bell_draw(key, shape, spread, limit, cuts=(), kind=jnp.bfloat16):
    result = spread * jax.random.normal(key, shape, jnp.float32)
    if cuts:
        result = result * level_of(key, shape, cuts, -0.22, 0.18)
    return jnp.clip(result, -limit, limit).astype(kind)


def setup_inputs(seed: int = 0) -> dict:
    key_list = jax.random.split(jax.random.key(seed), 6)
    return {
        "load": draw_load(jax.random.fold_in(key_list[5], 71), 0),
        "stiffness": jnp.clip(jnp.exp(math.log(2.0) - 4.6051702 * jax.random.uniform(key_list[1], (NX, NY, NZ), jnp.float32) ** level_of(key_list[1], (NX, NY, NZ), ((0, 16), (1, 4), (2, 2)), -0.2, 0.2)), 0.02, 2.0),
        "prestress": bell_draw(key_list[2], (NX, NZ), 1.0, 3.0, ((0, 64), (1, 2)), jnp.float32),
        "state_var": jnp.clip(jax.random.uniform(key_list[3], (NX, NZ), jnp.float32, -1.0, 1.0) * level_of(key_list[3], (NX, NZ), ((0, 64), (1, 2)), -0.4, 0.0), -1.0, 1.0),
        "normal_a": jnp.clip(jnp.exp(math.log(3.0) - 1.0986123 * jax.random.uniform(key_list[4], (NX, NZ), jnp.float32) ** level_of(key_list[4], (NX, NZ), ((0, 64), (1, 2)), -0.2, 0.2)), 1.0, 3.0),
    }


def shifted(padded, sizes_now, axis_num, offset):
    slicers = [slice(2, 2 + sizes_now[0]), slice(2, 2 + sizes_now[1]), slice(2, 2 + sizes_now[2])]
    slicers[axis_num] = slice(2 + offset, 2 + offset + sizes_now[axis_num])
    return padded[tuple(slicers)]


def operate(field, stiffness):
    padded = jnp.pad(field, 2)
    sizes_now = field.shape
    near_sum = jnp.zeros_like(field)
    for axis_num in range(3):
        near_sum = near_sum + 16.0 * (shifted(padded, sizes_now, axis_num, 1) + shifted(padded, sizes_now, axis_num, -1))
        near_sum = near_sum - (shifted(padded, sizes_now, axis_num, 2) + shifted(padded, sizes_now, axis_num, -2))
    return (7.5 + stiffness) * field - near_sum / 12.0


def reference(load, stiffness, prestress, state_var, normal_a):
    inverse = 1.0 / (7.5 + stiffness)
    solution = jnp.zeros_like(load)
    residual = load
    precond = inverse * residual
    direction = precond
    gamma = jnp.sum(residual * precond)
    for iteration in range(ITERS):
        image = operate(direction, stiffness)
        alpha = gamma / jnp.sum(direction * image)
        solution = solution + alpha * direction
        residual = residual - alpha * image
        if iteration + 1 < ITERS:
            precond = inverse * residual
            gamma_new = jnp.sum(residual * precond)
            direction = precond + (gamma_new / gamma) * direction
            gamma = gamma_new
    half = NY // 2
    traction = (solution[:, half - 2, :] - 27.0 * solution[:, half - 1, :]
                + 27.0 * solution[:, half, :] - solution[:, half + 1, :]) / 24.0
    slip_rate = jnp.exp(-state_var) * jnp.sinh((prestress + 2.0 * traction) / normal_a)
    return solution, slip_rate
```

```python
import functools

import jax
import jax.numpy as jnp
from jax import lax
from jax.experimental import pallas as pl
from jax.experimental.pallas import tpu as pltpu
from jax.sharding import PartitionSpec as P

MESH = pl.DeviceIdType.MESH
F32 = jnp.float32
BX, BY, BZ = 64, 64, 128
LOW = 8
PITCH = BY + LOW
ROWS = (BX + 4) * PITCH + LOW
FACE = PITCH + BY
TILES = BY // 8
STRIPS = BX // 8
CHUNKS = 8


def two_sum(a, b):
    s = a + b
    t = s - a
    return s, (a - (s - t)) + (b - t)


def split(a):
    t = a * 4097.0
    high = t - (t - a)
    return high, a - high


def two_prod(a, b):
    p = a * b
    ah, al = split(a)
    bh, bl = split(b)
    return p, ((ah * bh - p) + ah * bl + al * bh) + al * bl


def norm(h, l):
    s = h + l
    return s, l - (s - h)


def dd_sub(a, b):
    s, e = two_sum(a[0], -b[0])
    return norm(s, e + (a[1] - b[1]))


def dd_mul(a, b):
    p, e = two_prod(a[0], b[0])
    return norm(p, e + (a[0] * b[1] + a[1] * b[0]))


def dd_div(a, b):
    q = a[0] / b[0]
    p, e = two_prod(q, b[0])
    r = ((a[0] - p) - e) + (a[1] - q * b[1])
    return norm(q, r / b[0])


def lane_sum(v):
    total = jnp.sum(v, axis=1, keepdims=True)
    big = total * 4096.0
    high = (v + big) - big
    low = v - high
    return norm(jnp.sum(high, axis=1, keepdims=True), jnp.sum(low, axis=1, keepdims=True))


def coefficients(mu):
    theta = dd_div(mu[1], mu[0])
    s = [None] + [dd_sub(mu[j + 1], dd_mul(theta, mu[j])) for j in range(1, 5)]
    a1 = dd_sub(dd_div(s[2], s[1]), theta)
    b1 = dd_div(s[1], mu[0])

    def second(j):
        return dd_sub(dd_sub(s[j + 1], dd_mul(a1, s[j])), dd_mul(b1, mu[j]))

    t2, t3 = second(2), second(3)
    a2 = dd_sub(dd_sub(dd_div(t3, t2), a1), theta)
    b2 = dd_div(t2, s[1])
    a0, a1, a2, b1, b2 = theta[0], a1[0], a2[0], b1[0], b2[0]
    d0 = a0
    d1 = a1 - b1 / d0
    d2 = a2 - b2 / d1
    y2 = 1.0 / (d0 * d1 * d2)
    y1 = (-1.0 / d0 - b2 * y2) / d1
    y0 = (1.0 - b1 * y1) / d0
    c2 = y2
    c1 = y1 - (a0 + a1) * y2
    c0 = y0 - a0 * y1 + (a0 * a1 - b1) * y2
    return c0, c1, c2


def spot_of(x, y=0):
    return pl.multiple_of((x + 2) * PITCH + LOW, 8) + y


def zero_edges(w):
    z8 = jnp.zeros((8, BZ), F32)
    for t in range(2 * PITCH // 8):
        w[pl.ds(8 * t, 8), :] = z8
        w[pl.ds(ROWS - LOW - 2 * PITCH + LOW + 8 * t, 8), :] = z8

    def body(x, carry):
        w[pl.ds(pl.multiple_of((x + 2) * PITCH, 8), 8), :] = z8
        return carry

    lax.fori_loop(0, BX + 1, body, 0, unroll=5)


def krylov(
    load, stiff, w0, w1, w2, coef, fault_sum,
    bv, sv, minv, ypack, zpack, trac,
    hx, hy, hz, fault, part_a, part_b,
    in_sem, xs_sem, xr_sem, ys_sem, yr_sem, zs_sem, zr_sem, fs_sem, fr_sem, rs_sem, rr_sem,
):
    gx, gy, gz = (lax.axis_index(a) for a in ("gx", "gy", "gz"))
    nx, ny, nz = (lax.axis_size(a) for a in ("gx", "gy", "gz"))
    group = ny * nz
    spot = gy * nz + gz
    lane = lax.broadcasted_iota(jnp.int32, (8, BZ), 1)
    row = lax.broadcasted_iota(jnp.int32, (8, BZ), 0)
    out_base = jnp.where(gz == 0, BZ - 2, 0)
    in_base = jnp.where(gz == 0, 0, BZ - 2)
    out_lane = lane - out_base
    in_mask = ((lane - in_base) & (BZ - 1)) < 2

    step = BX // CHUNKS
    loads = []
    for i in range(CHUNKS):
        part = pl.ds(i * step, step)
        a = pltpu.make_async_copy(load.at[part], bv.at[part], in_sem.at[0, i])
        b = pltpu.make_async_copy(stiff.at[part], sv.at[part], in_sem.at[1, i])
        a.start()
        b.start()
        loads.append((a, b))

    barrier = pltpu.get_barrier_semaphore()
    peers = []
    for r in range(1, group):
        other = lax.rem(spot + r, group)
        peers.append((gx, other // nz, lax.rem(other, nz)))
    cross = [(lax.rem(gx + r, nx), gy, gz) for r in range(1, nx)]
    for peer in peers + cross:
        pl.semaphore_signal(barrier, inc=1, device_id=peer, device_id_type=MESH)

    for w in (w0, w1, w2):
        zero_edges(w)

    zero = jnp.zeros((8, BZ), F32)
    mu0 = zero
    for i in range(CHUNKS):
        loads[i][0].wait()
        loads[i][1].wait()

        def start_plane(x, acc):
            for t in range(TILES):
                at = pl.ds(8 * t, 8)
                b = bv[x, at, :]
                inverse = 1.0 / (7.5 + sv[x, at, :])
                w = b * inverse
                w0[pl.ds(spot_of(x, 8 * t), 8), :] = w
                minv[pl.ds(pl.multiple_of(x * BY, 8) + 8 * t, 8), :] = inverse * (1.0 / 12.0)
                acc = acc + b * w
            return acc

        mu0 = mu0 + lax.fori_loop(i * step, (i + 1) * step, start_plane, zero)

    pl.semaphore_wait(barrier, len(peers) + len(cross))

    def remote(src, dst, send, recv, device):
        return pltpu.make_async_remote_copy(
            src_ref=src, dst_ref=dst, send_sem=send, recv_sem=recv,
            device_id=device, device_id_type=MESH,
        )

    def x_copy(w, k, side):
        plane = 0 if side == 0 else BX - 2
        return remote(
            w.at[pl.ds(spot_of(plane), FACE), :], hx.at[k, 1 - side],
            xs_sem.at[k, side], xr_sem.at[k, 1 - side],
            (gx - 1 if side == 0 else gx + 1, gy, gz),
        )

    def y_copy(k, side):
        return remote(
            ypack.at[k, side], hy.at[k, 1 - side],
            ys_sem.at[k, side], yr_sem.at[k, 1 - side],
            (gx, gy - 1 if side == 0 else gy + 1, gz),
        )

    def z_copy(k):
        return remote(zpack.at[k], hz.at[k], zs_sem.at[k], zr_sem.at[k], (gx, gy, 1 - gz))

    has_x = (gx > 0, gx < nx - 1)
    has_y = (gy > 0, gy < ny - 1)
    near_fault = (gy == ny // 2 - 1) | (gy == ny // 2)
    source = gy - (ny // 2 - 1)
    low_side = jnp.where(gy == ny // 2, 1.0, 0.0)
    high_side = jnp.where(gy == ny // 2 - 1, 1.0, 0.0)
    own_rows = BX // ny

    def fault_copy(k, r):
        owner = lax.rem(gy + r, ny)
        return remote(
            trac.at[k, pl.ds(owner * own_rows, own_rows), :], fault.at[source, k],
            fs_sem.at[k, r - 1], fr_sem.at[source, k], (gx, owner, gz),
        )

    def exchange(w, k):
        for j in range(STRIPS):
            strip = []
            for n, y in enumerate((0, 1, BY - 2, BY - 1)):
                v = w[pl.ds(spot_of(8 * j, y), 8, stride=PITCH), :]
                ypack[k, n // 2, n % 2, pl.ds(8 * j, 8), :] = v
                strip.append(v)
            term = low_side * (27.0 * strip[0] - strip[1]) + high_side * (strip[2] - 27.0 * strip[3])
            trac[k, pl.ds(8 * j, 8), :] = term / 24.0
        for side in range(2):
            @pl.when(has_x[side])
            def _(side=side):
                x_copy(w, k, side).start()
        for side in range(2):
            @pl.when(has_y[side])
            def _(side=side):
                y_copy(k, side).start()

        def pack(x, acc):
            mask = ((out_lane - 2 * x) & (BZ - 1)) < 2
            return tuple(
                jnp.where(mask, pltpu.roll(w[pl.ds(spot_of(x, 8 * t), 8), :], 2 * x, 1), acc[t])
                for t in range(TILES)
            )

        packed = lax.fori_loop(0, BX, pack, (zero,) * TILES)
        for t in range(TILES):
            zpack[k, t] = packed[t]

        @pl.when(near_fault)
        def _():
            for r in range(1, ny):
                fault_copy(k, r).start()
            for i in range(own_rows // 8):
                fault[source, k, pl.ds(8 * i, 8), :] = trac[
                    k, pl.ds(pl.multiple_of(gy * own_rows + 8 * i, 8), 8), :
                ]

        z_copy(k).start()

    def bulk(w, out, k, init):
        z_copy(k).wait_recv()

        def plane(x, acc):
            for t in range(TILES):
                def at(dx, dy):
                    return w[pl.ds(spot_of(x, 8 * t) + (dx * PITCH + dy), 8), :]

                c = at(0, 0)
                h = pltpu.roll(hz[k, t], lax.rem(BZ - 2 * x, BZ), 1)
                h = jnp.where(in_mask, h, 0.0)
                r1 = pltpu.roll(jnp.where(lane == 0, h, c), BZ - 1, 1)
                r2 = pltpu.roll(jnp.where(lane < 2, h, c), BZ - 2, 1)
                l1 = pltpu.roll(jnp.where(lane == BZ - 1, h, c), 1, 1)
                l2 = pltpu.roll(jnp.where(lane >= BZ - 2, h, c), 2, 1)
                near = (at(1, 0) + at(-1, 0)) + (r1 + l1) + (at(0, 1) + at(0, -1))
                far = (at(2, 0) + at(-2, 0)) + (r2 + l2) + (at(0, 2) + at(0, -2))
                n = 16.0 * near - far
                acc = out(x, t, c, n, acc)
            return acc

        return lax.fori_loop(0, BX, plane, init)

    def fixes(k, apply_x, apply_y):
        for side in range(2):
            @pl.when(has_x[side])
            def _(side=side):
                x_copy(w0, k, 1 - side).wait_recv()
                inner, outer = (1, 0) if side == 0 else (0, 1)
                first, second = (0, 1) if side == 0 else (BX - 1, BX - 2)
                for t in range(TILES):
                    close = hx[k, side, pl.ds(inner * PITCH + 8 * t, 8), :]
                    distant = hx[k, side, pl.ds(outer * PITCH + 8 * t, 8), :]
                    apply_x(first, t, 16.0 * close - distant)
                    apply_x(second, t, -close)
        for side in range(2):
            @pl.when(has_y[side])
            def _(side=side):
                y_copy(k, 1 - side).wait_recv()
                inner, outer = (1, 0) if side == 0 else (0, 1)
                first, second = (0, 1) if side == 0 else (BY - 1, BY - 2)
                for j in range(STRIPS):
                    at = pl.ds(8 * j, 8)
                    close = hy[k, side, inner, at, :]
                    apply_y(j, first, 16.0 * close - hy[k, side, outer, at, :])
                    apply_y(j, second, -close)

    def basis_step(w, new, k, moments, init):
        exchange(w, k)

        def out(x, t, c, n, acc):
            new[pl.ds(spot_of(x, 8 * t), 8), :] = (
                c - minv[pl.ds(pl.multiple_of(x * BY, 8) + 8 * t, 8), :] * n
            )
            return moments(x, t, c, acc)

        sums = bulk(w, out, k, init)

        def apply_x(x, t, n):
            at = pl.ds(spot_of(x, 8 * t), 8)
            new[at, :] = new[at, :] - minv[pl.ds(x * BY + 8 * t, 8), :] * n

        def apply_y(j, y, n):
            at = pl.ds(spot_of(8 * j, y), 8, stride=PITCH)
            new[at, :] = new[at, :] - minv[pl.ds(8 * j * BY + y, 8, stride=BY), :] * n

        fixes(k, apply_x, apply_y)
        return sums

    basis_step(w0, w1, 0, lambda x, t, c, acc: acc, 0)

    def first_moments(x, t, c, acc):
        at = pl.ds(8 * t, 8)
        return (acc[0] + bv[x, at, :] * c, acc[1] + ((7.5 + sv[x, at, :]) * c) * c)

    mu1, mu2 = basis_step(w1, w2, 1, first_moments, (zero, zero))

    exchange(w2, 2)

    def last(x, t, c, n, acc):
        d = (7.5 + sv[x, pl.ds(8 * t, 8), :]) * c
        return (
            acc[0] + d * w1[pl.ds(spot_of(x, 8 * t), 8), :],
            acc[1] + d * c,
            acc[2] + c * (d - n * (1.0 / 12.0)),
        )

    mu3, mu4, mu5 = bulk(w2, last, 2, (zero, zero, zero))
    part_a[0] = zero

    def cross_x(x, t, n):
        part_a[0] = part_a[0] + w2[pl.ds(spot_of(x, 8 * t), 8), :] * n

    def cross_y(j, y, n):
        part_a[0] = part_a[0] + w2[pl.ds(spot_of(8 * j, y), 8, stride=PITCH), :] * n

    fixes(2, cross_x, cross_y)
    mu5 = mu5 - part_a[0] * (1.0 / 12.0)

    local = zero
    for j, m in enumerate((mu0, mu1, mu2, mu3, mu4, mu5)):
        local = jnp.where(row == j, jnp.sum(m, axis=0, keepdims=True), local)

    def reduce(value, buf, s, devices):
        buf[0] = value
        copies = [
            remote(buf.at[0], buf.at[r + 1], rs_sem.at[s, r], rr_sem.at[s, r], device)
            for r, device in enumerate(devices)
        ]
        for c in copies:
            c.start()
        for c in copies:
            c.wait_recv()
        total = value
        for r in range(len(devices)):
            total = total + buf[r + 1]
        return total, copies

    total, sent_a = reduce(local, part_a, 0, peers)
    total, sent_b = reduce(total, part_b, 1, cross)

    mu = []
    for j in range(6):
        mu.append(lane_sum(jnp.broadcast_to(total[j : j + 1, :], (8, BZ))))
    for j, c in enumerate(coefficients(mu)):
        coef[j] = jnp.broadcast_to(c, (8, BZ))

    for k in range(3):
        for s in range(2):
            @pl.when(gy != ny // 2 - 1 + s)
            def _(k=k, s=s):
                remote(
                    trac.at[k, pl.ds(0, own_rows), :], fault.at[s, k],
                    fs_sem.at[k, 0], fr_sem.at[s, k], (gx, gy, 1 - gz),
                ).wait_recv()
    for k in range(3):
        for i in range(own_rows // 8):
            at = pl.ds(8 * i, 8)
            fault_sum[k, at, :] = fault[0, k, at, :] + fault[1, k, at, :]

    for c in sent_a + sent_b:
        c.wait_send()
    for k in range(3):
        for side in range(2):
            @pl.when(has_x[side])
            def _(k=k, side=side):
                x_copy(w0, k, side).wait_send()
            @pl.when(has_y[side])
            def _(k=k, side=side):
                y_copy(k, side).wait_send()
        z_copy(k).wait_send()

        @pl.when(near_fault)
        def _(k=k):
            for r in range(1, ny):
                fault_copy(k, r).wait_send()


def combine(w0, w1, w2, coef, fault_sum, prestress, state, normal, u, slip, buf, sem):
    c0, c1, c2 = coef[0], coef[1], coef[2]
    step = BX // CHUNKS
    copies = []
    for i in range(CHUNKS):
        def plane(x, carry):
            for t in range(TILES):
                at = pl.ds(spot_of(x, 8 * t), 8)
                buf[x, pl.ds(8 * t, 8), :] = (c0 * w0[at, :] + c1 * w1[at, :]) + c2 * w2[at, :]
            return carry

        lax.fori_loop(i * step, (i + 1) * step, plane, 0)
        part = pl.ds(i * step, step)
        copy = pltpu.make_async_copy(buf.at[part], u.at[part], sem.at[i])
        copy.start()
        copies.append(copy)
    for i in range(slip.shape[0] // 8):
        at = pl.ds(8 * i, 8)
        traction = (c0 * fault_sum[0, at, :] + c1 * fault_sum[1, at, :]) + c2 * fault_sum[2, at, :]
        x = (prestress[at, :] + 2.0 * traction) / normal[at, :]
        half = 0.6931471805599453
        large = jnp.exp(x - half) - jnp.exp(-x - half)
        q = x * x
        small = x * (1.0 + q * (1 / 6 + q * (1 / 120 + q * (1 / 5040 + q * (1 / 362880 + q / 39916800)))))
        sinh = jnp.where(jnp.abs(x) < 1.0, small, large)
        slip[at, :] = jnp.exp(-state[at, :]) * sinh
    for copy in copies:
        copy.wait()


def per_device(load, stiffness, prestress, state_var, normal_a):
    vmem = pl.BlockSpec(memory_space=pltpu.VMEM)
    hbm = pl.BlockSpec(memory_space=pl.ANY)
    ny = lax.axis_size("gy")
    own = BX // ny
    group = ny * lax.axis_size("gz")
    nx = lax.axis_size("gx")
    big = (ROWS, BZ)
    DMA = pltpu.SemaphoreType.DMA
    outs = pl.pallas_call(
        krylov,
        out_shape=[
            pltpu.VMEM(big, F32), pltpu.VMEM(big, F32), pltpu.VMEM(big, F32),
            pltpu.VMEM((3, 8, BZ), F32), pltpu.VMEM((3, own, BZ), F32),
        ],
        in_specs=[pl.BlockSpec(memory_space=pltpu.HBM)] * 2,
        out_specs=[vmem] * 5,
        scratch_shapes=[
            pltpu.VMEM((BX, BY, BZ), F32),
            pltpu.VMEM((BX, BY, BZ), F32),
            pltpu.VMEM((BX * BY, BZ), F32),
            pltpu.VMEM((3, 2, 2, BX, BZ), F32),
            pltpu.VMEM((3, TILES, 8, BZ), F32),
            pltpu.VMEM((3, BX, BZ), F32),
            pltpu.VMEM((3, 2, FACE, BZ), F32),
            pltpu.VMEM((3, 2, 2, BX, BZ), F32),
            pltpu.VMEM((3, TILES, 8, BZ), F32),
            pltpu.VMEM((2, 3, own, BZ), F32),
            pltpu.VMEM((group, 8, BZ), F32),
            pltpu.VMEM((nx, 8, BZ), F32),
            DMA((2, CHUNKS)),
            DMA((3, 2)), DMA((3, 2)), DMA((3, 2)), DMA((3, 2)), DMA((3,)), DMA((3,)),
            DMA((3, ny - 1)), DMA((2, 3)),
            DMA((2, nx - 1)), DMA((2, nx - 1)),
        ],
        compiler_params=pltpu.CompilerParams(
            collective_id=0, has_side_effects=True, vmem_limit_bytes=40 * 2**20
        ),
        name="krylov",
    )(load, stiffness)
    return pl.pallas_call(
        combine,
        out_shape=[
            jax.ShapeDtypeStruct(load.shape, F32),
            jax.ShapeDtypeStruct(prestress.shape, F32),
        ],
        in_specs=[vmem] * 8,
        out_specs=[hbm, vmem],
        scratch_shapes=[pltpu.VMEM((BX, BY, BZ), F32), DMA((CHUNKS,))],
        compiler_params=pltpu.CompilerParams(vmem_limit_bytes=24 * 2**20),
        name="combine",
    )(*outs, prestress, state_var, normal_a)


def solution(mesh):
    block = P("gx", "gy", "gz")
    fault = P(("gx", "gy"), "gz")
    return jax.shard_map(
        per_device,
        mesh=mesh,
        in_specs=(block, block, fault, fault, fault),
        out_specs=(block, fault),
        check_vma=False,
    )
```

```python
import functools

import jax
import jax.numpy as jnp
from jax import lax
from jax.experimental import pallas as pl
from jax.experimental.pallas import tpu as pltpu
from jax.sharding import PartitionSpec as P

MESH = pl.DeviceIdType.MESH
F32 = jnp.float32
BX, BY, BZ = 64, 64, 128
LOW = 8
PITCH = BY + LOW
ROWS = (BX + 4) * PITCH + LOW
FACE = PITCH + BY
TILES = BY // 8
STRIPS = BX // 8
CHUNKS = 8
SLOTS = 32
UNROLL = 8


def two_sum(a, b):
    s = a + b
    t = s - a
    return s, (a - (s - t)) + (b - t)


def split(a):
    t = a * 4097.0
    high = t - (t - a)
    return high, a - high


def two_prod(a, b):
    p = a * b
    ah, al = split(a)
    bh, bl = split(b)
    return p, ((ah * bh - p) + ah * bl + al * bh) + al * bl


def norm(h, l):
    s = h + l
    return s, l - (s - h)


def dd_sub(a, b):
    s, e = two_sum(a[0], -b[0])
    return norm(s, e + (a[1] - b[1]))


def dd_mul(a, b):
    p, e = two_prod(a[0], b[0])
    return norm(p, e + (a[0] * b[1] + a[1] * b[0]))


def dd_div(a, b):
    q = a[0] / b[0]
    p, e = two_prod(q, b[0])
    r = ((a[0] - p) - e) + (a[1] - q * b[1])
    return norm(q, r / b[0])


def lane_sum(v):
    total = jnp.sum(v, axis=1, keepdims=True)
    big = total * 4096.0
    high = (v + big) - big
    low = v - high
    return norm(jnp.sum(high, axis=1, keepdims=True), jnp.sum(low, axis=1, keepdims=True))


def coefficients(mu):
    theta = dd_div(mu[1], mu[0])
    s = [None] + [dd_sub(mu[j + 1], dd_mul(theta, mu[j])) for j in range(1, 5)]
    a1 = dd_sub(dd_div(s[2], s[1]), theta)
    b1 = dd_div(s[1], mu[0])

    def second(j):
        return dd_sub(dd_sub(s[j + 1], dd_mul(a1, s[j])), dd_mul(b1, mu[j]))

    t2, t3 = second(2), second(3)
    a2 = dd_sub(dd_sub(dd_div(t3, t2), a1), theta)
    b2 = dd_div(t2, s[1])
    a0, a1, a2, b1, b2 = theta[0], a1[0], a2[0], b1[0], b2[0]
    d0 = a0
    d1 = a1 - b1 / d0
    d2 = a2 - b2 / d1
    y2 = 1.0 / (d0 * d1 * d2)
    y1 = (-1.0 / d0 - b2 * y2) / d1
    y0 = (1.0 - b1 * y1) / d0
    c2 = y2
    c1 = y1 - (a0 + a1) * y2
    c0 = y0 - a0 * y1 + (a0 * a1 - b1) * y2
    return c0, c1, c2


def spot_of(x, y=0):
    return pl.multiple_of((x + 2) * PITCH + LOW, 8) + y


def zero_edges(w):
    z8 = jnp.zeros((8, BZ), F32)
    for t in range(2 * PITCH // 8):
        w[pl.ds(8 * t, 8), :] = z8
        w[pl.ds(ROWS - LOW - 2 * PITCH + LOW + 8 * t, 8), :] = z8

    def body(x, carry):
        w[pl.ds(pl.multiple_of((x + 2) * PITCH, 8), 8), :] = z8
        return carry

    lax.fori_loop(0, BX + 1, body, 0, unroll=5)


def krylov(
    load, stiff, w0, w1, w2, coef, fault_sum,
    bv, sv, minv, ypack, zpack, edge, trac,
    hx, hy, hz, fault, part_a, part_b,
    in_sem, xs_sem, xr_sem, ys_sem, yr_sem, zs_sem, zr_sem, fs_sem, fr_sem, rs_sem, rr_sem,
):
    gx, gy, gz = (lax.axis_index(a) for a in ("gx", "gy", "gz"))
    nx, ny, nz = (lax.axis_size(a) for a in ("gx", "gy", "gz"))
    group = ny * nz
    spot = gy * nz + gz
    lane = lax.broadcasted_iota(jnp.int32, (8, BZ), 1)
    row = lax.broadcasted_iota(jnp.int32, (8, BZ), 0)
    place = (lane + 2) & 3
    halo_here = (place >> 1) == (1 - gz)
    packs = (BX // SLOTS) * TILES

    step = BX // CHUNKS
    loads = []
    for i in range(CHUNKS):
        part = pl.ds(i * step, step)
        a = pltpu.make_async_copy(load.at[part], bv.at[part], in_sem.at[0, i])
        b = pltpu.make_async_copy(stiff.at[part], sv.at[part], in_sem.at[1, i])
        a.start()
        b.start()
        loads.append((a, b))

    barrier = pltpu.get_barrier_semaphore()
    peers = []
    for r in range(1, group):
        other = lax.rem(spot + r, group)
        peers.append((gx, other // nz, lax.rem(other, nz)))
    cross = [(lax.rem(gx + r, nx), gy, gz) for r in range(1, nx)]
    for peer in peers + cross:
        pl.semaphore_signal(barrier, inc=1, device_id=peer, device_id_type=MESH)

    for w in (w0, w1, w2):
        zero_edges(w)

    zero = jnp.zeros((8, BZ), F32)
    mu0 = zero
    for i in range(CHUNKS):
        loads[i][0].wait()
        loads[i][1].wait()

        def start_plane(x, acc):
            for t in range(TILES):
                at = pl.ds(8 * t, 8)
                b = bv[x, at, :]
                inverse = 1.0 / (7.5 + sv[x, at, :])
                w = b * inverse
                w0[pl.ds(spot_of(x, 8 * t), 8), :] = w
                minv[pl.ds(pl.multiple_of(x * BY, 8) + 8 * t, 8), :] = inverse * (1.0 / 12.0)
                acc = acc + b * w
            return acc

        mu0 = lax.fori_loop(i * step, (i + 1) * step, start_plane, mu0, unroll=min(step, UNROLL))

    pl.semaphore_wait(barrier, len(peers) + len(cross))

    def remote(src, dst, send, recv, device):
        return pltpu.make_async_remote_copy(
            src_ref=src, dst_ref=dst, send_sem=send, recv_sem=recv,
            device_id=device, device_id_type=MESH,
        )

    def x_copy(w, k, side):
        plane = 0 if side == 0 else BX - 2
        return remote(
            w.at[pl.ds(spot_of(plane), FACE), :], hx.at[k, 1 - side],
            xs_sem.at[k, side], xr_sem.at[k, 1 - side],
            (gx - 1 if side == 0 else gx + 1, gy, gz),
        )

    def y_copy(k, side):
        return remote(
            ypack.at[k, side], hy.at[k, 1 - side],
            ys_sem.at[k, side], yr_sem.at[k, 1 - side],
            (gx, gy - 1 if side == 0 else gy + 1, gz),
        )

    def z_copy(k):
        return remote(zpack.at[k], hz.at[k], zs_sem.at[k], zr_sem.at[k], (gx, gy, 1 - gz))

    has_x = (gx > 0, gx < nx - 1)
    has_y = (gy > 0, gy < ny - 1)
    near_fault = (gy == ny // 2 - 1) | (gy == ny // 2)
    source = gy - (ny // 2 - 1)
    low_side = jnp.where(gy == ny // 2, 1.0, 0.0)
    high_side = jnp.where(gy == ny // 2 - 1, 1.0, 0.0)
    own_rows = BX // ny

    def fault_copy(k, r):
        owner = lax.rem(gy + r, ny)
        return remote(
            trac.at[k, pl.ds(owner * own_rows, own_rows), :], fault.at[source, k],
            fs_sem.at[k, r - 1], fr_sem.at[source, k], (gx, owner, gz),
        )

    def exchange(w, k):
        for j in range(STRIPS):
            strip = []
            for n, y in enumerate((0, 1, BY - 2, BY - 1)):
                v = w[pl.ds(spot_of(8 * j, y), 8, stride=PITCH), :]
                ypack[k, n // 2, n % 2, pl.ds(8 * j, 8), :] = v
                strip.append(v)
            term = low_side * (27.0 * strip[0] - strip[1]) + high_side * (strip[2] - 27.0 * strip[3])
            trac[k, pl.ds(8 * j, 8), :] = term / 24.0
        for side in range(2):
            @pl.when(has_x[side])
            def _(side=side):
                x_copy(w, k, side).start()
        for side in range(2):
            @pl.when(has_y[side])
            def _(side=side):
                y_copy(k, side).start()

        for half in range(BX // SLOTS):
            def pack(q, acc, half=half):
                mask = ((lane + 2 - 4 * q) & (BZ - 1)) < 4
                return tuple(
                    jnp.where(
                        mask,
                        pltpu.roll(w[pl.ds(spot_of(half * SLOTS + q, 8 * t), 8), :], 4 * q, 1),
                        acc[t],
                    )
                    for t in range(TILES)
                )

            packed = lax.fori_loop(0, SLOTS, pack, (zero,) * TILES, unroll=2 * UNROLL)
            for t in range(TILES):
                zpack[k, half * TILES + t] = packed[t]

        @pl.when(near_fault)
        def _():
            for r in range(1, ny):
                fault_copy(k, r).start()
            for i in range(own_rows // 8):
                fault[source, k, pl.ds(8 * i, 8), :] = trac[
                    k, pl.ds(pl.multiple_of(gy * own_rows + 8 * i, 8), 8), :
                ]

        z_copy(k).start()

    def edge_terms(d):
        near = jnp.where(place == 1, pltpu.roll(d, BZ - 1, 1), pltpu.roll(d, 1, 1))
        near = jnp.where((place == 1) | (place == 2), near, 0.0)
        return 16.0 * near - jnp.where(place < 2, pltpu.roll(d, BZ - 2, 1), pltpu.roll(d, 2, 1))

    def bulk(w, out, k, init, with_halo):
        if with_halo:
            z_copy(k).wait_recv()
        for i in range(packs):
            d = -zpack[k, i]
            if with_halo:
                d = d + jnp.where(halo_here, hz[k, i], 0.0)
            edge[i] = edge_terms(d)

        def plane(x, acc):
            q = lax.rem(x, SLOTS)
            mask = ((lane + 2) & (BZ - 1)) < 4
            for t in range(TILES):
                def at(dx, dy):
                    return w[pl.ds(spot_of(x, 8 * t) + (dx * PITCH + dy), 8), :]

                c = at(0, 0)
                e = pltpu.roll(edge[(x // SLOTS) * TILES + t], lax.rem(BZ - 4 * q, BZ), 1)
                near = pltpu.roll(c, BZ - 1, 1) + pltpu.roll(c, 1, 1)
                far = pltpu.roll(c, BZ - 2, 1) + pltpu.roll(c, 2, 1)
                near = (at(1, 0) + at(-1, 0)) + near + (at(0, 1) + at(0, -1))
                far = (at(2, 0) + at(-2, 0)) + far + (at(0, 2) + at(0, -2))
                n = (16.0 * near - far) + jnp.where(mask, e, 0.0)
                acc = out(x, t, c, n, acc)
            return acc

        return lax.fori_loop(0, BX, plane, init, unroll=UNROLL)

    def fixes(k, apply_x, apply_y):
        for side in range(2):
            @pl.when(has_x[side])
            def _(side=side):
                x_copy(w0, k, 1 - side).wait_recv()
                inner, outer = (1, 0) if side == 0 else (0, 1)
                first, second = (0, 1) if side == 0 else (BX - 1, BX - 2)
                for t in range(TILES):
                    close = hx[k, side, pl.ds(inner * PITCH + 8 * t, 8), :]
                    distant = hx[k, side, pl.ds(outer * PITCH + 8 * t, 8), :]
                    apply_x(first, t, 16.0 * close - distant)
                    apply_x(second, t, -close)
        for side in range(2):
            @pl.when(has_y[side])
            def _(side=side):
                y_copy(k, 1 - side).wait_recv()
                inner, outer = (1, 0) if side == 0 else (0, 1)
                first, second = (0, 1) if side == 0 else (BY - 1, BY - 2)
                for j in range(STRIPS):
                    at = pl.ds(8 * j, 8)
                    close = hy[k, side, inner, at, :]
                    apply_y(j, first, 16.0 * close - hy[k, side, outer, at, :])
                    apply_y(j, second, -close)

    def basis_step(w, new, k, moments, init):
        exchange(w, k)

        def out(x, t, c, n, acc):
            new[pl.ds(spot_of(x, 8 * t), 8), :] = (
                c - minv[pl.ds(pl.multiple_of(x * BY, 8) + 8 * t, 8), :] * n
            )
            return moments(x, t, c, acc)

        sums = bulk(w, out, k, init, True)

        def apply_x(x, t, n):
            at = pl.ds(spot_of(x, 8 * t), 8)
            new[at, :] = new[at, :] - minv[pl.ds(x * BY + 8 * t, 8), :] * n

        def apply_y(j, y, n):
            at = pl.ds(spot_of(8 * j, y), 8, stride=PITCH)
            new[at, :] = new[at, :] - minv[pl.ds(8 * j * BY + y, 8, stride=BY), :] * n

        fixes(k, apply_x, apply_y)
        return sums

    basis_step(w0, w1, 0, lambda x, t, c, acc: acc, 0)

    def first_moments(x, t, c, acc):
        at = pl.ds(8 * t, 8)
        return (acc[0] + bv[x, at, :] * c, acc[1] + ((7.5 + sv[x, at, :]) * c) * c)

    mu1, mu2 = basis_step(w1, w2, 1, first_moments, (zero, zero))

    exchange(w2, 2)

    def last(x, t, c, n, acc):
        d = (7.5 + sv[x, pl.ds(8 * t, 8), :]) * c
        return (
            acc[0] + d * w1[pl.ds(spot_of(x, 8 * t), 8), :],
            acc[1] + d * c,
            acc[2] + c * (d - n * (1.0 / 12.0)),
        )

    mu3, mu4, mu5 = bulk(w2, last, 2, (zero, zero, zero), False)
    part_a[0] = zero

    def cross_x(x, t, n):
        part_a[0] = part_a[0] + w2[pl.ds(spot_of(x, 8 * t), 8), :] * n

    def cross_y(j, y, n):
        part_a[0] = part_a[0] + w2[pl.ds(spot_of(8 * j, y), 8, stride=PITCH), :] * n

    z_copy(2).wait_recv()
    crossing = zero
    for i in range(packs):
        crossing = crossing + zpack[2, i] * edge_terms(jnp.where(halo_here, hz[2, i], 0.0))
    fixes(2, cross_x, cross_y)
    mu5 = mu5 - (part_a[0] + crossing) * (1.0 / 12.0)

    local = zero
    for j, m in enumerate((mu0, mu1, mu2, mu3, mu4, mu5)):
        local = jnp.where(row == j, jnp.sum(m, axis=0, keepdims=True), local)

    def reduce(value, buf, s, devices):
        buf[0] = value
        copies = [
            remote(buf.at[0], buf.at[r + 1], rs_sem.at[s, r], rr_sem.at[s, r], device)
            for r, device in enumerate(devices)
        ]
        for c in copies:
            c.start()
        for c in copies:
            c.wait_recv()
        total = value
        for r in range(len(devices)):
            total = total + buf[r + 1]
        return total, copies

    total, sent_a = reduce(local, part_a, 0, peers)
    total, sent_b = reduce(total, part_b, 1, cross)

    mu = []
    for j in range(6):
        mu.append(lane_sum(jnp.broadcast_to(total[j : j + 1, :], (8, BZ))))
    for j, c in enumerate(coefficients(mu)):
        coef[j] = jnp.broadcast_to(c, (8, BZ))

    for k in range(3):
        for s in range(2):
            @pl.when(gy != ny // 2 - 1 + s)
            def _(k=k, s=s):
                remote(
                    trac.at[k, pl.ds(0, own_rows), :], fault.at[s, k],
                    fs_sem.at[k, 0], fr_sem.at[s, k], (gx, gy, 1 - gz),
                ).wait_recv()
    for k in range(3):
        for i in range(own_rows // 8):
            at = pl.ds(8 * i, 8)
            fault_sum[k, at, :] = fault[0, k, at, :] + fault[1, k, at, :]

    for c in sent_a + sent_b:
        c.wait_send()
    for k in range(3):
        for side in range(2):
            @pl.when(has_x[side])
            def _(k=k, side=side):
                x_copy(w0, k, side).wait_send()
            @pl.when(has_y[side])
            def _(k=k, side=side):
                y_copy(k, side).wait_send()
        z_copy(k).wait_send()

        @pl.when(near_fault)
        def _(k=k):
            for r in range(1, ny):
                fault_copy(k, r).wait_send()


def combine(w0, w1, w2, coef, fault_sum, prestress, state, normal, u, slip, buf, sem):
    c0, c1, c2 = coef[0], coef[1], coef[2]
    step = BX // CHUNKS
    copies = []
    for i in range(CHUNKS):
        def plane(x, carry):
            for t in range(TILES):
                at = pl.ds(spot_of(x, 8 * t), 8)
                buf[x, pl.ds(8 * t, 8), :] = (c0 * w0[at, :] + c1 * w1[at, :]) + c2 * w2[at, :]
            return carry

        lax.fori_loop(i * step, (i + 1) * step, plane, 0)
        part = pl.ds(i * step, step)
        copy = pltpu.make_async_copy(buf.at[part], u.at[part], sem.at[i])
        copy.start()
        copies.append(copy)
    for i in range(slip.shape[0] // 8):
        at = pl.ds(8 * i, 8)
        traction = (c0 * fault_sum[0, at, :] + c1 * fault_sum[1, at, :]) + c2 * fault_sum[2, at, :]
        x = (prestress[at, :] + 2.0 * traction) / normal[at, :]
        half = 0.6931471805599453
        large = jnp.exp(x - half) - jnp.exp(-x - half)
        q = x * x
        small = x * (1.0 + q * (1 / 6 + q * (1 / 120 + q * (1 / 5040 + q * (1 / 362880 + q / 39916800)))))
        sinh = jnp.where(jnp.abs(x) < 1.0, small, large)
        slip[at, :] = jnp.exp(-state[at, :]) * sinh
    for copy in copies:
        copy.wait()


def per_device(load, stiffness, prestress, state_var, normal_a):
    vmem = pl.BlockSpec(memory_space=pltpu.VMEM)
    hbm = pl.BlockSpec(memory_space=pl.ANY)
    ny = lax.axis_size("gy")
    own = BX // ny
    group = ny * lax.axis_size("gz")
    nx = lax.axis_size("gx")
    big = (ROWS, BZ)
    packs = (BX // SLOTS) * TILES
    DMA = pltpu.SemaphoreType.DMA
    outs = pl.pallas_call(
        krylov,
        out_shape=[
            pltpu.VMEM(big, F32), pltpu.VMEM(big, F32), pltpu.VMEM(big, F32),
            pltpu.VMEM((3, 8, BZ), F32), pltpu.VMEM((3, own, BZ), F32),
        ],
        in_specs=[pl.BlockSpec(memory_space=pltpu.HBM)] * 2,
        out_specs=[vmem] * 5,
        scratch_shapes=[
            pltpu.VMEM((BX, BY, BZ), F32),
            pltpu.VMEM((BX, BY, BZ), F32),
            pltpu.VMEM((BX * BY, BZ), F32),
            pltpu.VMEM((3, 2, 2, BX, BZ), F32),
            pltpu.VMEM((3, packs, 8, BZ), F32),
            pltpu.VMEM((packs, 8, BZ), F32),
            pltpu.VMEM((3, BX, BZ), F32),
            pltpu.VMEM((3, 2, FACE, BZ), F32),
            pltpu.VMEM((3, 2, 2, BX, BZ), F32),
            pltpu.VMEM((3, packs, 8, BZ), F32),
            pltpu.VMEM((2, 3, own, BZ), F32),
            pltpu.VMEM((group, 8, BZ), F32),
            pltpu.VMEM((nx, 8, BZ), F32),
            DMA((2, CHUNKS)),
            DMA((3, 2)), DMA((3, 2)), DMA((3, 2)), DMA((3, 2)), DMA((3,)), DMA((3,)),
            DMA((3, ny - 1)), DMA((2, 3)),
            DMA((2, nx - 1)), DMA((2, nx - 1)),
        ],
        compiler_params=pltpu.CompilerParams(
            collective_id=0, has_side_effects=True, vmem_limit_bytes=55 * 2**20
        ),
        name="krylov",
    )(load, stiffness)
    return pl.pallas_call(
        combine,
        out_shape=[
            jax.ShapeDtypeStruct(load.shape, F32),
            jax.ShapeDtypeStruct(prestress.shape, F32),
        ],
        in_specs=[vmem] * 8,
        out_specs=[hbm, vmem],
        scratch_shapes=[pltpu.VMEM((BX, BY, BZ), F32), DMA((CHUNKS,))],
        compiler_params=pltpu.CompilerParams(vmem_limit_bytes=24 * 2**20),
        name="combine",
    )(*outs, prestress, state_var, normal_a)


def solution(mesh):
    block = P("gx", "gy", "gz")
    fault = P(("gx", "gy"), "gz")
    return jax.shard_map(
        per_device,
        mesh=mesh,
        in_specs=(block, block, fault, fault, fault),
        out_specs=(block, fault),
        check_vma=False,
    )
```

```python
import functools

import jax
import jax.numpy as jnp
from jax import lax
from jax.experimental import pallas as pl
from jax.experimental.pallas import tpu as pltpu
from jax.sharding import PartitionSpec as P

MESH = pl.DeviceIdType.MESH
F32 = jnp.float32
BX, BY, BZ = 64, 64, 128
LOW = 8
PITCH = BY + LOW
ROWS = (BX + 4) * PITCH + LOW
FACE = PITCH + BY
TILES = BY // 8
STRIPS = BX // 8
CHUNKS = 8
SLOTS = 32
UNROLL = 8


def two_sum(a, b):
    s = a + b
    t = s - a
    return s, (a - (s - t)) + (b - t)


def split(a):
    t = a * 4097.0
    high = t - (t - a)
    return high, a - high


def two_prod(a, b):
    p = a * b
    ah, al = split(a)
    bh, bl = split(b)
    return p, ((ah * bh - p) + ah * bl + al * bh) + al * bl


def norm(h, l):
    s = h + l
    return s, l - (s - h)


def dd_sub(a, b):
    s, e = two_sum(a[0], -b[0])
    return norm(s, e + (a[1] - b[1]))


def dd_mul(a, b):
    p, e = two_prod(a[0], b[0])
    return norm(p, e + (a[0] * b[1] + a[1] * b[0]))


def dd_div(a, b):
    q = a[0] / b[0]
    p, e = two_prod(q, b[0])
    r = ((a[0] - p) - e) + (a[1] - q * b[1])
    return norm(q, r / b[0])


def lane_sum(v):
    total = jnp.sum(v, axis=1, keepdims=True)
    big = total * 4096.0
    high = (v + big) - big
    low = v - high
    return norm(jnp.sum(high, axis=1, keepdims=True), jnp.sum(low, axis=1, keepdims=True))


def coefficients(mu):
    theta = dd_div(mu[1], mu[0])
    s = [None] + [dd_sub(mu[j + 1], dd_mul(theta, mu[j])) for j in range(1, 5)]
    a1 = dd_sub(dd_div(s[2], s[1]), theta)
    b1 = dd_div(s[1], mu[0])

    def second(j):
        return dd_sub(dd_sub(s[j + 1], dd_mul(a1, s[j])), dd_mul(b1, mu[j]))

    t2, t3 = second(2), second(3)
    a2 = dd_sub(dd_sub(dd_div(t3, t2), a1), theta)
    b2 = dd_div(t2, s[1])
    a0, a1, a2, b1, b2 = theta[0], a1[0], a2[0], b1[0], b2[0]
    d0 = a0
    d1 = a1 - b1 / d0
    d2 = a2 - b2 / d1
    y2 = 1.0 / (d0 * d1 * d2)
    y1 = (-1.0 / d0 - b2 * y2) / d1
    y0 = (1.0 - b1 * y1) / d0
    c2 = y2
    c1 = y1 - (a0 + a1) * y2
    c0 = y0 - a0 * y1 + (a0 * a1 - b1) * y2
    return c0, c1, c2


def spot_of(x, y=0):
    return pl.multiple_of((x + 2) * PITCH + LOW, 8) + y


def zero_edges(w):
    z8 = jnp.zeros((8, BZ), F32)
    for t in range(2 * PITCH // 8):
        w[pl.ds(8 * t, 8), :] = z8
        w[pl.ds(ROWS - LOW - 2 * PITCH + LOW + 8 * t, 8), :] = z8

    def body(x, carry):
        w[pl.ds(pl.multiple_of((x + 2) * PITCH, 8), 8), :] = z8
        return carry

    lax.fori_loop(0, BX + 1, body, 0, unroll=5)


def krylov(
    load, stiff, w0, w1, w2, coef, fault_sum,
    bv, sv, minv, ypack, zpack, edge, trac,
    hx, hy, hz, fault, part_a, part_b,
    in_sem, xs_sem, xr_sem, ys_sem, yr_sem, zs_sem, zr_sem, fs_sem, fr_sem, rs_sem, rr_sem, token,
):
    gx, gy, gz = (lax.axis_index(a) for a in ("gx", "gy", "gz"))
    nx, ny, nz = (lax.axis_size(a) for a in ("gx", "gy", "gz"))
    group = ny * nz
    spot = gy * nz + gz
    lane = lax.broadcasted_iota(jnp.int32, (8, BZ), 1)
    row = lax.broadcasted_iota(jnp.int32, (8, BZ), 0)
    place = (lane + 2) & 3
    halo_here = (place >> 1) == (1 - gz)
    packs = (BX // SLOTS) * TILES

    step = BX // CHUNKS
    loads = []
    order = [0, CHUNKS - 1] + list(range(1, CHUNKS - 1))
    for i in order:
        part = pl.ds(i * step, step)
        a = pltpu.make_async_copy(load.at[part], bv.at[part], in_sem.at[0, i])
        b = pltpu.make_async_copy(stiff.at[part], sv.at[part], in_sem.at[1, i])
        a.start()
        b.start()
        loads.append((a, b))

    barrier = pltpu.get_barrier_semaphore()
    peers = []
    for r in range(1, group):
        other = lax.rem(spot + r, group)
        peers.append((gx, other // nz, lax.rem(other, nz)))
    cross = [(lax.rem(gx + r, nx), gy, gz) for r in range(1, nx)]
    has_x = (gx > 0, gx < nx - 1)
    has_y = (gy > 0, gy < ny - 1)

    def one(flag):
        return jnp.where(flag, 1, 0)

    def sides(distance):
        return ((gx >= distance, gx - distance), (gx + distance < nx, gx + distance))

    def signal(k, distance):
        for side, (there, target) in enumerate(sides(distance)):
            @pl.when(there)
            def _(side=side, target=target):
                pl.semaphore_signal(
                    token.at[k, 1 - side], inc=1, device_id=(target, gy, gz), device_id_type=MESH
                )

    def await_signals(k, distance):
        for side, (there, _) in enumerate(sides(distance)):
            @pl.when(there)
            def _(side=side):
                pl.semaphore_wait(token.at[k, side], 1)

    for there, target in sides(1):
        @pl.when(there)
        def _(target=target):
            pl.semaphore_signal(barrier, inc=1, device_id=(target, gy, gz), device_id_type=MESH)
    for side in range(2):
        @pl.when(has_y[side])
        def _(side=side):
            pl.semaphore_signal(
                barrier, inc=1, device_id=(gx, gy + 2 * side - 1, gz), device_id_type=MESH
            )
    pl.semaphore_signal(barrier, inc=1, device_id=(gx, gy, 1 - gz), device_id_type=MESH)

    for w in (w0, w1, w2):
        zero_edges(w)

    def remote(src, dst, send, recv, device):
        return pltpu.make_async_remote_copy(
            src_ref=src, dst_ref=dst, send_sem=send, recv_sem=recv,
            device_id=device, device_id_type=MESH,
        )

    def x_copies(w, k, side):
        plane = 0 if side == 0 else BX - 2
        device = (gx - 1 if side == 0 else gx + 1, gy, gz)
        if k < 2:
            return [
                remote(
                    w.at[pl.ds(spot_of(plane), FACE), :], hx.at[k, 1 - side],
                    xs_sem.at[k, side, 0], xr_sem.at[k, 1 - side, 0], device,
                )
            ]
        half = BY // 2
        return [
            remote(
                w.at[pl.ds(spot_of(plane + n, side * half), half), :],
                hx.at[k, 1 - side, pl.ds(n * PITCH + side * half, half), :],
                xs_sem.at[k, side, n], xr_sem.at[k, 1 - side, n], device,
            )
            for n in range(2)
        ]

    def y_copy(k, side):
        strips = pl.ds(0, BX) if k < 2 else pl.ds(side * (BX // 2), BX // 2)
        return remote(
            ypack.at[k, side, :, strips, :], hy.at[k, 1 - side, :, strips, :],
            ys_sem.at[k, side], yr_sem.at[k, 1 - side],
            (gx, gy - 1 if side == 0 else gy + 1, gz),
        )

    def z_copy(k):
        return remote(zpack.at[k], hz.at[k], zs_sem.at[k], zr_sem.at[k], (gx, gy, 1 - gz))

    near_fault = (gy == ny // 2 - 1) | (gy == ny // 2)
    source = gy - (ny // 2 - 1)
    low_side = jnp.where(gy == ny // 2, 1.0, 0.0)
    high_side = jnp.where(gy == ny // 2 - 1, 1.0, 0.0)
    own_rows = BX // ny

    def fault_copy(k, r):
        owner = lax.rem(gy + r, ny)
        return remote(
            trac.at[k, pl.ds(owner * own_rows, own_rows), :], fault.at[source, k],
            fs_sem.at[k, r - 1], fr_sem.at[source, k], (gx, owner, gz),
        )

    def send_x(w, k):
        for side in range(2):
            @pl.when(has_x[side])
            def _(side=side):
                for copy in x_copies(w, k, side):
                    copy.start()

    def send_fault(k):
        @pl.when(near_fault)
        def _():
            for r in range(1, ny):
                fault_copy(k, r).start()
            for i in range(own_rows // 8):
                fault[source, k, pl.ds(8 * i, 8), :] = trac[
                    k, pl.ds(pl.multiple_of(gy * own_rows + 8 * i, 8), 8), :
                ]

    def exchange(w, k):
        for j in range(STRIPS):
            strip = []
            for n, y in enumerate((0, 1, BY - 2, BY - 1)):
                v = w[pl.ds(spot_of(8 * j, y), 8, stride=PITCH), :]
                ypack[k, n // 2, n % 2, pl.ds(8 * j, 8), :] = v
                strip.append(v)
            term = low_side * (27.0 * strip[0] - strip[1]) + high_side * (strip[2] - 27.0 * strip[3])
            trac[k, pl.ds(8 * j, 8), :] = term / 24.0
        for side in range(2):
            @pl.when(has_y[side])
            def _(side=side):
                y_copy(k, side).start()

        for half in range(BX // SLOTS):
            def pack(q, acc, half=half):
                mask = ((lane + 2 - 4 * q) & (BZ - 1)) < 4
                return tuple(
                    jnp.where(
                        mask,
                        pltpu.roll(w[pl.ds(spot_of(half * SLOTS + q, 8 * t), 8), :], 4 * q, 1),
                        acc[t],
                    )
                    for t in range(TILES)
                )

            packed = lax.fori_loop(0, SLOTS, pack, (zero,) * TILES, unroll=2 * UNROLL)
            for t in range(TILES):
                zpack[k, half * TILES + t] = packed[t]

        z_copy(k).start()
        if k == 2:
            for n in range(3):
                send_fault(n)

    zero = jnp.zeros((8, BZ), F32)
    mu0 = zero
    for n, i in enumerate(order):
        first_wait, second_wait = loads[n]
        first_wait.wait()
        second_wait.wait()

        def start_plane(x, acc):
            for t in range(TILES):
                at = pl.ds(8 * t, 8)
                b = bv[x, at, :]
                inverse = 1.0 / (7.5 + sv[x, at, :])
                w = b * inverse
                w0[pl.ds(spot_of(x, 8 * t), 8), :] = w
                minv[pl.ds(pl.multiple_of(x * BY, 8) + 8 * t, 8), :] = inverse * (1.0 / 12.0)
                acc = acc + b * w
            return acc

        mu0 = lax.fori_loop(i * step, (i + 1) * step, start_plane, mu0, unroll=min(step, UNROLL))
        if n == 1:
            pl.semaphore_wait(
                barrier,
                1 + one(has_x[0]) + one(has_x[1]) + one(has_y[0]) + one(has_y[1]),
            )
            send_x(w0, 0)

    def edge_terms(d):
        near = jnp.where(place == 1, pltpu.roll(d, BZ - 1, 1), pltpu.roll(d, 1, 1))
        near = jnp.where((place == 1) | (place == 2), near, 0.0)
        return 16.0 * near - jnp.where(place < 2, pltpu.roll(d, BZ - 2, 1), pltpu.roll(d, 2, 1))

    def bulk(w, out, k, init, with_halo):
        if with_halo:
            z_copy(k).wait_recv()
        for i in range(packs):
            d = -zpack[k, i]
            if with_halo:
                d = d + jnp.where(halo_here, hz[k, i], 0.0)
            edge[i] = edge_terms(d)

        def plane(x, acc):
            q = lax.rem(x, SLOTS)
            mask = ((lane + 2) & (BZ - 1)) < 4
            for t in range(TILES):
                def at(dx, dy):
                    return w[pl.ds(spot_of(x, 8 * t) + (dx * PITCH + dy), 8), :]

                c = at(0, 0)
                e = pltpu.roll(edge[(x // SLOTS) * TILES + t], lax.rem(BZ - 4 * q, BZ), 1)
                near = pltpu.roll(c, BZ - 1, 1) + pltpu.roll(c, 1, 1)
                far = pltpu.roll(c, BZ - 2, 1) + pltpu.roll(c, 2, 1)
                near = (at(1, 0) + at(-1, 0)) + near + (at(0, 1) + at(0, -1))
                far = (at(2, 0) + at(-2, 0)) + far + (at(0, 2) + at(0, -2))
                n = (16.0 * near - far) + jnp.where(mask, e, 0.0)
                acc = out(x, t, c, n, acc)
            return acc

        return lax.fori_loop(0, BX, plane, init, unroll=UNROLL)

    def fixes(k, apply_x, apply_y):
        whole = k < 2
        for side in range(2):
            @pl.when(has_y[side])
            def _(side=side):
                y_copy(k, 1 - side).wait_recv()
                inner, outer = (1, 0) if side == 0 else (0, 1)
                first, second = (0, 1) if side == 0 else (BY - 1, BY - 2)
                span = range(STRIPS)
                if not whole:
                    span = range((1 - side) * STRIPS // 2, (2 - side) * STRIPS // 2)
                for j in span:
                    at = pl.ds(8 * j, 8)
                    close = hy[k, side, inner, at, :]
                    apply_y(j, first, 16.0 * close - hy[k, side, outer, at, :])
                    apply_y(j, second, -close)
        for side in range(2):
            @pl.when(has_x[side])
            def _(side=side):
                for copy in x_copies(w0, k, 1 - side):
                    copy.wait_recv()
                inner, outer = (1, 0) if side == 0 else (0, 1)
                first, second = (0, 1) if side == 0 else (BX - 1, BX - 2)
                span = range(TILES)
                if not whole:
                    span = range((1 - side) * TILES // 2, (2 - side) * TILES // 2)
                for t in span:
                    close = hx[k, side, pl.ds(inner * PITCH + 8 * t, 8), :]
                    distant = hx[k, side, pl.ds(outer * PITCH + 8 * t, 8), :]
                    apply_x(first, t, 16.0 * close - distant)
                    apply_x(second, t, -close)

    def basis_step(w, new, k, moments, init):
        exchange(w, k)

        def out(x, t, c, n, acc):
            new[pl.ds(spot_of(x, 8 * t), 8), :] = (
                c - minv[pl.ds(pl.multiple_of(x * BY, 8) + 8 * t, 8), :] * n
            )
            return moments(x, t, c, acc)

        sums = bulk(w, out, k, init, True)

        def apply_x(x, t, n):
            at = pl.ds(spot_of(x, 8 * t), 8)
            new[at, :] = new[at, :] - minv[pl.ds(x * BY + 8 * t, 8), :] * n

        def apply_y(j, y, n):
            at = pl.ds(spot_of(8 * j, y), 8, stride=PITCH)
            new[at, :] = new[at, :] - minv[pl.ds(8 * j * BY + y, 8, stride=BY), :] * n

        fixes(k, apply_x, apply_y)
        if k > 0:
            await_signals(k - 1, 1 << k)
        send_x(new, k + 1)
        signal(k, 2 << k)
        return sums

    basis_step(w0, w1, 0, lambda x, t, c, acc: acc, 0)

    def first_moments(x, t, c, acc):
        at = pl.ds(8 * t, 8)
        return (acc[0] + bv[x, at, :] * c, acc[1] + ((7.5 + sv[x, at, :]) * c) * c)

    mu1, mu2 = basis_step(w1, w2, 1, first_moments, (zero, zero))

    exchange(w2, 2)

    def last(x, t, c, n, acc):
        d = (7.5 + sv[x, pl.ds(8 * t, 8), :]) * c
        return (
            acc[0] + d * w1[pl.ds(spot_of(x, 8 * t), 8), :],
            acc[1] + d * c,
            acc[2] + c * (d - n * (1.0 / 12.0)),
        )

    mu3, mu4, mu5 = bulk(w2, last, 2, (zero, zero, zero), False)
    part_a[0] = zero

    def cross_x(x, t, n):
        part_a[0] = part_a[0] + w2[pl.ds(spot_of(x, 8 * t), 8), :] * n

    def cross_y(j, y, n):
        part_a[0] = part_a[0] + w2[pl.ds(spot_of(8 * j, y), 8, stride=PITCH), :] * n

    z_copy(2).wait_recv()
    crossing = zero
    for i in range(packs):
        crossing = crossing + zpack[2, i] * edge_terms(jnp.where(halo_here, hz[2, i], 0.0))
    fixes(2, cross_x, cross_y)
    mu5 = mu5 - (2.0 * part_a[0] + crossing) * (1.0 / 12.0)
    await_signals(1, 4)
    signal(2, 8)

    local = zero
    for j, m in enumerate((mu0, mu1, mu2, mu3, mu4, mu5)):
        local = jnp.where(row == j, jnp.sum(m, axis=0, keepdims=True), local)

    def reduce(value, buf, s, devices):
        buf[0] = value
        copies = [
            remote(buf.at[0], buf.at[r + 1], rs_sem.at[s, r], rr_sem.at[s, r], device)
            for r, device in enumerate(devices)
        ]
        for c in copies:
            c.start()
        for c in copies:
            c.wait_recv()
        total = value
        for r in range(len(devices)):
            total = total + buf[r + 1]
        return total, copies

    total, sent_a = reduce(local, part_a, 0, peers)
    await_signals(2, 8)
    total, sent_b = reduce(total, part_b, 1, cross)

    mu = []
    for j in range(6):
        mu.append(lane_sum(jnp.broadcast_to(total[j : j + 1, :], (8, BZ))))
    for j, c in enumerate(coefficients(mu)):
        coef[j] = jnp.broadcast_to(c, (8, BZ))

    for k in range(3):
        for s in range(2):
            @pl.when(gy != ny // 2 - 1 + s)
            def _(k=k, s=s):
                remote(
                    trac.at[k, pl.ds(0, own_rows), :], fault.at[s, k],
                    fs_sem.at[k, 0], fr_sem.at[s, k], (gx, gy, 1 - gz),
                ).wait_recv()
    for k in range(3):
        for i in range(own_rows // 8):
            at = pl.ds(8 * i, 8)
            fault_sum[k, at, :] = fault[0, k, at, :] + fault[1, k, at, :]

    for c in sent_a + sent_b:
        c.wait_send()
    for k in range(3):
        for side in range(2):
            @pl.when(has_x[side])
            def _(k=k, side=side):
                for copy in x_copies(w0, k, side):
                    copy.wait_send()
            @pl.when(has_y[side])
            def _(k=k, side=side):
                y_copy(k, side).wait_send()
        z_copy(k).wait_send()

        @pl.when(near_fault)
        def _(k=k):
            for r in range(1, ny):
                fault_copy(k, r).wait_send()


def combine(w0, w1, w2, coef, fault_sum, prestress, state, normal, u, slip, buf, sem):
    c0, c1, c2 = coef[0], coef[1], coef[2]
    step = BX // CHUNKS
    copies = []
    for i in range(CHUNKS):
        def plane(x, carry):
            for t in range(TILES):
                at = pl.ds(spot_of(x, 8 * t), 8)
                buf[x, pl.ds(8 * t, 8), :] = (c0 * w0[at, :] + c1 * w1[at, :]) + c2 * w2[at, :]
            return carry

        lax.fori_loop(i * step, (i + 1) * step, plane, 0)
        part = pl.ds(i * step, step)
        copy = pltpu.make_async_copy(buf.at[part], u.at[part], sem.at[i])
        copy.start()
        copies.append(copy)
    for i in range(slip.shape[0] // 8):
        at = pl.ds(8 * i, 8)
        traction = (c0 * fault_sum[0, at, :] + c1 * fault_sum[1, at, :]) + c2 * fault_sum[2, at, :]
        x = (prestress[at, :] + 2.0 * traction) / normal[at, :]
        half = 0.6931471805599453
        large = jnp.exp(x - half) - jnp.exp(-x - half)
        q = x * x
        small = x * (1.0 + q * (1 / 6 + q * (1 / 120 + q * (1 / 5040 + q * (1 / 362880 + q / 39916800)))))
        sinh = jnp.where(jnp.abs(x) < 1.0, small, large)
        slip[at, :] = jnp.exp(-state[at, :]) * sinh
    for copy in copies:
        copy.wait()


def per_device(load, stiffness, prestress, state_var, normal_a):
    vmem = pl.BlockSpec(memory_space=pltpu.VMEM)
    hbm = pl.BlockSpec(memory_space=pl.ANY)
    ny = lax.axis_size("gy")
    own = BX // ny
    group = ny * lax.axis_size("gz")
    nx = lax.axis_size("gx")
    big = (ROWS, BZ)
    packs = (BX // SLOTS) * TILES
    DMA = pltpu.SemaphoreType.DMA
    outs = pl.pallas_call(
        krylov,
        out_shape=[
            pltpu.VMEM(big, F32), pltpu.VMEM(big, F32), pltpu.VMEM(big, F32),
            pltpu.VMEM((3, 8, BZ), F32), pltpu.VMEM((3, own, BZ), F32),
        ],
        in_specs=[pl.BlockSpec(memory_space=pltpu.HBM)] * 2,
        out_specs=[vmem] * 5,
        scratch_shapes=[
            pltpu.VMEM((BX, BY, BZ), F32),
            pltpu.VMEM((BX, BY, BZ), F32),
            pltpu.VMEM((BX * BY, BZ), F32),
            pltpu.VMEM((3, 2, 2, BX, BZ), F32),
            pltpu.VMEM((3, packs, 8, BZ), F32),
            pltpu.VMEM((packs, 8, BZ), F32),
            pltpu.VMEM((3, BX, BZ), F32),
            pltpu.VMEM((3, 2, FACE, BZ), F32),
            pltpu.VMEM((3, 2, 2, BX, BZ), F32),
            pltpu.VMEM((3, packs, 8, BZ), F32),
            pltpu.VMEM((2, 3, own, BZ), F32),
            pltpu.VMEM((group, 8, BZ), F32),
            pltpu.VMEM((nx, 8, BZ), F32),
            DMA((2, CHUNKS)),
            DMA((3, 2, 2)), DMA((3, 2, 2)), DMA((3, 2)), DMA((3, 2)), DMA((3,)), DMA((3,)),
            DMA((3, ny - 1)), DMA((2, 3)),
            DMA((2, nx - 1)), DMA((2, nx - 1)),
            pltpu.SemaphoreType.REGULAR((3, 2)),
        ],
        compiler_params=pltpu.CompilerParams(
            collective_id=0, has_side_effects=True, vmem_limit_bytes=55 * 2**20
        ),
        name="krylov",
    )(load, stiffness)
    return pl.pallas_call(
        combine,
        out_shape=[
            jax.ShapeDtypeStruct(load.shape, F32),
            jax.ShapeDtypeStruct(prestress.shape, F32),
        ],
        in_specs=[vmem] * 8,
        out_specs=[hbm, vmem],
        scratch_shapes=[pltpu.VMEM((BX, BY, BZ), F32), DMA((CHUNKS,))],
        compiler_params=pltpu.CompilerParams(vmem_limit_bytes=24 * 2**20),
        name="combine",
    )(*outs, prestress, state_var, normal_a)


def solution(mesh):
    block = P("gx", "gy", "gz")
    fault = P(("gx", "gy"), "gz")
    return jax.shard_map(
        per_device,
        mesh=mesh,
        in_specs=(block, block, fault, fault, fault),
        out_specs=(block, fault),
        check_vma=False,
    )
```

```python
import functools

import jax
import jax.numpy as jnp
from jax import lax
from jax.experimental import pallas as pl
from jax.experimental.pallas import tpu as pltpu
from jax.sharding import PartitionSpec as P

MESH = pl.DeviceIdType.MESH
F32 = jnp.float32
BF16 = jnp.bfloat16
BX, BY, BZ = 64, 64, 128
LOW = 8
PITCH = BY + LOW
ROWS = (BX + 4) * PITCH + LOW
FACE = PITCH + BY
TILES = BY // 8
STRIPS = BX // 8
CHUNKS = 8
SLOTS = 32
GROUP = 4
UNROLL = 8


def two_sum(a, b):
    s = a + b
    t = s - a
    return s, (a - (s - t)) + (b - t)


def split(a):
    t = a * 4097.0
    high = t - (t - a)
    return high, a - high


def two_prod(a, b):
    p = a * b
    ah, al = split(a)
    bh, bl = split(b)
    return p, ((ah * bh - p) + ah * bl + al * bh) + al * bl


def norm(h, l):
    s = h + l
    return s, l - (s - h)


def dd_sub(a, b):
    s, e = two_sum(a[0], -b[0])
    return norm(s, e + (a[1] - b[1]))


def dd_mul(a, b):
    p, e = two_prod(a[0], b[0])
    return norm(p, e + (a[0] * b[1] + a[1] * b[0]))


def dd_div(a, b):
    q = a[0] / b[0]
    p, e = two_prod(q, b[0])
    r = ((a[0] - p) - e) + (a[1] - q * b[1])
    return norm(q, r / b[0])


def lane_sum(v):
    total = jnp.sum(v, axis=1, keepdims=True)
    big = total * 4096.0
    high = (v + big) - big
    low = v - high
    return norm(jnp.sum(high, axis=1, keepdims=True), jnp.sum(low, axis=1, keepdims=True))


def coefficients(mu):
    theta = dd_div(mu[1], mu[0])
    s = [None] + [dd_sub(mu[j + 1], dd_mul(theta, mu[j])) for j in range(1, 5)]
    a1 = dd_sub(dd_div(s[2], s[1]), theta)
    b1 = dd_div(s[1], mu[0])

    def second(j):
        return dd_sub(dd_sub(s[j + 1], dd_mul(a1, s[j])), dd_mul(b1, mu[j]))

    t2, t3 = second(2), second(3)
    a2 = dd_sub(dd_sub(dd_div(t3, t2), a1), theta)
    b2 = dd_div(t2, s[1])
    a0, a1, a2, b1, b2 = theta[0], a1[0], a2[0], b1[0], b2[0]
    d0 = a0
    d1 = a1 - b1 / d0
    d2 = a2 - b2 / d1
    y2 = 1.0 / (d0 * d1 * d2)
    y1 = (-1.0 / d0 - b2 * y2) / d1
    y0 = (1.0 - b1 * y1) / d0
    c2 = y2
    c1 = y1 - (a0 + a1) * y2
    c0 = y0 - a0 * y1 + (a0 * a1 - b1) * y2
    return c0, c1, c2


def spot_of(x, y=0):
    return pl.multiple_of((x + 2) * PITCH + LOW, 8) + y


def zero_edges(w):
    z8 = jnp.zeros((8, BZ), F32)
    for t in range(2 * PITCH // 8):
        w[pl.ds(8 * t, 8), :] = z8
        w[pl.ds(ROWS - LOW - 2 * PITCH + LOW + 8 * t, 8), :] = z8

    def body(x, carry):
        w[pl.ds(pl.multiple_of((x + 2) * PITCH, 8), 8), :] = z8
        return carry

    lax.fori_loop(0, BX + 1, body, 0, unroll=5)


def krylov(
    load, stiff, w0, w1, w2, coef, fault_sum,
    bv, sv, minv, ypack, zpack, edge, trac,
    hx, hy, hz, fault, part_a, part_b, band, even, odd,
    in_sem, xs_sem, xr_sem, ys_sem, yr_sem, zs_sem, zr_sem, fs_sem, fr_sem, rs_sem, rr_sem, token,
):
    gx, gy, gz = (lax.axis_index(a) for a in ("gx", "gy", "gz"))
    nx, ny, nz = (lax.axis_size(a) for a in ("gx", "gy", "gz"))
    group = ny * nz
    spot = gy * nz + gz
    lane = lax.broadcasted_iota(jnp.int32, (8, BZ), 1)
    row = lax.broadcasted_iota(jnp.int32, (8, BZ), 0)
    place = (lane + 2) & 3
    halo_here = (place >> 1) == (1 - gz)
    packs = (BX // SLOTS) * TILES

    step = BX // CHUNKS
    loads = []
    order = [0, CHUNKS - 1] + list(range(1, CHUNKS - 1))
    for i in order:
        part = pl.ds(i * step, step)
        a = pltpu.make_async_copy(load.at[part], bv.at[part], in_sem.at[0, i])
        b = pltpu.make_async_copy(stiff.at[part], sv.at[part], in_sem.at[1, i])
        a.start()
        b.start()
        loads.append((a, b))

    barrier = pltpu.get_barrier_semaphore()
    peers = []
    for r in range(1, group):
        other = lax.rem(spot + r, group)
        peers.append((gx, other // nz, lax.rem(other, nz)))
    cross = [(lax.rem(gx + r, nx), gy, gz) for r in range(1, nx)]
    has_x = (gx > 0, gx < nx - 1)
    has_y = (gy > 0, gy < ny - 1)

    def one(flag):
        return jnp.where(flag, 1, 0)

    def sides(distance):
        return ((gx >= distance, gx - distance), (gx + distance < nx, gx + distance))

    def signal(k, distance):
        for side, (there, target) in enumerate(sides(distance)):
            @pl.when(there)
            def _(side=side, target=target):
                pl.semaphore_signal(
                    token.at[k, 1 - side], inc=1, device_id=(target, gy, gz), device_id_type=MESH
                )

    def await_signals(k, distance):
        for side, (there, _) in enumerate(sides(distance)):
            @pl.when(there)
            def _(side=side):
                pl.semaphore_wait(token.at[k, side], 1)

    for there, target in sides(1):
        @pl.when(there)
        def _(target=target):
            pl.semaphore_signal(barrier, inc=1, device_id=(target, gy, gz), device_id_type=MESH)
    for side in range(2):
        @pl.when(has_y[side])
        def _(side=side):
            pl.semaphore_signal(
                barrier, inc=1, device_id=(gx, gy + 2 * side - 1, gz), device_id_type=MESH
            )
    pl.semaphore_signal(barrier, inc=1, device_id=(gx, gy, 1 - gz), device_id_type=MESH)

    for w in (w0, w1, w2):
        zero_edges(w)

    def remote(src, dst, send, recv, device):
        return pltpu.make_async_remote_copy(
            src_ref=src, dst_ref=dst, send_sem=send, recv_sem=recv,
            device_id=device, device_id_type=MESH,
        )

    def x_copies(w, k, side):
        plane = 0 if side == 0 else BX - 2
        device = (gx - 1 if side == 0 else gx + 1, gy, gz)
        if k < 2:
            return [
                remote(
                    w.at[pl.ds(spot_of(plane), FACE), :], hx.at[k, 1 - side],
                    xs_sem.at[k, side, 0], xr_sem.at[k, 1 - side, 0], device,
                )
            ]
        half = BY // 2
        return [
            remote(
                w.at[pl.ds(spot_of(plane + n, side * half), half), :],
                hx.at[k, 1 - side, pl.ds(n * PITCH + side * half, half), :],
                xs_sem.at[k, side, n], xr_sem.at[k, 1 - side, n], device,
            )
            for n in range(2)
        ]

    def y_copy(k, side):
        strips = pl.ds(0, BX) if k < 2 else pl.ds(side * (BX // 2), BX // 2)
        return remote(
            ypack.at[k, side, :, strips, :], hy.at[k, 1 - side, :, strips, :],
            ys_sem.at[k, side], yr_sem.at[k, 1 - side],
            (gx, gy - 1 if side == 0 else gy + 1, gz),
        )

    def z_copy(k):
        return remote(zpack.at[k], hz.at[k], zs_sem.at[k], zr_sem.at[k], (gx, gy, 1 - gz))

    near_fault = (gy == ny // 2 - 1) | (gy == ny // 2)
    source = gy - (ny // 2 - 1)
    low_side = jnp.where(gy == ny // 2, 1.0, 0.0)
    high_side = jnp.where(gy == ny // 2 - 1, 1.0, 0.0)
    own_rows = BX // ny

    def fault_copy(k, r):
        owner = lax.rem(gy + r, ny)
        return remote(
            trac.at[k, pl.ds(owner * own_rows, own_rows), :], fault.at[source, k],
            fs_sem.at[k, r - 1], fr_sem.at[source, k], (gx, owner, gz),
        )

    def send_x(w, k):
        for side in range(2):
            @pl.when(has_x[side])
            def _(side=side):
                for copy in x_copies(w, k, side):
                    copy.start()

    def send_fault(k):
        @pl.when(near_fault)
        def _():
            for r in range(1, ny):
                fault_copy(k, r).start()
            for i in range(own_rows // 8):
                fault[source, k, pl.ds(8 * i, 8), :] = trac[
                    k, pl.ds(pl.multiple_of(gy * own_rows + 8 * i, 8), 8), :
                ]

    def exchange(w, k):
        for j in range(STRIPS):
            strip = []
            for n, y in enumerate((0, 1, BY - 2, BY - 1)):
                v = w[pl.ds(spot_of(8 * j, y), 8, stride=PITCH), :]
                ypack[k, n // 2, n % 2, pl.ds(8 * j, 8), :] = v
                strip.append(v)
            term = low_side * (27.0 * strip[0] - strip[1]) + high_side * (strip[2] - 27.0 * strip[3])
            trac[k, pl.ds(8 * j, 8), :] = term / 24.0
        for side in range(2):
            @pl.when(has_y[side])
            def _(side=side):
                y_copy(k, side).start()

        for half in range(BX // SLOTS):
            def pack(q, acc, half=half):
                mask = ((lane + 2 - 4 * q) & (BZ - 1)) < 4
                return tuple(
                    jnp.where(
                        mask,
                        pltpu.roll(w[pl.ds(spot_of(half * SLOTS + q, 8 * t), 8), :], 4 * q, 1),
                        acc[t],
                    )
                    for t in range(TILES)
                )

            packed = lax.fori_loop(0, SLOTS, pack, (zero,) * TILES, unroll=2 * UNROLL)
            for t in range(TILES):
                zpack[k, half * TILES + t] = packed[t]

        z_copy(k).start()
        if k == 2:
            for n in range(3):
                send_fault(n)

    at_row = lax.rem(lax.broadcasted_iota(jnp.int32, (3 * BZ, BZ), 0), BZ)
    gap = jnp.abs(at_row - lax.broadcasted_iota(jnp.int32, (3 * BZ, BZ), 1))
    band[...] = jnp.where(gap == 1, 16.0, jnp.where(gap == 2, -1.0, 0.0)).astype(BF16)

    zero = jnp.zeros((8, BZ), F32)
    mu0 = zero
    for n, i in enumerate(order):
        first_wait, second_wait = loads[n]
        first_wait.wait()
        second_wait.wait()

        def start_plane(x, acc):
            for t in range(TILES):
                at = pl.ds(8 * t, 8)
                b = bv[x, at, :]
                inverse = 1.0 / (7.5 + sv[x, at, :])
                w = b * inverse
                w0[pl.ds(spot_of(x, 8 * t), 8), :] = w
                minv[pl.ds(pl.multiple_of(x * BY, 8) + 8 * t, 8), :] = inverse * (1.0 / 12.0)
                acc = acc + b * w
            return acc

        mu0 = lax.fori_loop(i * step, (i + 1) * step, start_plane, mu0, unroll=min(step, UNROLL))
        if n == 1:
            pl.semaphore_wait(
                barrier,
                1 + one(has_x[0]) + one(has_x[1]) + one(has_y[0]) + one(has_y[1]),
            )
            send_x(w0, 0)

    def edge_terms(d):
        near = jnp.where(place == 1, pltpu.roll(d, BZ - 1, 1), pltpu.roll(d, 1, 1))
        near = jnp.where((place == 1) | (place == 2), near, 0.0)
        return 16.0 * near - jnp.where(place < 2, pltpu.roll(d, BZ - 2, 1), pltpu.roll(d, 2, 1))

    def along_z(w, x):
        c = w[pl.ds(spot_of(x), GROUP * PITCH), :]
        high = c.astype(BF16)
        rest = c - high.astype(F32)
        middle = rest.astype(BF16)
        low = (rest - middle.astype(F32)).astype(BF16)
        return jnp.dot(
            jnp.concatenate([high, middle, low], axis=1), band[...], preferred_element_type=F32
        )

    def bulk(w, out, k, init, with_halo):
        if with_halo:
            z_copy(k).wait_recv()
            for i in range(packs):
                edge[i] = edge_terms(jnp.where(halo_here, hz[k, i], 0.0))
        mask = ((lane + 2) & (BZ - 1)) < 4

        def group(g, zz, acc):
            for t in range(TILES):
                def at(p, dy):
                    return w[pl.ds(spot_of(g * GROUP, 8 * t) + (p * PITCH + dy), 8), :]

                line = [at(p, 0) for p in range(-2, GROUP + 2)]
                for p in range(GROUP):
                    x = g * GROUP + p
                    near = (line[p + 3] + line[p + 1]) + (at(p, 1) + at(p, -1))
                    far = (line[p + 4] + line[p]) + (at(p, 2) + at(p, -2))
                    n = (16.0 * near - far) + zz[pl.ds(p * PITCH + 8 * t, 8), :]
                    if with_halo:
                        turn = lax.rem(BZ - 4 * lax.rem(x, SLOTS), BZ)
                        e = pltpu.roll(edge[(x // SLOTS) * TILES + t], turn, 1)
                        n = n + jnp.where(mask, e, 0.0)
                    acc = out(x, t, line[p + 2], n, acc)
            return acc

        groups = BX // GROUP
        even[...] = along_z(w, 0)

        def pair(i, acc):
            odd[...] = along_z(w, (2 * i + 1) * GROUP)
            acc = group(2 * i, even, acc)
            even[...] = along_z(w, jnp.minimum(2 * i + 2, groups - 1) * GROUP)
            return group(2 * i + 1, odd, acc)

        return lax.fori_loop(0, groups // 2, pair, init)

    def fixes(k, apply_x, apply_y):
        whole = k < 2
        for side in range(2):
            @pl.when(has_y[side])
            def _(side=side):
                y_copy(k, 1 - side).wait_recv()
                inner, outer = (1, 0) if side == 0 else (0, 1)
                first, second = (0, 1) if side == 0 else (BY - 1, BY - 2)
                span = range(STRIPS)
                if not whole:
                    span = range((1 - side) * STRIPS // 2, (2 - side) * STRIPS // 2)
                for j in span:
                    at = pl.ds(8 * j, 8)
                    close = hy[k, side, inner, at, :]
                    apply_y(j, first, 16.0 * close - hy[k, side, outer, at, :])
                    apply_y(j, second, -close)
        for side in range(2):
            @pl.when(has_x[side])
            def _(side=side):
                for copy in x_copies(w0, k, 1 - side):
                    copy.wait_recv()
                inner, outer = (1, 0) if side == 0 else (0, 1)
                first, second = (0, 1) if side == 0 else (BX - 1, BX - 2)
                span = range(TILES)
                if not whole:
                    span = range((1 - side) * TILES // 2, (2 - side) * TILES // 2)
                for t in span:
                    close = hx[k, side, pl.ds(inner * PITCH + 8 * t, 8), :]
                    distant = hx[k, side, pl.ds(outer * PITCH + 8 * t, 8), :]
                    apply_x(first, t, 16.0 * close - distant)
                    apply_x(second, t, -close)

    def basis_step(w, new, k, moments, init):
        exchange(w, k)

        def out(x, t, c, n, acc):
            new[pl.ds(spot_of(x, 8 * t), 8), :] = (
                c - minv[pl.ds(pl.multiple_of(x * BY, 8) + 8 * t, 8), :] * n
            )
            return moments(x, t, c, acc)

        sums = bulk(w, out, k, init, True)

        def apply_x(x, t, n):
            at = pl.ds(spot_of(x, 8 * t), 8)
            new[at, :] = new[at, :] - minv[pl.ds(x * BY + 8 * t, 8), :] * n

        def apply_y(j, y, n):
            at = pl.ds(spot_of(8 * j, y), 8, stride=PITCH)
            new[at, :] = new[at, :] - minv[pl.ds(8 * j * BY + y, 8, stride=BY), :] * n

        fixes(k, apply_x, apply_y)
        if k > 0:
            await_signals(k - 1, 1 << k)
        send_x(new, k + 1)
        signal(k, 2 << k)
        return sums

    basis_step(w0, w1, 0, lambda x, t, c, acc: acc, 0)

    def first_moments(x, t, c, acc):
        at = pl.ds(8 * t, 8)
        return (acc[0] + bv[x, at, :] * c, acc[1] + ((7.5 + sv[x, at, :]) * c) * c)

    mu1, mu2 = basis_step(w1, w2, 1, first_moments, (zero, zero))

    exchange(w2, 2)

    def last(x, t, c, n, acc):
        d = (7.5 + sv[x, pl.ds(8 * t, 8), :]) * c
        return (
            acc[0] + d * w1[pl.ds(spot_of(x, 8 * t), 8), :],
            acc[1] + d * c,
            acc[2] + c * (d - n * (1.0 / 12.0)),
        )

    mu3, mu4, mu5 = bulk(w2, last, 2, (zero, zero, zero), False)
    part_a[0] = zero

    def cross_x(x, t, n):
        part_a[0] = part_a[0] + w2[pl.ds(spot_of(x, 8 * t), 8), :] * n

    def cross_y(j, y, n):
        part_a[0] = part_a[0] + w2[pl.ds(spot_of(8 * j, y), 8, stride=PITCH), :] * n

    z_copy(2).wait_recv()
    crossing = zero
    for i in range(packs):
        crossing = crossing + zpack[2, i] * edge_terms(jnp.where(halo_here, hz[2, i], 0.0))
    fixes(2, cross_x, cross_y)
    mu5 = mu5 - (2.0 * part_a[0] + crossing) * (1.0 / 12.0)
    await_signals(1, 4)
    signal(2, 8)

    local = zero
    for j, m in enumerate((mu0, mu1, mu2, mu3, mu4, mu5)):
        local = jnp.where(row == j, jnp.sum(m, axis=0, keepdims=True), local)

    def reduce(value, buf, s, devices):
        buf[0] = value
        copies = [
            remote(buf.at[0], buf.at[r + 1], rs_sem.at[s, r], rr_sem.at[s, r], device)
            for r, device in enumerate(devices)
        ]
        for c in copies:
            c.start()
        for c in copies:
            c.wait_recv()
        total = value
        for r in range(len(devices)):
            total = total + buf[r + 1]
        return total, copies

    total, sent_a = reduce(local, part_a, 0, peers)
    await_signals(2, 8)
    total, sent_b = reduce(total, part_b, 1, cross)

    mu = []
    for j in range(6):
        mu.append(lane_sum(jnp.broadcast_to(total[j : j + 1, :], (8, BZ))))
    for j, c in enumerate(coefficients(mu)):
        coef[j] = jnp.broadcast_to(c, (8, BZ))

    for k in range(3):
        for s in range(2):
            @pl.when(gy != ny // 2 - 1 + s)
            def _(k=k, s=s):
                remote(
                    trac.at[k, pl.ds(0, own_rows), :], fault.at[s, k],
                    fs_sem.at[k, 0], fr_sem.at[s, k], (gx, gy, 1 - gz),
                ).wait_recv()
    for k in range(3):
        for i in range(own_rows // 8):
            at = pl.ds(8 * i, 8)
            fault_sum[k, at, :] = fault[0, k, at, :] + fault[1, k, at, :]

    for c in sent_a + sent_b:
        c.wait_send()
    for k in range(3):
        for side in range(2):
            @pl.when(has_x[side])
            def _(k=k, side=side):
                for copy in x_copies(w0, k, side):
                    copy.wait_send()
            @pl.when(has_y[side])
            def _(k=k, side=side):
                y_copy(k, side).wait_send()
        z_copy(k).wait_send()

        @pl.when(near_fault)
        def _(k=k):
            for r in range(1, ny):
                fault_copy(k, r).wait_send()


def combine(w0, w1, w2, coef, fault_sum, prestress, state, normal, u, slip, buf, sem):
    c0, c1, c2 = coef[0], coef[1], coef[2]
    step = BX // CHUNKS
    copies = []
    for i in range(CHUNKS):
        def plane(x, carry):
            for t in range(TILES):
                at = pl.ds(spot_of(x, 8 * t), 8)
                buf[x, pl.ds(8 * t, 8), :] = (c0 * w0[at, :] + c1 * w1[at, :]) + c2 * w2[at, :]
            return carry

        lax.fori_loop(i * step, (i + 1) * step, plane, 0)
        part = pl.ds(i * step, step)
        copy = pltpu.make_async_copy(buf.at[part], u.at[part], sem.at[i])
        copy.start()
        copies.append(copy)
    for i in range(slip.shape[0] // 8):
        at = pl.ds(8 * i, 8)
        traction = (c0 * fault_sum[0, at, :] + c1 * fault_sum[1, at, :]) + c2 * fault_sum[2, at, :]
        x = (prestress[at, :] + 2.0 * traction) / normal[at, :]
        half = 0.6931471805599453
        large = jnp.exp(x - half) - jnp.exp(-x - half)
        q = x * x
        small = x * (1.0 + q * (1 / 6 + q * (1 / 120 + q * (1 / 5040 + q * (1 / 362880 + q / 39916800)))))
        sinh = jnp.where(jnp.abs(x) < 1.0, small, large)
        slip[at, :] = jnp.exp(-state[at, :]) * sinh
    for copy in copies:
        copy.wait()


def per_device(load, stiffness, prestress, state_var, normal_a):
    vmem = pl.BlockSpec(memory_space=pltpu.VMEM)
    hbm = pl.BlockSpec(memory_space=pl.ANY)
    ny = lax.axis_size("gy")
    own = BX // ny
    group = ny * lax.axis_size("gz")
    nx = lax.axis_size("gx")
    big = (ROWS, BZ)
    packs = (BX // SLOTS) * TILES
    DMA = pltpu.SemaphoreType.DMA
    outs = pl.pallas_call(
        krylov,
        out_shape=[
            pltpu.VMEM(big, F32), pltpu.VMEM(big, F32), pltpu.VMEM(big, F32),
            pltpu.VMEM((3, 8, BZ), F32), pltpu.VMEM((3, own, BZ), F32),
        ],
        in_specs=[pl.BlockSpec(memory_space=pltpu.HBM)] * 2,
        out_specs=[vmem] * 5,
        scratch_shapes=[
            pltpu.VMEM((BX, BY, BZ), F32),
            pltpu.VMEM((BX, BY, BZ), F32),
            pltpu.VMEM((BX * BY, BZ), F32),
            pltpu.VMEM((3, 2, 2, BX, BZ), F32),
            pltpu.VMEM((3, packs, 8, BZ), F32),
            pltpu.VMEM((packs, 8, BZ), F32),
            pltpu.VMEM((3, BX, BZ), F32),
            pltpu.VMEM((3, 2, FACE, BZ), F32),
            pltpu.VMEM((3, 2, 2, BX, BZ), F32),
            pltpu.VMEM((3, packs, 8, BZ), F32),
            pltpu.VMEM((2, 3, own, BZ), F32),
            pltpu.VMEM((group, 8, BZ), F32),
            pltpu.VMEM((nx, 8, BZ), F32),
            pltpu.VMEM((3 * BZ, BZ), BF16),
            pltpu.VMEM((GROUP * PITCH, BZ), F32),
            pltpu.VMEM((GROUP * PITCH, BZ), F32),
            DMA((2, CHUNKS)),
            DMA((3, 2, 2)), DMA((3, 2, 2)), DMA((3, 2)), DMA((3, 2)), DMA((3,)), DMA((3,)),
            DMA((3, ny - 1)), DMA((2, 3)),
            DMA((2, nx - 1)), DMA((2, nx - 1)),
            pltpu.SemaphoreType.REGULAR((3, 2)),
        ],
        compiler_params=pltpu.CompilerParams(
            collective_id=0, has_side_effects=True, vmem_limit_bytes=55 * 2**20
        ),
        name="krylov",
    )(load, stiffness)
    return pl.pallas_call(
        combine,
        out_shape=[
            jax.ShapeDtypeStruct(load.shape, F32),
            jax.ShapeDtypeStruct(prestress.shape, F32),
        ],
        in_specs=[vmem] * 8,
        out_specs=[hbm, vmem],
        scratch_shapes=[pltpu.VMEM((BX, BY, BZ), F32), DMA((CHUNKS,))],
        compiler_params=pltpu.CompilerParams(vmem_limit_bytes=24 * 2**20),
        name="combine",
    )(*outs, prestress, state_var, normal_a)


def solution(mesh):
    block = P("gx", "gy", "gz")
    fault = P(("gx", "gy"), "gz")
    return jax.shard_map(
        per_device,
        mesh=mesh,
        in_specs=(block, block, fault, fault, fault),
        out_specs=(block, fault),
        check_vma=False,
    )
```

```python
import functools

import jax
import jax.numpy as jnp
from jax import lax
from jax.experimental import pallas as pl
from jax.experimental.pallas import tpu as pltpu
from jax.sharding import PartitionSpec as P

MESH = pl.DeviceIdType.MESH
F32 = jnp.float32
BF16 = jnp.bfloat16
BX, BY, BZ = 64, 64, 128
LOW = 8
PITCH = BY + LOW
ROWS = (BX + 4) * PITCH + LOW
TILES = BY // 8
STRIPS = BX // 8
CHUNKS = 8
INNER = 6
SLOTS = 32
GROUP = 4
UNROLL = 8


def two_sum(a, b):
    s = a + b
    t = s - a
    return s, (a - (s - t)) + (b - t)


def split(a):
    t = a * 4097.0
    high = t - (t - a)
    return high, a - high


def two_prod(a, b):
    p = a * b
    ah, al = split(a)
    bh, bl = split(b)
    return p, ((ah * bh - p) + ah * bl + al * bh) + al * bl


def norm(h, l):
    s = h + l
    return s, l - (s - h)


def dd_sub(a, b):
    s, e = two_sum(a[0], -b[0])
    return norm(s, e + (a[1] - b[1]))


def dd_mul(a, b):
    p, e = two_prod(a[0], b[0])
    return norm(p, e + (a[0] * b[1] + a[1] * b[0]))


def dd_div(a, b):
    q = a[0] / b[0]
    p, e = two_prod(q, b[0])
    r = ((a[0] - p) - e) + (a[1] - q * b[1])
    return norm(q, r / b[0])


def coefficients(mu):
    theta = dd_div(mu[1], mu[0])
    s = [None] + [dd_sub(mu[j + 1], dd_mul(theta, mu[j])) for j in range(1, 5)]
    a1 = dd_sub(dd_div(s[2], s[1]), theta)
    b1 = dd_div(s[1], mu[0])

    def second(j):
        return dd_sub(dd_sub(s[j + 1], dd_mul(a1, s[j])), dd_mul(b1, mu[j]))

    t2, t3 = second(2), second(3)
    a2 = dd_sub(dd_sub(dd_div(t3, t2), a1), theta)
    b2 = dd_div(t2, s[1])
    a0, a1, a2, b1, b2 = theta[0], a1[0], a2[0], b1[0], b2[0]
    d0 = a0
    d1 = a1 - b1 / d0
    d2 = a2 - b2 / d1
    y2 = 1.0 / (d0 * d1 * d2)
    y1 = (-1.0 / d0 - b2 * y2) / d1
    y0 = (1.0 - b1 * y1) / d0
    c2 = y2
    c1 = y1 - (a0 + a1) * y2
    c0 = y0 - a0 * y1 + (a0 * a1 - b1) * y2
    return c0, c1, c2


def spot_of(x, y=0):
    return pl.multiple_of((x + 2) * PITCH + LOW, 8) + y


def zero_edges(w):
    z8 = jnp.zeros((8, BZ), F32)
    for t in range(2 * PITCH // 8):
        w[pl.ds(8 * t, 8), :] = z8
        w[pl.ds(ROWS - LOW - 2 * PITCH + LOW + 8 * t, 8), :] = z8

    def body(x, carry):
        w[pl.ds(pl.multiple_of((x + 2) * PITCH, 8), 8), :] = z8
        return carry

    lax.fori_loop(0, BX + 1, body, 0, unroll=5)


def krylov(
    load, stiff, w0, w1, w2, coef, fault_sum,
    bs, minv, ypack, zpack, edge, trac,
    hx, hy, hz, fault, part_a, part_b, cross_sum, band, even, odd,
    in_sem, xs_sem, xr_sem, ys_sem, yr_sem, zs_sem, zr_sem, fs_sem, fr_sem, rs_sem, rr_sem, token,
):
    gx, gy, gz = (lax.axis_index(a) for a in ("gx", "gy", "gz"))
    nx, ny, nz = (lax.axis_size(a) for a in ("gx", "gy", "gz"))
    group = ny * nz
    spot = gy * nz + gz
    lane = lax.broadcasted_iota(jnp.int32, (8, BZ), 1)
    row = lax.broadcasted_iota(jnp.int32, (8, BZ), 0)
    place = (lane + 2) & 3
    halo_here = (place >> 1) == (1 - gz)
    packs = (BX // SLOTS) * TILES
    zero = jnp.zeros((8, BZ), F32)

    regions = [
        (0, 2, 0, BY), (BX - 2, BX, 0, BY), (2, BX - 2, 0, 8), (2, BX - 2, BY - 8, BY)
    ]
    cuts = [2 + (BX - 4) * i // INNER for i in range(INNER + 1)]
    regions += [(lo, hi, 8, BY - 8) for lo, hi in zip(cuts, cuts[1:])]
    for n, (xa, xb, ya, yb) in enumerate(regions):
        part = (pl.ds(xa, xb - xa), pl.ds(ya, yb - ya))
        for i, source in enumerate((load, stiff)):
            pltpu.make_async_copy(source.at[part], bs.at[(i,) + part], in_sem.at[n]).start()

    barrier = pltpu.get_barrier_semaphore()
    peers = []
    for r in range(1, group):
        other = lax.rem(spot + r, group)
        peers.append((gx, other // nz, lax.rem(other, nz)))
    cross = [(lax.rem(gx + r, nx), gy, gz) for r in range(1, nx)]
    has_x = (gx > 0, gx < nx - 1)
    has_y = (gy > 0, gy < ny - 1)

    def one(flag):
        return jnp.where(flag, 1, 0)

    def sides(distance):
        return ((gx >= distance, gx - distance), (gx + distance < nx, gx + distance))

    def signal(k, distance):
        for side, (there, target) in enumerate(sides(distance)):
            @pl.when(there)
            def _(side=side, target=target):
                pl.semaphore_signal(
                    token.at[k, 1 - side], inc=1, device_id=(target, gy, gz), device_id_type=MESH
                )

    def await_signals(k, distance):
        for side, (there, _) in enumerate(sides(distance)):
            @pl.when(there)
            def _(side=side):
                pl.semaphore_wait(token.at[k, side], 1)

    for there, target in sides(1):
        @pl.when(there)
        def _(target=target):
            pl.semaphore_signal(barrier, inc=1, device_id=(target, gy, gz), device_id_type=MESH)
    for side in range(2):
        @pl.when(has_y[side])
        def _(side=side):
            pl.semaphore_signal(
                barrier, inc=1, device_id=(gx, gy + 2 * side - 1, gz), device_id_type=MESH
            )
    pl.semaphore_signal(barrier, inc=1, device_id=(gx, gy, 1 - gz), device_id_type=MESH)

    for w in (w0, w1, w2):
        zero_edges(w)

    at_row = lax.rem(lax.broadcasted_iota(jnp.int32, (3 * BZ, BZ), 0), BZ)
    gap = jnp.abs(at_row - lax.broadcasted_iota(jnp.int32, (3 * BZ, BZ), 1))
    band[...] = jnp.where(gap == 1, 16.0, jnp.where(gap == 2, -1.0, 0.0)).astype(BF16)

    def remote(src, dst, send, recv, device):
        return pltpu.make_async_remote_copy(
            src_ref=src, dst_ref=dst, send_sem=send, recv_sem=recv,
            device_id=device, device_id_type=MESH,
        )

    partner = (gx, gy, 1 - gz)
    half = BY // 2

    def x_sent(k, side, h):
        return k < 2 or h == side

    def x_send(w, k, side, h):
        device = (gx - 1 if side == 0 else gx + 1, gy, gz)
        for n in range(2):
            plane = n if side == 0 else BX - 2 + n
            remote(
                w.at[pl.ds(spot_of(plane, h * half), half), :], hx.at[k, 1 - side, h, n],
                xs_sem.at[k, side], xr_sem.at[k, 1 - side, h], device,
            ).start()

    def x_arrived(k, side, h):
        land = hx.at[k, side, h]
        remote(land, land, xs_sem.at[k, side], xr_sem.at[k, side, h], partner).wait_recv()

    def y_copy(k, side):
        strips = pl.ds(0, BX) if k < 2 else pl.ds(side * (BX // 2), BX // 2)
        return remote(
            ypack.at[k, side, :, strips, :], hy.at[k, 1 - side, :, strips, :],
            ys_sem.at[k, side], yr_sem.at[k, 1 - side],
            (gx, gy - 1 if side == 0 else gy + 1, gz),
        )

    def z_copy(k):
        return remote(zpack.at[k], hz.at[k], zs_sem.at[0], zr_sem.at[k], partner)

    near_fault = (gy == ny // 2 - 1) | (gy == ny // 2)
    source = gy - (ny // 2 - 1)
    low_side = jnp.where(gy == ny // 2, 1.0, 0.0)
    high_side = jnp.where(gy == ny // 2 - 1, 1.0, 0.0)
    own_rows = BX // ny

    def send_fault():
        @pl.when(near_fault)
        def _():
            for r in range(1, ny):
                owner = lax.rem(gy + r, ny)
                remote(
                    trac.at[:, pl.ds(pl.multiple_of(owner * own_rows, 8), own_rows), :],
                    fault.at[source], fs_sem.at[0], fr_sem.at[source], (gx, owner, gz),
                ).start()
            for k in range(3):
                for i in range(own_rows // 8):
                    fault[source, k, pl.ds(8 * i, 8), :] = trac[
                        k, pl.ds(pl.multiple_of(gy * own_rows + 8 * i, 8), 8), :
                    ]

    def send_y(w, k):
        for j in range(STRIPS):
            strip = []
            for n, y in enumerate((0, 1, BY - 2, BY - 1)):
                v = w[pl.ds(spot_of(8 * j, y), 8, stride=PITCH), :]
                ypack[k, n // 2, n % 2, pl.ds(8 * j, 8), :] = v
                strip.append(v)
            term = low_side * (27.0 * strip[0] - strip[1]) + high_side * (strip[2] - 27.0 * strip[3])
            trac[k, pl.ds(8 * j, 8), :] = term / 24.0
        for side in range(2):
            @pl.when(has_y[side])
            def _(side=side):
                y_copy(k, side).start()

    def send_z(w, k):
        for block in range(BX // SLOTS):
            def pack(q, acc, block=block):
                mask = ((lane + 2 - 4 * q) & (BZ - 1)) < 4
                return tuple(
                    jnp.where(
                        mask,
                        pltpu.roll(w[pl.ds(spot_of(block * SLOTS + q, 8 * t), 8), :], 4 * q, 1),
                        acc[t],
                    )
                    for t in range(TILES)
                )

            packed = lax.fori_loop(0, SLOTS, pack, (zero,) * TILES, unroll=2 * UNROLL)
            for t in range(TILES):
                zpack[k, block * TILES + t] = packed[t]
        z_copy(k).start()

    mu0 = zero
    for n, (xa, xb, ya, yb) in enumerate(regions):
        part = (slice(None), pl.ds(xa, xb - xa), pl.ds(ya, yb - ya))
        pltpu.make_async_copy(bs.at[part], bs.at[part], in_sem.at[n]).wait()

        def start_plane(x, acc):
            for t in range(ya // 8, yb // 8):
                at = pl.ds(8 * t, 8)
                b = bs[0, x, at, :]
                inverse = 1.0 / (7.5 + bs[1, x, at, :])
                w = b * inverse
                w0[pl.ds(spot_of(x, 8 * t), 8), :] = w
                minv[pl.ds(pl.multiple_of(x * BY, 8) + 8 * t, 8), :] = inverse * (1.0 / 12.0)
                acc = acc + b * w
            return acc

        count = xb - xa
        tiles = (yb - ya) // 8
        unroll = max(u for u in range(1, count + 1) if count % u == 0 and u * tiles <= 60 or u == 1)
        mu0 = lax.fori_loop(xa, xb, start_plane, mu0, unroll=unroll)
        if n == 1:
            pl.semaphore_wait(
                barrier,
                1 + one(has_x[0]) + one(has_x[1]) + one(has_y[0]) + one(has_y[1]),
            )
            for side in range(2):
                @pl.when(has_x[side])
                def _(side=side):
                    for h in range(2):
                        x_send(w0, 0, side, h)
        if n == 3:
            send_y(w0, 0)
    send_z(w0, 0)

    def edge_terms(d):
        near = jnp.where(place == 1, pltpu.roll(d, BZ - 1, 1), pltpu.roll(d, 1, 1))
        near = jnp.where((place == 1) | (place == 2), near, 0.0)
        return 16.0 * near - jnp.where(place < 2, pltpu.roll(d, BZ - 2, 1), pltpu.roll(d, 2, 1))

    def along_z(w, x):
        c = w[pl.ds(spot_of(x), GROUP * PITCH), :]
        high = c.astype(BF16)
        rest = c - high.astype(F32)
        middle = rest.astype(BF16)
        low = (rest - middle.astype(F32)).astype(BF16)
        return jnp.dot(
            jnp.concatenate([high, middle, low], axis=1), band[...], preferred_element_type=F32
        )

    def bulk(w, out, k, init, with_halo):
        if with_halo:
            z_copy(k).wait_recv()
            for i in range(packs):
                edge[i] = edge_terms(jnp.where(halo_here, hz[k, i], 0.0))
        mask = ((lane + 2) & (BZ - 1)) < 4

        def group(g, zz, acc):
            for t in range(TILES):
                def at(p, dy):
                    return w[pl.ds(spot_of(g * GROUP, 8 * t) + (p * PITCH + dy), 8), :]

                line = [at(p, 0) for p in range(-2, GROUP + 2)]
                for p in range(GROUP):
                    x = g * GROUP + p
                    near = (line[p + 3] + line[p + 1]) + (at(p, 1) + at(p, -1))
                    far = (line[p + 4] + line[p]) + (at(p, 2) + at(p, -2))
                    n = (16.0 * near - far) + zz[pl.ds(p * PITCH + 8 * t, 8), :]
                    if with_halo:
                        turn = lax.rem(BZ - 4 * lax.rem(x, SLOTS), BZ)
                        e = pltpu.roll(edge[(x // SLOTS) * TILES + t], turn, 1)
                        n = n + jnp.where(mask, e, 0.0)
                    acc = out(x, t, line[p + 2], n, acc)
            return acc

        groups = BX // GROUP
        even[...] = along_z(w, 0)

        def pair(i, acc):
            odd[...] = along_z(w, (2 * i + 1) * GROUP)
            acc = group(2 * i, even, acc)
            even[...] = along_z(w, jnp.minimum(2 * i + 2, groups - 1) * GROUP)
            return group(2 * i + 1, odd, acc)

        return lax.fori_loop(0, groups // 2, pair, init)

    def fixes(k, apply_x, apply_y, then):
        whole = k < 2
        for side in range(2):
            @pl.when(has_y[side])
            def _(side=side):
                y_copy(k, 1 - side).wait_recv()
                inner, outer = (1, 0) if side == 0 else (0, 1)
                first, second = (0, 1) if side == 0 else (BY - 1, BY - 2)
                span = range(STRIPS)
                if not whole:
                    span = range((1 - side) * STRIPS // 2, (2 - side) * STRIPS // 2)
                for j in span:
                    at = pl.ds(8 * j, 8)
                    close = hy[k, side, inner, at, :]
                    apply_y(j, first, 16.0 * close - hy[k, side, outer, at, :])
                    apply_y(j, second, -close)
        for h in range(2):
            for side in range(2):
                if not x_sent(k, 1 - side, h):
                    continue

                @pl.when(has_x[side])
                def _(side=side, h=h):
                    x_arrived(k, side, h)
                    inner, outer = (1, 0) if side == 0 else (0, 1)
                    first, second = (0, 1) if side == 0 else (BX - 1, BX - 2)
                    for u in range(TILES // 2):
                        t = h * (TILES // 2) + u
                        close = hx[k, side, h, inner, pl.ds(8 * u, 8), :]
                        distant = hx[k, side, h, outer, pl.ds(8 * u, 8), :]
                        apply_x(first, t, 16.0 * close - distant)
                        apply_x(second, t, -close)
                    then(side, h)

    def basis_step(w, new, k, moments, init):
        def out(x, t, c, n, acc):
            new[pl.ds(spot_of(x, 8 * t), 8), :] = (
                c - minv[pl.ds(pl.multiple_of(x * BY, 8) + 8 * t, 8), :] * n
            )
            return moments(x, t, c, acc)

        sums = bulk(w, out, k, init, True)

        def apply_x(x, t, n):
            at = pl.ds(spot_of(x, 8 * t), 8)
            new[at, :] = new[at, :] - minv[pl.ds(x * BY + 8 * t, 8), :] * n

        def apply_y(j, y, n):
            at = pl.ds(spot_of(8 * j, y), 8, stride=PITCH)
            new[at, :] = new[at, :] - minv[pl.ds(8 * j * BY + y, 8, stride=BY), :] * n

        def then(side, h):
            if x_sent(k + 1, side, h):
                x_send(new, k + 1, side, h)

        fixes(k, apply_x, apply_y, then)
        send_y(new, k + 1)
        if k > 0:
            await_signals(k - 1, 1 << k)
        signal(k, 2 << k)
        send_z(new, k + 1)
        return sums

    basis_step(w0, w1, 0, lambda x, t, c, acc: acc, 0)

    def first_moments(x, t, c, acc):
        at = pl.ds(8 * t, 8)
        return (acc[0] + bs[0, x, at, :] * c, acc[1] + ((7.5 + bs[1, x, at, :]) * c) * c)

    mu1, mu2 = basis_step(w1, w2, 1, first_moments, (zero, zero))
    send_fault()

    def last(x, t, c, n, acc):
        d = (7.5 + bs[1, x, pl.ds(8 * t, 8), :]) * c
        return (
            acc[0] + d * w1[pl.ds(spot_of(x, 8 * t), 8), :],
            acc[1] + d * c,
            acc[2] + c * (d - n * (1.0 / 12.0)),
        )

    mu3, mu4, mu5 = bulk(w2, last, 2, (zero, zero, zero), False)
    cross_sum[...] = zero

    def cross_x(x, t, n):
        cross_sum[...] = cross_sum[...] + w2[pl.ds(spot_of(x, 8 * t), 8), :] * n

    def cross_y(j, y, n):
        cross_sum[...] = cross_sum[...] + w2[pl.ds(spot_of(8 * j, y), 8, stride=PITCH), :] * n

    z_copy(2).wait_recv()
    crossing = zero
    for i in range(packs):
        crossing = crossing + zpack[2, i] * edge_terms(jnp.where(halo_here, hz[2, i], 0.0))
    await_signals(1, 4)
    signal(2, 8)
    fixes(2, cross_x, cross_y, lambda side, h: None)
    mu5 = mu5 - (2.0 * cross_sum[...] + crossing) * (1.0 / 12.0)

    local = zero
    for j, m in enumerate((mu0, mu1, mu2, mu3, mu4, mu5)):
        local = jnp.where(row == j, jnp.sum(m, axis=0, keepdims=True), local)
    local = jnp.where(lane == row, jnp.sum(local, axis=1, keepdims=True), 0.0)
    local = jnp.sum(local, axis=0, keepdims=True)

    def reduce(value, low, buf, s, devices):
        buf[0, pl.ds(0, 1), :] = value
        buf[0, pl.ds(1, 1), :] = low
        for r, device in enumerate(devices):
            remote(buf.at[0], buf.at[r + 1], rs_sem.at[s], rr_sem.at[s], device).start()
        land = buf.at[pl.ds(1, len(devices))]
        remote(land, land, rs_sem.at[s], rr_sem.at[s], partner).wait_recv()
        terms = [(value, low)]
        for r in range(len(devices)):
            terms.append((buf[r + 1, pl.ds(0, 1), :], buf[r + 1, pl.ds(1, 1), :]))
        while len(terms) > 1:
            pairs = []
            for a, b in zip(terms[::2], terms[1::2]):
                h, e = two_sum(a[0], b[0])
                pairs.append((h, e + (a[1] + b[1])))
            terms = pairs
        return terms[0]

    total = reduce(local, jnp.zeros((1, BZ), F32), part_a, 0, peers)
    await_signals(2, 8)
    total = reduce(total[0], total[1], part_b, 1, cross)

    mu = []
    for j in range(6):
        mu.append(norm(*(jnp.broadcast_to(v[:, j : j + 1], (8, BZ)) for v in total)))
    for j, c in enumerate(coefficients(mu)):
        coef[j] = c

    for s in range(2):
        @pl.when(gy != ny // 2 - 1 + s)
        def _(s=s):
            land = fault.at[s]
            remote(land, land, fs_sem.at[0], fr_sem.at[s], partner).wait_recv()
    for k in range(3):
        for i in range(own_rows // 8):
            at = pl.ds(8 * i, 8)
            fault_sum[k, at, :] = fault[0, k, at, :] + fault[1, k, at, :]

    for s, buf in enumerate((part_a, part_b)):
        sent = buf.at[pl.ds(1, buf.shape[0] - 1)]
        remote(sent, sent, rs_sem.at[s], rr_sem.at[s], partner).wait_send()
    remote(zpack, hz, zs_sem.at[0], zr_sem.at[0], partner).wait_send()
    for k in range(3):
        for side in range(2):
            @pl.when(has_x[side])
            def _(k=k, side=side):
                sent = hx.at[k, side] if k < 2 else hx.at[k, side, 0]
                remote(sent, sent, xs_sem.at[k, side], xr_sem.at[k, side, 0], partner).wait_send()
            @pl.when(has_y[side])
            def _(k=k, side=side):
                y_copy(k, side).wait_send()

    @pl.when(near_fault)
    def _():
        sent = trac.at[:, pl.ds(0, (ny - 1) * own_rows), :]
        remote(sent, sent, fs_sem.at[0], fr_sem.at[0], partner).wait_send()


def combine(w0, w1, w2, coef, fault_sum, prestress, state, normal, u, slip, buf, sem):
    c0, c1, c2 = coef[0], coef[1], coef[2]
    step = BX // CHUNKS
    copies = []
    for i in range(CHUNKS):
        def plane(x, carry):
            for t in range(TILES):
                at = pl.ds(spot_of(x, 8 * t), 8)
                buf[x, pl.ds(8 * t, 8), :] = (c0 * w0[at, :] + c1 * w1[at, :]) + c2 * w2[at, :]
            return carry

        lax.fori_loop(i * step, (i + 1) * step, plane, 0)
        part = pl.ds(i * step, step)
        copy = pltpu.make_async_copy(buf.at[part], u.at[part], sem.at[i])
        copy.start()
        copies.append(copy)
    for i in range(slip.shape[0] // 8):
        at = pl.ds(8 * i, 8)
        traction = (c0 * fault_sum[0, at, :] + c1 * fault_sum[1, at, :]) + c2 * fault_sum[2, at, :]
        x = (prestress[at, :] + 2.0 * traction) / normal[at, :]
        half = 0.6931471805599453
        large = jnp.exp(x - half) - jnp.exp(-x - half)
        q = x * x
        small = x * (1.0 + q * (1 / 6 + q * (1 / 120 + q * (1 / 5040 + q * (1 / 362880 + q / 39916800)))))
        sinh = jnp.where(jnp.abs(x) < 1.0, small, large)
        slip[at, :] = jnp.exp(-state[at, :]) * sinh
    for copy in copies:
        copy.wait()


def per_device(load, stiffness, prestress, state_var, normal_a):
    vmem = pl.BlockSpec(memory_space=pltpu.VMEM)
    hbm = pl.BlockSpec(memory_space=pl.ANY)
    ny = lax.axis_size("gy")
    own = BX // ny
    group = ny * lax.axis_size("gz")
    nx = lax.axis_size("gx")
    big = (ROWS, BZ)
    packs = (BX // SLOTS) * TILES
    DMA = pltpu.SemaphoreType.DMA
    outs = pl.pallas_call(
        krylov,
        out_shape=[
            pltpu.VMEM(big, F32), pltpu.VMEM(big, F32), pltpu.VMEM(big, F32),
            pltpu.VMEM((3, 8, BZ), F32), pltpu.VMEM((3, own, BZ), F32),
        ],
        in_specs=[pl.BlockSpec(memory_space=pltpu.HBM)] * 2,
        out_specs=[vmem] * 5,
        scratch_shapes=[
            pltpu.VMEM((2, BX, BY, BZ), F32),
            pltpu.VMEM((BX * BY, BZ), F32),
            pltpu.VMEM((3, 2, 2, BX, BZ), F32),
            pltpu.VMEM((3, packs, 8, BZ), F32),
            pltpu.VMEM((packs, 8, BZ), F32),
            pltpu.VMEM((3, BX, BZ), F32),
            pltpu.VMEM((3, 2, 2, 2, BY // 2, BZ), F32),
            pltpu.VMEM((3, 2, 2, BX, BZ), F32),
            pltpu.VMEM((3, packs, 8, BZ), F32),
            pltpu.VMEM((2, 3, own, BZ), F32),
            pltpu.VMEM((group, 2, BZ), F32),
            pltpu.VMEM((nx, 2, BZ), F32),
            pltpu.VMEM((8, BZ), F32),
            pltpu.VMEM((3 * BZ, BZ), BF16),
            pltpu.VMEM((GROUP * PITCH, BZ), F32),
            pltpu.VMEM((GROUP * PITCH, BZ), F32),
            DMA((4 + INNER,)),
            DMA((3, 2)), DMA((3, 2, 2)), DMA((3, 2)), DMA((3, 2)), DMA((1,)), DMA((3,)),
            DMA((1,)), DMA((2,)),
            DMA((2,)), DMA((2,)),
            pltpu.SemaphoreType.REGULAR((3, 2)),
        ],
        compiler_params=pltpu.CompilerParams(
            collective_id=0, has_side_effects=True, vmem_limit_bytes=55 * 2**20
        ),
        name="krylov",
    )(load, stiffness)
    return pl.pallas_call(
        combine,
        out_shape=[
            jax.ShapeDtypeStruct(load.shape, F32),
            jax.ShapeDtypeStruct(prestress.shape, F32),
        ],
        in_specs=[vmem] * 8,
        out_specs=[hbm, vmem],
        scratch_shapes=[pltpu.VMEM((BX, BY, BZ), F32), DMA((CHUNKS,))],
        compiler_params=pltpu.CompilerParams(vmem_limit_bytes=24 * 2**20),
        name="combine",
    )(*outs, prestress, state_var, normal_a)


def solution(mesh):
    block = P("gx", "gy", "gz")
    fault = P(("gx", "gy"), "gz")
    return jax.shard_map(
        per_device,
        mesh=mesh,
        in_specs=(block, block, fault, fault, fault),
        out_specs=(block, fault),
        check_vma=False,
    )
```

```python
import functools

import jax
import jax.numpy as jnp
from jax import lax
from jax.experimental import pallas as pl
from jax.experimental.pallas import tpu as pltpu
from jax.sharding import PartitionSpec as P

MESH = pl.DeviceIdType.MESH
F32 = jnp.float32
BF16 = jnp.bfloat16
BX, BY, BZ = 64, 64, 128
LOW = 8
PITCH = BY + LOW
ROWS = (BX + 4) * PITCH + LOW
TILES = BY // 8
STRIPS = BX // 8
CHUNKS = 8
INNER = 6
SLOTS = 32
GROUP = 4
UNROLL = 8


def two_sum(a, b):
    s = a + b
    t = s - a
    return s, (a - (s - t)) + (b - t)


def split(a):
    t = a * 4097.0
    high = t - (t - a)
    return high, a - high


def two_prod(a, b):
    p = a * b
    ah, al = split(a)
    bh, bl = split(b)
    return p, ((ah * bh - p) + ah * bl + al * bh) + al * bl


def norm(h, l):
    s = h + l
    return s, l - (s - h)


def dd_sub(a, b):
    s, e = two_sum(a[0], -b[0])
    return norm(s, e + (a[1] - b[1]))


def dd_mul(a, b):
    p, e = two_prod(a[0], b[0])
    return norm(p, e + (a[0] * b[1] + a[1] * b[0]))


def dd_div(a, b):
    q = a[0] / b[0]
    p, e = two_prod(q, b[0])
    r = ((a[0] - p) - e) + (a[1] - q * b[1])
    return norm(q, r / b[0])


def coefficients(mu):
    theta = dd_div(mu[1], mu[0])
    s = [None] + [dd_sub(mu[j + 1], dd_mul(theta, mu[j])) for j in range(1, 5)]
    a1 = dd_sub(dd_div(s[2], s[1]), theta)
    b1 = dd_div(s[1], mu[0])

    def second(j):
        return dd_sub(dd_sub(s[j + 1], dd_mul(a1, s[j])), dd_mul(b1, mu[j]))

    t2, t3 = second(2), second(3)
    a2 = dd_sub(dd_sub(dd_div(t3, t2), a1), theta)
    b2 = dd_div(t2, s[1])
    a0, a1, a2, b1, b2 = theta[0], a1[0], a2[0], b1[0], b2[0]
    d0 = a0
    d1 = a1 - b1 / d0
    d2 = a2 - b2 / d1
    y2 = 1.0 / (d0 * d1 * d2)
    y1 = (-1.0 / d0 - b2 * y2) / d1
    y0 = (1.0 - b1 * y1) / d0
    c2 = y2
    c1 = y1 - (a0 + a1) * y2
    c0 = y0 - a0 * y1 + (a0 * a1 - b1) * y2
    return c0, c1, c2


def spot_of(x, y=0):
    return pl.multiple_of((x + 2) * PITCH + LOW, 8) + y


def zero_edges(w):
    z8 = jnp.zeros((8, BZ), F32)
    for t in range(2 * PITCH // 8):
        w[pl.ds(8 * t, 8), :] = z8
        w[pl.ds(ROWS - LOW - 2 * PITCH + LOW + 8 * t, 8), :] = z8

    def body(x, carry):
        w[pl.ds(pl.multiple_of((x + 2) * PITCH, 8), 8), :] = z8
        return carry

    lax.fori_loop(0, BX + 1, body, 0, unroll=5)


def krylov(
    load, stiff, w0, w1, w2, coef, fault_sum,
    bs, minv, ypack, zpack, edge, trac,
    hx, hy, hz, fault, part_a, part_b, cross_sum, band, even, odd,
    in_sem, xs_sem, xr_sem, ys_sem, yr_sem, zs_sem, zr_sem, fs_sem, fr_sem, rs_sem, rr_sem, token,
):
    gx, gy, gz = (lax.axis_index(a) for a in ("gx", "gy", "gz"))
    nx, ny, nz = (lax.axis_size(a) for a in ("gx", "gy", "gz"))
    group = ny * nz
    spot = gy * nz + gz
    lane = lax.broadcasted_iota(jnp.int32, (8, BZ), 1)
    row = lax.broadcasted_iota(jnp.int32, (8, BZ), 0)
    place = (lane + 2) & 3
    halo_here = (place >> 1) == (1 - gz)
    packs = (BX // SLOTS) * TILES
    zero = jnp.zeros((8, BZ), F32)

    regions = [
        (0, 2, 0, BY), (BX - 2, BX, 0, BY), (2, BX - 2, 0, 8), (2, BX - 2, BY - 8, BY)
    ]
    cuts = [2 + (BX - 4) * i // INNER for i in range(INNER + 1)]
    regions += [(lo, hi, 8, BY - 8) for lo, hi in zip(cuts, cuts[1:])]
    for n, (xa, xb, ya, yb) in enumerate(regions):
        part = (pl.ds(xa, xb - xa), pl.ds(ya, yb - ya))
        for i, source in enumerate((load, stiff)):
            pltpu.make_async_copy(source.at[part], bs.at[(i,) + part], in_sem.at[n]).start()

    barrier = pltpu.get_barrier_semaphore()
    peers = []
    for r in range(1, group):
        other = lax.rem(spot + r, group)
        peers.append((gx, other // nz, lax.rem(other, nz)))
    cross = [(lax.rem(gx + r, nx), gy, gz) for r in range(1, nx)]
    has_x = (gx > 0, gx < nx - 1)
    has_y = (gy > 0, gy < ny - 1)

    def one(flag):
        return jnp.where(flag, 1, 0)

    def sides(distance):
        return ((gx >= distance, gx - distance), (gx + distance < nx, gx + distance))

    def signal(k, distance):
        for side, (there, target) in enumerate(sides(distance)):
            @pl.when(there)
            def _(side=side, target=target):
                pl.semaphore_signal(
                    token.at[k, 1 - side], inc=1, device_id=(target, gy, gz), device_id_type=MESH
                )

    def await_signals(k, distance):
        for side, (there, _) in enumerate(sides(distance)):
            @pl.when(there)
            def _(side=side):
                pl.semaphore_wait(token.at[k, side], 1)

    for there, target in sides(1):
        @pl.when(there)
        def _(target=target):
            pl.semaphore_signal(barrier, inc=1, device_id=(target, gy, gz), device_id_type=MESH)
    for side in range(2):
        @pl.when(has_y[side])
        def _(side=side):
            pl.semaphore_signal(
                barrier, inc=1, device_id=(gx, gy + 2 * side - 1, gz), device_id_type=MESH
            )
    pl.semaphore_signal(barrier, inc=1, device_id=(gx, gy, 1 - gz), device_id_type=MESH)

    for w in (w0, w1, w2):
        zero_edges(w)

    at_row = lax.rem(lax.broadcasted_iota(jnp.int32, (3 * BZ, BZ), 0), BZ)
    gap = jnp.abs(at_row - lax.broadcasted_iota(jnp.int32, (3 * BZ, BZ), 1))
    band[...] = jnp.where(gap == 1, 16.0, jnp.where(gap == 2, -1.0, 0.0)).astype(BF16)

    def remote(src, dst, send, recv, device):
        return pltpu.make_async_remote_copy(
            src_ref=src, dst_ref=dst, send_sem=send, recv_sem=recv,
            device_id=device, device_id_type=MESH,
        )

    partner = (gx, gy, 1 - gz)
    half = BY // 2

    def x_sent(k, side, h):
        return k < 2 or h == side

    def x_send(w, k, side, h):
        device = (gx - 1 if side == 0 else gx + 1, gy, gz)
        for n in range(2):
            plane = n if side == 0 else BX - 2 + n
            remote(
                w.at[pl.ds(spot_of(plane, h * half), half), :], hx.at[k, 1 - side, h, n],
                xs_sem.at[k, side], xr_sem.at[k, 1 - side, h], device,
            ).start()

    def x_arrived(k, side, h):
        land = hx.at[k, side, h]
        remote(land, land, xs_sem.at[k, side], xr_sem.at[k, side, h], partner).wait_recv()

    def y_copy(k, side):
        strips = pl.ds(0, BX) if k < 2 else pl.ds(side * (BX // 2), BX // 2)
        return remote(
            ypack.at[k, side, :, strips, :], hy.at[k, 1 - side, :, strips, :],
            ys_sem.at[k, side], yr_sem.at[k, 1 - side],
            (gx, gy - 1 if side == 0 else gy + 1, gz),
        )

    def z_copy(k):
        return remote(zpack.at[k], hz.at[k], zs_sem.at[0], zr_sem.at[k], partner)

    near_fault = (gy == ny // 2 - 1) | (gy == ny // 2)
    source = gy - (ny // 2 - 1)
    low_side = jnp.where(gy == ny // 2, 1.0, 0.0)
    high_side = jnp.where(gy == ny // 2 - 1, 1.0, 0.0)
    own_rows = BX // ny

    def send_fault():
        @pl.when(near_fault)
        def _():
            for r in range(1, ny):
                owner = lax.rem(gy + r, ny)
                remote(
                    trac.at[:, pl.ds(pl.multiple_of(owner * own_rows, 8), own_rows), :],
                    fault.at[source], fs_sem.at[0], fr_sem.at[source], (gx, owner, gz),
                ).start()
            for k in range(3):
                for i in range(own_rows // 8):
                    fault[source, k, pl.ds(8 * i, 8), :] = trac[
                        k, pl.ds(pl.multiple_of(gy * own_rows + 8 * i, 8), 8), :
                    ]

    def send_y(w, k):
        for j in range(STRIPS):
            strip = []
            for n, y in enumerate((0, 1, BY - 2, BY - 1)):
                v = w[pl.ds(spot_of(8 * j, y), 8, stride=PITCH), :]
                ypack[k, n // 2, n % 2, pl.ds(8 * j, 8), :] = v
                strip.append(v)
            term = low_side * (27.0 * strip[0] - strip[1]) + high_side * (strip[2] - 27.0 * strip[3])
            trac[k, pl.ds(8 * j, 8), :] = term / 24.0
        for side in range(2):
            @pl.when(has_y[side])
            def _(side=side):
                y_copy(k, side).start()

    def pack(w, k, i):
        for t in range(TILES):
            packed = zero
            for q in range(SLOTS):
                mask = ((lane + 2 - 4 * q) & (BZ - 1)) < 4
                tile = w[pl.ds(spot_of(i * SLOTS + q, 8 * t), 8), :]
                packed = jnp.where(mask, pltpu.roll(tile, 4 * q, 1), packed)
            zpack[k, i * TILES + t] = packed

    mu0 = zero
    for n, (xa, xb, ya, yb) in enumerate(regions):
        part = (slice(None), pl.ds(xa, xb - xa), pl.ds(ya, yb - ya))
        pltpu.make_async_copy(bs.at[part], bs.at[part], in_sem.at[n]).wait()

        def start_plane(x, acc):
            for t in range(ya // 8, yb // 8):
                at = pl.ds(8 * t, 8)
                b = bs[0, x, at, :]
                inverse = 1.0 / (7.5 + bs[1, x, at, :])
                w = b * inverse
                w0[pl.ds(spot_of(x, 8 * t), 8), :] = w
                minv[pl.ds(pl.multiple_of(x * BY, 8) + 8 * t, 8), :] = inverse * (1.0 / 12.0)
                acc = acc + b * w
            return acc

        count = xb - xa
        tiles = (yb - ya) // 8
        unroll = max(u for u in range(1, count + 1) if count % u == 0 and u * tiles <= 60 or u == 1)
        mu0 = lax.fori_loop(xa, xb, start_plane, mu0, unroll=unroll)
        if n == 1:
            pl.semaphore_wait(
                barrier,
                1 + one(has_x[0]) + one(has_x[1]) + one(has_y[0]) + one(has_y[1]),
            )
            for side in range(2):
                @pl.when(has_x[side])
                def _(side=side):
                    for h in range(2):
                        x_send(w0, 0, side, h)
        if n == 3:
            send_y(w0, 0)

    def edge_terms(d):
        near = jnp.where(place == 1, pltpu.roll(d, BZ - 1, 1), pltpu.roll(d, 1, 1))
        near = jnp.where((place == 1) | (place == 2), near, 0.0)
        return 16.0 * near - jnp.where(place < 2, pltpu.roll(d, BZ - 2, 1), pltpu.roll(d, 2, 1))

    def along_z(w, x):
        c = w[pl.ds(spot_of(x), GROUP * PITCH), :]
        high = c.astype(BF16)
        rest = c - high.astype(F32)
        middle = rest.astype(BF16)
        low = (rest - middle.astype(F32)).astype(BF16)
        return jnp.dot(
            jnp.concatenate([high, middle, low], axis=1), band[...], preferred_element_type=F32
        )

    edge_mask = ((lane + 2) & (BZ - 1)) < 4

    def z_term(x, t):
        turn = lax.rem(BZ - 4 * lax.rem(x, SLOTS), BZ)
        return jnp.where(edge_mask, pltpu.roll(edge[(x // SLOTS) * TILES + t], turn, 1), 0.0)

    def bulk(w, out, k, init, z_fix=None):
        def group(g, zz, acc, with_z):
            for t in range(TILES):
                def at(p, dy):
                    return w[pl.ds(spot_of(g * GROUP, 8 * t) + (p * PITCH + dy), 8), :]

                line = [at(p, 0) for p in range(-2, GROUP + 2)]
                for p in range(GROUP):
                    x = g * GROUP + p
                    near = (line[p + 3] + line[p + 1]) + (at(p, 1) + at(p, -1))
                    far = (line[p + 4] + line[p]) + (at(p, 2) + at(p, -2))
                    n = (16.0 * near - far) + zz[pl.ds(p * PITCH + 8 * t, 8), :]
                    if with_z:
                        n = n + z_term(x, t)
                    acc = out(x, t, line[p + 2], n, acc)
            return acc

        groups = BX // GROUP
        even[...] = along_z(w, 0)

        pairs = groups // 2
        ends = BX // SLOTS
        inside = (pairs - ends) * 2 * GROUP // ends

        def pair(i, acc, with_z=False):
            odd[...] = along_z(w, (2 * i + 1) * GROUP)
            acc = group(2 * i, even, acc, with_z)
            even[...] = along_z(w, jnp.minimum(2 * i + 2, groups - 1) * GROUP)
            return group(2 * i + 1, odd, acc, with_z)

        def first_pair(i, acc):
            pack(w, k, i)
            return pair(i, acc)

        def last_pair(i, acc):
            for p in range(inside):
                for t in range(TILES):
                    z_fix((i - (pairs - ends)) * inside + p, t)
            return pair(i, acc, True)

        acc = lax.fori_loop(0, ends, first_pair, init)
        z_copy(k).start()
        if z_fix is None:
            return lax.fori_loop(ends, pairs, pair, acc)
        acc = lax.fori_loop(ends, pairs - ends, pair, acc)
        z_copy(k).wait_recv()
        for i in range(packs):
            edge[i] = edge_terms(jnp.where(halo_here, hz[k, i], 0.0))
        return lax.fori_loop(pairs - ends, pairs, last_pair, acc)

    def fixes(k, apply_x, apply_y, then):
        whole = k < 2
        for side in range(2):
            @pl.when(has_y[side])
            def _(side=side):
                y_copy(k, 1 - side).wait_recv()
                inner, outer = (1, 0) if side == 0 else (0, 1)
                first, second = (0, 1) if side == 0 else (BY - 1, BY - 2)
                span = range(STRIPS)
                if not whole:
                    span = range((1 - side) * STRIPS // 2, (2 - side) * STRIPS // 2)
                for j in span:
                    at = pl.ds(8 * j, 8)
                    close = hy[k, side, inner, at, :]
                    apply_y(j, first, 16.0 * close - hy[k, side, outer, at, :])
                    apply_y(j, second, -close)
        for h in range(2):
            for side in range(2):
                if not x_sent(k, 1 - side, h):
                    continue

                @pl.when(has_x[side])
                def _(side=side, h=h):
                    x_arrived(k, side, h)
                    inner, outer = (1, 0) if side == 0 else (0, 1)
                    first, second = (0, 1) if side == 0 else (BX - 1, BX - 2)
                    for u in range(TILES // 2):
                        t = h * (TILES // 2) + u
                        close = hx[k, side, h, inner, pl.ds(8 * u, 8), :]
                        distant = hx[k, side, h, outer, pl.ds(8 * u, 8), :]
                        apply_x(first, t, 16.0 * close - distant)
                        apply_x(second, t, -close)
                    then(side, h)

    def basis_step(w, new, k, moments, init):
        def out(x, t, c, n, acc):
            new[pl.ds(spot_of(x, 8 * t), 8), :] = (
                c - minv[pl.ds(pl.multiple_of(x * BY, 8) + 8 * t, 8), :] * n
            )
            return moments(x, t, c, acc)

        def z_fix(x, t):
            at = pl.ds(spot_of(x, 8 * t), 8)
            m = minv[pl.ds(pl.multiple_of(x * BY, 8) + 8 * t, 8), :]
            new[at, :] = new[at, :] - m * z_term(x, t)

        sums = bulk(w, out, k, init, z_fix)

        def apply_x(x, t, n):
            at = pl.ds(spot_of(x, 8 * t), 8)
            new[at, :] = new[at, :] - minv[pl.ds(x * BY + 8 * t, 8), :] * n

        def apply_y(j, y, n):
            at = pl.ds(spot_of(8 * j, y), 8, stride=PITCH)
            new[at, :] = new[at, :] - minv[pl.ds(8 * j * BY + y, 8, stride=BY), :] * n

        def then(side, h):
            if x_sent(k + 1, side, h):
                x_send(new, k + 1, side, h)

        fixes(k, apply_x, apply_y, then)
        send_y(new, k + 1)
        if k > 0:
            await_signals(k - 1, 1 << k)
        signal(k, 2 << k)
        return sums

    basis_step(w0, w1, 0, lambda x, t, c, acc: acc, 0)

    def first_moments(x, t, c, acc):
        at = pl.ds(8 * t, 8)
        return (acc[0] + bs[0, x, at, :] * c, acc[1] + ((7.5 + bs[1, x, at, :]) * c) * c)

    mu1, mu2 = basis_step(w1, w2, 1, first_moments, (zero, zero))
    send_fault()

    def last(x, t, c, n, acc):
        d = (7.5 + bs[1, x, pl.ds(8 * t, 8), :]) * c
        return (
            acc[0] + d * w1[pl.ds(spot_of(x, 8 * t), 8), :],
            acc[1] + d * c,
            acc[2] + c * (d - n * (1.0 / 12.0)),
        )

    mu3, mu4, mu5 = bulk(w2, last, 2, (zero, zero, zero))
    cross_sum[...] = zero

    def cross_x(x, t, n):
        cross_sum[...] = cross_sum[...] + w2[pl.ds(spot_of(x, 8 * t), 8), :] * n

    def cross_y(j, y, n):
        cross_sum[...] = cross_sum[...] + w2[pl.ds(spot_of(8 * j, y), 8, stride=PITCH), :] * n

    z_copy(2).wait_recv()
    crossing = zero
    for i in range(packs):
        crossing = crossing + zpack[2, i] * edge_terms(jnp.where(halo_here, hz[2, i], 0.0))
    await_signals(1, 4)
    signal(2, 8)
    fixes(2, cross_x, cross_y, lambda side, h: None)
    mu5 = mu5 - (2.0 * cross_sum[...] + crossing) * (1.0 / 12.0)

    local = zero
    for j, m in enumerate((mu0, mu1, mu2, mu3, mu4, mu5)):
        local = jnp.where(row == j, jnp.sum(m, axis=0, keepdims=True), local)
    local = jnp.where(lane == row, jnp.sum(local, axis=1, keepdims=True), 0.0)
    local = jnp.sum(local, axis=0, keepdims=True)

    def reduce(value, low, buf, s, devices):
        buf[0, pl.ds(0, 1), :] = value
        buf[0, pl.ds(1, 1), :] = low
        for r, device in enumerate(devices):
            remote(buf.at[0], buf.at[r + 1], rs_sem.at[s], rr_sem.at[s], device).start()
        land = buf.at[pl.ds(1, len(devices))]
        remote(land, land, rs_sem.at[s], rr_sem.at[s], partner).wait_recv()
        terms = [(value, low)]
        for r in range(len(devices)):
            terms.append((buf[r + 1, pl.ds(0, 1), :], buf[r + 1, pl.ds(1, 1), :]))
        while len(terms) > 1:
            pairs = []
            for a, b in zip(terms[::2], terms[1::2]):
                h, e = two_sum(a[0], b[0])
                pairs.append((h, e + (a[1] + b[1])))
            terms = pairs
        return terms[0]

    total = reduce(local, jnp.zeros((1, BZ), F32), part_a, 0, peers)
    await_signals(2, 8)
    total = reduce(total[0], total[1], part_b, 1, cross)

    mu = []
    for j in range(6):
        mu.append(norm(*(jnp.broadcast_to(v[:, j : j + 1], (8, BZ)) for v in total)))
    for j, c in enumerate(coefficients(mu)):
        coef[j] = c

    for s in range(2):
        @pl.when(gy != ny // 2 - 1 + s)
        def _(s=s):
            land = fault.at[s]
            remote(land, land, fs_sem.at[0], fr_sem.at[s], partner).wait_recv()
    for k in range(3):
        for i in range(own_rows // 8):
            at = pl.ds(8 * i, 8)
            fault_sum[k, at, :] = fault[0, k, at, :] + fault[1, k, at, :]

    for s, buf in enumerate((part_a, part_b)):
        sent = buf.at[pl.ds(1, buf.shape[0] - 1)]
        remote(sent, sent, rs_sem.at[s], rr_sem.at[s], partner).wait_send()
    remote(zpack, hz, zs_sem.at[0], zr_sem.at[0], partner).wait_send()
    for k in range(3):
        for side in range(2):
            @pl.when(has_x[side])
            def _(k=k, side=side):
                sent = hx.at[k, side] if k < 2 else hx.at[k, side, 0]
                remote(sent, sent, xs_sem.at[k, side], xr_sem.at[k, side, 0], partner).wait_send()
            @pl.when(has_y[side])
            def _(k=k, side=side):
                y_copy(k, side).wait_send()

    @pl.when(near_fault)
    def _():
        sent = trac.at[:, pl.ds(0, (ny - 1) * own_rows), :]
        remote(sent, sent, fs_sem.at[0], fr_sem.at[0], partner).wait_send()


def combine(w0, w1, w2, coef, fault_sum, prestress, state, normal, u, slip, buf, sem):
    c0, c1, c2 = coef[0], coef[1], coef[2]
    step = BX // CHUNKS
    copies = []
    for i in range(CHUNKS):
        def plane(x, carry):
            for t in range(TILES):
                at = pl.ds(spot_of(x, 8 * t), 8)
                buf[x, pl.ds(8 * t, 8), :] = (c0 * w0[at, :] + c1 * w1[at, :]) + c2 * w2[at, :]
            return carry

        lax.fori_loop(i * step, (i + 1) * step, plane, 0)
        part = pl.ds(i * step, step)
        copy = pltpu.make_async_copy(buf.at[part], u.at[part], sem.at[i])
        copy.start()
        copies.append(copy)
    for i in range(slip.shape[0] // 8):
        at = pl.ds(8 * i, 8)
        traction = (c0 * fault_sum[0, at, :] + c1 * fault_sum[1, at, :]) + c2 * fault_sum[2, at, :]
        x = (prestress[at, :] + 2.0 * traction) / normal[at, :]
        half = 0.6931471805599453
        large = jnp.exp(x - half) - jnp.exp(-x - half)
        q = x * x
        small = x * (1.0 + q * (1 / 6 + q * (1 / 120 + q * (1 / 5040 + q * (1 / 362880 + q / 39916800)))))
        sinh = jnp.where(jnp.abs(x) < 1.0, small, large)
        slip[at, :] = jnp.exp(-state[at, :]) * sinh
    for copy in copies:
        copy.wait()


def per_device(load, stiffness, prestress, state_var, normal_a):
    vmem = pl.BlockSpec(memory_space=pltpu.VMEM)
    hbm = pl.BlockSpec(memory_space=pl.ANY)
    ny = lax.axis_size("gy")
    own = BX // ny
    group = ny * lax.axis_size("gz")
    nx = lax.axis_size("gx")
    big = (ROWS, BZ)
    packs = (BX // SLOTS) * TILES
    DMA = pltpu.SemaphoreType.DMA
    outs = pl.pallas_call(
        krylov,
        out_shape=[
            pltpu.VMEM(big, F32), pltpu.VMEM(big, F32), pltpu.VMEM(big, F32),
            pltpu.VMEM((3, 8, BZ), F32), pltpu.VMEM((3, own, BZ), F32),
        ],
        in_specs=[pl.BlockSpec(memory_space=pltpu.HBM)] * 2,
        out_specs=[vmem] * 5,
        scratch_shapes=[
            pltpu.VMEM((2, BX, BY, BZ), F32),
            pltpu.VMEM((BX * BY, BZ), F32),
            pltpu.VMEM((3, 2, 2, BX, BZ), F32),
            pltpu.VMEM((3, packs, 8, BZ), F32),
            pltpu.VMEM((packs, 8, BZ), F32),
            pltpu.VMEM((3, BX, BZ), F32),
            pltpu.VMEM((3, 2, 2, 2, BY // 2, BZ), F32),
            pltpu.VMEM((3, 2, 2, BX, BZ), F32),
            pltpu.VMEM((3, packs, 8, BZ), F32),
            pltpu.VMEM((2, 3, own, BZ), F32),
            pltpu.VMEM((group, 2, BZ), F32),
            pltpu.VMEM((nx, 2, BZ), F32),
            pltpu.VMEM((8, BZ), F32),
            pltpu.VMEM((3 * BZ, BZ), BF16),
            pltpu.VMEM((GROUP * PITCH, BZ), F32),
            pltpu.VMEM((GROUP * PITCH, BZ), F32),
            DMA((4 + INNER,)),
            DMA((3, 2)), DMA((3, 2, 2)), DMA((3, 2)), DMA((3, 2)), DMA((1,)), DMA((3,)),
            DMA((1,)), DMA((2,)),
            DMA((2,)), DMA((2,)),
            pltpu.SemaphoreType.REGULAR((3, 2)),
        ],
        compiler_params=pltpu.CompilerParams(
            collective_id=0, has_side_effects=True, vmem_limit_bytes=55 * 2**20
        ),
        name="krylov",
    )(load, stiffness)
    return pl.pallas_call(
        combine,
        out_shape=[
            jax.ShapeDtypeStruct(load.shape, F32),
            jax.ShapeDtypeStruct(prestress.shape, F32),
        ],
        in_specs=[vmem] * 8,
        out_specs=[hbm, vmem],
        scratch_shapes=[pltpu.VMEM((BX, BY, BZ), F32), DMA((CHUNKS,))],
        compiler_params=pltpu.CompilerParams(vmem_limit_bytes=24 * 2**20),
        name="combine",
    )(*outs, prestress, state_var, normal_a)


def solution(mesh):
    block = P("gx", "gy", "gz")
    fault = P(("gx", "gy"), "gz")
    return jax.shard_map(
        per_device,
        mesh=mesh,
        in_specs=(block, block, fault, fault, fault),
        out_specs=(block, fault),
        check_vma=False,
    )
```

```python
import functools

import jax
import jax.numpy as jnp
from jax import lax
from jax.experimental import pallas as pl
from jax.experimental.pallas import tpu as pltpu
from jax.sharding import PartitionSpec as P

MESH = pl.DeviceIdType.MESH
F32 = jnp.float32
BF16 = jnp.bfloat16
BX, BY, BZ = 64, 64, 128
LOW = 8
PITCH = BY + LOW
ROWS = (BX + 4) * PITCH + LOW
TILES = BY // 8
STRIPS = BX // 8
CHUNKS = 8
INNER = 6
SLOTS = 32
GROUP = 4
UNROLL = 8


def two_sum(a, b):
    s = a + b
    t = s - a
    return s, (a - (s - t)) + (b - t)


def split(a):
    t = a * 4097.0
    high = t - (t - a)
    return high, a - high


def two_prod(a, b):
    p = a * b
    ah, al = split(a)
    bh, bl = split(b)
    return p, ((ah * bh - p) + ah * bl + al * bh) + al * bl


def norm(h, l):
    s = h + l
    return s, l - (s - h)


def dd_sub(a, b):
    s, e = two_sum(a[0], -b[0])
    return norm(s, e + (a[1] - b[1]))


def dd_mul(a, b):
    p, e = two_prod(a[0], b[0])
    return norm(p, e + (a[0] * b[1] + a[1] * b[0]))


def dd_div(a, b):
    q = a[0] / b[0]
    p, e = two_prod(q, b[0])
    r = ((a[0] - p) - e) + (a[1] - q * b[1])
    return norm(q, r / b[0])


def coefficients(mu):
    theta = dd_div(mu[1], mu[0])
    s = [None] + [dd_sub(mu[j + 1], dd_mul(theta, mu[j])) for j in range(1, 5)]
    a1 = dd_sub(dd_div(s[2], s[1]), theta)
    b1 = dd_div(s[1], mu[0])

    def second(j):
        return dd_sub(dd_sub(s[j + 1], dd_mul(a1, s[j])), dd_mul(b1, mu[j]))

    t2, t3 = second(2), second(3)
    a2 = dd_sub(dd_sub(dd_div(t3, t2), a1), theta)
    b2 = dd_div(t2, s[1])
    a0, a1, a2, b1, b2 = theta[0], a1[0], a2[0], b1[0], b2[0]
    d0 = a0
    d1 = a1 - b1 / d0
    d2 = a2 - b2 / d1
    y2 = 1.0 / (d0 * d1 * d2)
    y1 = (-1.0 / d0 - b2 * y2) / d1
    y0 = (1.0 - b1 * y1) / d0
    c2 = y2
    c1 = y1 - (a0 + a1) * y2
    c0 = y0 - a0 * y1 + (a0 * a1 - b1) * y2
    return c0, c1, c2


def spot_of(x, y=0):
    return pl.multiple_of((x + 2) * PITCH + LOW, 8) + y


def zero_edges(w):
    z8 = jnp.zeros((8, BZ), F32)
    for t in range(2 * PITCH // 8):
        w[pl.ds(8 * t, 8), :] = z8
        w[pl.ds(ROWS - LOW - 2 * PITCH + LOW + 8 * t, 8), :] = z8

    def body(x, carry):
        w[pl.ds(pl.multiple_of((x + 2) * PITCH, 8), 8), :] = z8
        return carry

    lax.fori_loop(0, BX + 1, body, 0, unroll=5)


def krylov(
    load, stiff, w0, w1, w2, coef, fault_sum,
    bs, minv, ypack, zpack, edge, trac,
    hx, hy, hz, fault, part_a, cross_sum, band, even, odd,
    in_sem, xs_sem, xr_sem, ys_sem, yr_sem, zs_sem, zr_sem, fs_sem, fr_sem, rs_sem, rr_sem, token, column,
):
    gx, gy, gz = (lax.axis_index(a) for a in ("gx", "gy", "gz"))
    nx, ny, nz = (lax.axis_size(a) for a in ("gx", "gy", "gz"))
    lane = lax.broadcasted_iota(jnp.int32, (8, BZ), 1)
    row = lax.broadcasted_iota(jnp.int32, (8, BZ), 0)
    place = (lane + 2) & 3
    halo_here = (place >> 1) == (1 - gz)
    packs = (BX // SLOTS) * TILES
    zero = jnp.zeros((8, BZ), F32)

    regions = [
        (0, 2, 0, BY), (BX - 2, BX, 0, BY), (2, BX - 2, 0, 8), (2, BX - 2, BY - 8, BY)
    ]
    cuts = [2 + (BX - 4) * i // INNER for i in range(INNER + 1)]
    regions += [(lo, hi, 8, BY - 8) for lo, hi in zip(cuts, cuts[1:])]
    for n, (xa, xb, ya, yb) in enumerate(regions):
        part = (pl.ds(xa, xb - xa), pl.ds(ya, yb - ya))
        for i, source in enumerate((load, stiff)):
            pltpu.make_async_copy(source.at[part], bs.at[(i,) + part], in_sem.at[n]).start()

    barrier = pltpu.get_barrier_semaphore()
    side_x = 4 if nx % 4 == 0 else nx
    offsets = [
        (dy, dx, dz, dc)
        for dy in range(nx // side_x) for dx in range(side_x) for dz in range(ny) for dc in range(nz)
    ]

    def hops(o):
        sizes = (nx // side_x, side_x, ny)
        return sum(min(d, n - d) for d, n in zip(o, sizes)) + 0.5 * o[3]

    offsets = sorted(offsets, key=hops, reverse=True)[:-1]
    everyone = [
        (
            lax.rem(gx // side_x + dy, nx // side_x) * side_x + lax.rem(gx + dx, side_x),
            lax.rem(gy + dz, ny),
            lax.rem(gz + dc, nz),
        )
        for dy, dx, dz, dc in offsets
    ]
    has_x = (gx > 0, gx < nx - 1)
    has_y = (gy > 0, gy < ny - 1)

    def one(flag):
        return jnp.where(flag, 1, 0)

    def sides(distance):
        return ((gx >= distance, gx - distance), (gx + distance < nx, gx + distance))

    def signal(k, distance):
        for side, (there, target) in enumerate(sides(distance)):
            @pl.when(there)
            def _(side=side, target=target):
                pl.semaphore_signal(
                    token.at[k, 1 - side], inc=1, device_id=(target, gy, gz), device_id_type=MESH
                )

    def await_signals(k, distance):
        for side, (there, _) in enumerate(sides(distance)):
            @pl.when(there)
            def _(side=side):
                pl.semaphore_wait(token.at[k, side], 1)

    for there, target in sides(1):
        @pl.when(there)
        def _(target=target):
            pl.semaphore_signal(barrier, inc=1, device_id=(target, gy, gz), device_id_type=MESH)
    for side in range(2):
        @pl.when(has_y[side])
        def _(side=side):
            pl.semaphore_signal(
                barrier, inc=1, device_id=(gx, gy + 2 * side - 1, gz), device_id_type=MESH
            )
    pl.semaphore_signal(barrier, inc=1, device_id=(gx, gy, 1 - gz), device_id_type=MESH)

    for w in (w0, w1, w2):
        zero_edges(w)

    at_row = lax.rem(lax.broadcasted_iota(jnp.int32, (3 * BZ, BZ), 0), BZ)
    gap = jnp.abs(at_row - lax.broadcasted_iota(jnp.int32, (3 * BZ, BZ), 1))
    band[...] = jnp.where(gap == 1, 16.0, jnp.where(gap == 2, -1.0, 0.0)).astype(BF16)

    def remote(src, dst, send, recv, device):
        return pltpu.make_async_remote_copy(
            src_ref=src, dst_ref=dst, send_sem=send, recv_sem=recv,
            device_id=device, device_id_type=MESH,
        )

    partner = (gx, gy, 1 - gz)
    half = BY // 2

    def x_sent(k, side, h):
        return k < 2 or h == side

    def x_send(w, k, side, h):
        device = (gx - 1 if side == 0 else gx + 1, gy, gz)
        for n in range(2):
            plane = n if side == 0 else BX - 2 + n
            remote(
                w.at[pl.ds(spot_of(plane, h * half), half), :], hx.at[k, 1 - side, h, n],
                xs_sem.at[k, side], xr_sem.at[k, 1 - side, h], device,
            ).start()

    def x_arrived(k, side, h):
        land = hx.at[k, side, h]
        remote(land, land, xs_sem.at[k, side], xr_sem.at[k, side, h], partner).wait_recv()

    def y_copy(k, side):
        strips = pl.ds(0, BX) if k < 2 else pl.ds(side * (BX // 2), BX // 2)
        return remote(
            ypack.at[k, side, :, strips, :], hy.at[k, 1 - side, :, strips, :],
            ys_sem.at[k, side], yr_sem.at[k, 1 - side],
            (gx, gy - 1 if side == 0 else gy + 1, gz),
        )

    def z_copy(k):
        return remote(zpack.at[k], hz.at[k], zs_sem.at[0], zr_sem.at[k], partner)

    near_fault = (gy == ny // 2 - 1) | (gy == ny // 2)
    source = gy - (ny // 2 - 1)
    low_side = jnp.where(gy == ny // 2, 1.0, 0.0)
    high_side = jnp.where(gy == ny // 2 - 1, 1.0, 0.0)
    own_rows = BX // ny

    def send_fault():
        @pl.when(near_fault)
        def _():
            for r in range(1, ny):
                owner = lax.rem(gy + r, ny)
                remote(
                    trac.at[:, pl.ds(pl.multiple_of(owner * own_rows, 8), own_rows), :],
                    fault.at[source], fs_sem.at[0], fr_sem.at[source], (gx, owner, gz),
                ).start()
            for k in range(3):
                for i in range(own_rows // 8):
                    fault[source, k, pl.ds(8 * i, 8), :] = trac[
                        k, pl.ds(pl.multiple_of(gy * own_rows + 8 * i, 8), 8), :
                    ]

    def send_y(w, k):
        for j in range(STRIPS):
            strip = []
            for n, y in enumerate((0, 1, BY - 2, BY - 1)):
                v = w[pl.ds(spot_of(8 * j, y), 8, stride=PITCH), :]
                ypack[k, n // 2, n % 2, pl.ds(8 * j, 8), :] = v
                strip.append(v)
            term = low_side * (27.0 * strip[0] - strip[1]) + high_side * (strip[2] - 27.0 * strip[3])
            trac[k, pl.ds(8 * j, 8), :] = term / 24.0
        for side in range(2):
            @pl.when(has_y[side])
            def _(side=side):
                y_copy(k, side).start()

    def pack(w, k, i):
        for t in range(TILES):
            packed = zero
            for q in range(SLOTS):
                mask = ((lane + 2 - 4 * q) & (BZ - 1)) < 4
                tile = w[pl.ds(spot_of(i * SLOTS + q, 8 * t), 8), :]
                packed = jnp.where(mask, pltpu.roll(tile, 4 * q, 1), packed)
            zpack[k, i * TILES + t] = packed

    mu0 = zero
    for n, (xa, xb, ya, yb) in enumerate(regions):
        part = (slice(None), pl.ds(xa, xb - xa), pl.ds(ya, yb - ya))
        pltpu.make_async_copy(bs.at[part], bs.at[part], in_sem.at[n]).wait()

        def start_plane(x, acc):
            for t in range(ya // 8, yb // 8):
                at = pl.ds(8 * t, 8)
                b = bs[0, x, at, :]
                inverse = 1.0 / (7.5 + bs[1, x, at, :])
                w = b * inverse
                w0[pl.ds(spot_of(x, 8 * t), 8), :] = w
                minv[pl.ds(pl.multiple_of(x * BY, 8) + 8 * t, 8), :] = inverse * (1.0 / 12.0)
                acc = acc + b * w
            return acc

        count = xb - xa
        tiles = (yb - ya) // 8
        unroll = max(u for u in range(1, count + 1) if count % u == 0 and u * tiles <= 60 or u == 1)
        mu0 = lax.fori_loop(xa, xb, start_plane, mu0, unroll=unroll)
        if n == 1:
            pl.semaphore_wait(
                barrier,
                1 + one(has_x[0]) + one(has_x[1]) + one(has_y[0]) + one(has_y[1]),
            )
            for side in range(2):
                @pl.when(has_x[side])
                def _(side=side):
                    for h in range(2):
                        x_send(w0, 0, side, h)
        if n == 3:
            send_y(w0, 0)

    def edge_terms(d):
        near = jnp.where(place == 1, pltpu.roll(d, BZ - 1, 1), pltpu.roll(d, 1, 1))
        near = jnp.where((place == 1) | (place == 2), near, 0.0)
        return 16.0 * near - jnp.where(place < 2, pltpu.roll(d, BZ - 2, 1), pltpu.roll(d, 2, 1))

    def along_z(w, x):
        c = w[pl.ds(spot_of(x), GROUP * PITCH), :]
        high = c.astype(BF16)
        rest = c - high.astype(F32)
        middle = rest.astype(BF16)
        low = (rest - middle.astype(F32)).astype(BF16)
        return jnp.dot(
            jnp.concatenate([high, middle, low], axis=1), band[...], preferred_element_type=F32
        )

    edge_mask = ((lane + 2) & (BZ - 1)) < 4

    def z_term(x, t):
        turn = lax.rem(BZ - 4 * lax.rem(x, SLOTS), BZ)
        return jnp.where(edge_mask, pltpu.roll(edge[(x // SLOTS) * TILES + t], turn, 1), 0.0)

    def bulk(w, out, k, init, z_fix=None):
        def group(g, zz, acc, with_z):
            for t in range(TILES):
                def at(p, dy):
                    return w[pl.ds(spot_of(g * GROUP, 8 * t) + (p * PITCH + dy), 8), :]

                line = [at(p, 0) for p in range(-2, GROUP + 2)]
                for p in range(GROUP):
                    x = g * GROUP + p
                    near = (line[p + 3] + line[p + 1]) + (at(p, 1) + at(p, -1))
                    far = (line[p + 4] + line[p]) + (at(p, 2) + at(p, -2))
                    n = (16.0 * near - far) + zz[pl.ds(p * PITCH + 8 * t, 8), :]
                    if with_z:
                        n = n + z_term(x, t)
                    acc = out(x, t, line[p + 2], n, acc)
            return acc

        groups = BX // GROUP
        even[...] = along_z(w, 0)

        pairs = groups // 2
        ends = BX // SLOTS
        inside = (pairs - ends) * 2 * GROUP // ends

        def pair(i, acc, with_z=False):
            odd[...] = along_z(w, (2 * i + 1) * GROUP)
            acc = group(2 * i, even, acc, with_z)
            even[...] = along_z(w, jnp.minimum(2 * i + 2, groups - 1) * GROUP)
            return group(2 * i + 1, odd, acc, with_z)

        def first_pair(i, acc):
            pack(w, k, i)
            return pair(i, acc)

        def last_pair(i, acc):
            for p in range(inside):
                for t in range(TILES):
                    z_fix((i - (pairs - ends)) * inside + p, t)
            return pair(i, acc, True)

        acc = lax.fori_loop(0, ends, first_pair, init)
        z_copy(k).start()
        acc = lax.fori_loop(ends, pairs - ends, pair, acc)
        z_copy(k).wait_recv()
        if k == 2:
            await_signals(2, 8)
            for r in range(1, ny):
                pl.semaphore_signal(
                    column.at[0], inc=1, device_id=(gx, lax.rem(gy + r, ny), gz),
                    device_id_type=MESH,
                )
            return lax.fori_loop(pairs - ends, pairs, pair, acc)
        if k == 1:
            await_signals(0, 2)
            signal(1, 4)
        for i in range(packs):
            edge[i] = edge_terms(jnp.where(halo_here, hz[k, i], 0.0))
        return lax.fori_loop(pairs - ends, pairs, last_pair, acc)

    def fixes(k, apply_x, apply_y, then):
        whole = k < 2
        for side in range(2):
            @pl.when(has_y[side])
            def _(side=side):
                y_copy(k, 1 - side).wait_recv()
                inner, outer = (1, 0) if side == 0 else (0, 1)
                first, second = (0, 1) if side == 0 else (BY - 1, BY - 2)
                span = range(STRIPS)
                if not whole:
                    span = range((1 - side) * STRIPS // 2, (2 - side) * STRIPS // 2)
                for j in span:
                    at = pl.ds(8 * j, 8)
                    close = hy[k, side, inner, at, :]
                    apply_y(j, first, 16.0 * close - hy[k, side, outer, at, :])
                    apply_y(j, second, -close)
        for h in range(2):
            for side in range(2):
                if not x_sent(k, 1 - side, h):
                    continue

                @pl.when(has_x[side])
                def _(side=side, h=h):
                    x_arrived(k, side, h)
                    inner, outer = (1, 0) if side == 0 else (0, 1)
                    first, second = (0, 1) if side == 0 else (BX - 1, BX - 2)
                    for u in range(TILES // 2):
                        t = h * (TILES // 2) + u
                        close = hx[k, side, h, inner, pl.ds(8 * u, 8), :]
                        distant = hx[k, side, h, outer, pl.ds(8 * u, 8), :]
                        apply_x(first, t, 16.0 * close - distant)
                        apply_x(second, t, -close)
                    then(side, h)

    def basis_step(w, new, k, moments, init):
        def out(x, t, c, n, acc):
            new[pl.ds(spot_of(x, 8 * t), 8), :] = (
                c - minv[pl.ds(pl.multiple_of(x * BY, 8) + 8 * t, 8), :] * n
            )
            return moments(x, t, c, acc)

        def z_fix(x, t):
            at = pl.ds(spot_of(x, 8 * t), 8)
            m = minv[pl.ds(pl.multiple_of(x * BY, 8) + 8 * t, 8), :]
            new[at, :] = new[at, :] - m * z_term(x, t)

        sums = bulk(w, out, k, init, z_fix)

        def apply_x(x, t, n):
            at = pl.ds(spot_of(x, 8 * t), 8)
            new[at, :] = new[at, :] - minv[pl.ds(x * BY + 8 * t, 8), :] * n

        def apply_y(j, y, n):
            at = pl.ds(spot_of(8 * j, y), 8, stride=PITCH)
            new[at, :] = new[at, :] - minv[pl.ds(8 * j * BY + y, 8, stride=BY), :] * n

        def then(side, h):
            if x_sent(k + 1, side, h):
                x_send(new, k + 1, side, h)

        fixes(k, apply_x, apply_y, then)
        send_y(new, k + 1)
        if k == 0:
            signal(0, 2)
        else:
            await_signals(1, 4)
            signal(2, 8)
        return sums

    basis_step(w0, w1, 0, lambda x, t, c, acc: acc, 0)

    def first_moments(x, t, c, acc):
        at = pl.ds(8 * t, 8)
        return (acc[0] + bs[0, x, at, :] * c, acc[1] + ((7.5 + bs[1, x, at, :]) * c) * c)

    mu1, mu2 = basis_step(w1, w2, 1, first_moments, (zero, zero))
    send_fault()

    def last(x, t, c, n, acc):
        d = (7.5 + bs[1, x, pl.ds(8 * t, 8), :]) * c
        return (
            acc[0] + d * w1[pl.ds(spot_of(x, 8 * t), 8), :],
            acc[1] + d * c,
            acc[2] + c * (d - n * (1.0 / 12.0)),
        )

    mu3, mu4, mu5 = bulk(w2, last, 2, (zero, zero, zero))
    cross_sum[...] = zero

    def cross_x(x, t, n):
        cross_sum[...] = cross_sum[...] + w2[pl.ds(spot_of(x, 8 * t), 8), :] * n

    def cross_y(j, y, n):
        cross_sum[...] = cross_sum[...] + w2[pl.ds(spot_of(8 * j, y), 8, stride=PITCH), :] * n

    crossing = zero
    for i in range(packs):
        crossing = crossing + zpack[2, i] * edge_terms(jnp.where(halo_here, hz[2, i], 0.0))
    fixes(2, cross_x, cross_y, lambda side, h: None)
    mu5 = mu5 - (2.0 * cross_sum[...] + crossing) * (1.0 / 12.0)

    local = zero
    for j, m in enumerate((mu0, mu1, mu2, mu3, mu4, mu5)):
        local = jnp.where(row == j, jnp.sum(m, axis=0, keepdims=True), local)
    local = jnp.where(lane == row, jnp.sum(local, axis=1, keepdims=True), 0.0)
    local = jnp.sum(local, axis=0, keepdims=True)

    pl.semaphore_wait(column.at[0], ny - 1)
    last_slot = len(everyone)
    part_a[last_slot] = local
    for r, device in enumerate(everyone):
        remote(part_a.at[last_slot], part_a.at[r], rs_sem.at[0], rr_sem.at[0], device).start()
    land = part_a.at[pl.ds(0, last_slot)]
    remote(land, land, rs_sem.at[0], rr_sem.at[0], partner).wait_recv()

    def tree(terms):
        while len(terms) > 1:
            pairs = []
            for a, b in zip(terms[::2], terms[1::2]):
                h, e = two_sum(a[0], b[0])
                pairs.append((h, e + (a[1] + b[1])))
            terms = pairs
        return terms[0]

    rows = [
        (part_a[pl.ds(8 * i, 8)].reshape(8, BZ), zero) for i in range((last_slot + 1) // 8)
    ]
    high, low = tree(rows)
    total = tree([(high[i : i + 1], low[i : i + 1]) for i in range(8)])

    mu = []
    for j in range(6):
        mu.append(norm(*(jnp.broadcast_to(v[:, j : j + 1], (8, BZ)) for v in total)))
    for j, c in enumerate(coefficients(mu)):
        coef[j] = c

    for s in range(2):
        @pl.when(gy != ny // 2 - 1 + s)
        def _(s=s):
            land = fault.at[s]
            remote(land, land, fs_sem.at[0], fr_sem.at[s], partner).wait_recv()
    for k in range(3):
        for i in range(own_rows // 8):
            at = pl.ds(8 * i, 8)
            fault_sum[k, at, :] = fault[0, k, at, :] + fault[1, k, at, :]

    remote(land, land, rs_sem.at[0], rr_sem.at[0], partner).wait_send()
    remote(zpack, hz, zs_sem.at[0], zr_sem.at[0], partner).wait_send()
    for k in range(3):
        for side in range(2):
            @pl.when(has_x[side])
            def _(k=k, side=side):
                sent = hx.at[k, side] if k < 2 else hx.at[k, side, 0]
                remote(sent, sent, xs_sem.at[k, side], xr_sem.at[k, side, 0], partner).wait_send()
            @pl.when(has_y[side])
            def _(k=k, side=side):
                y_copy(k, side).wait_send()

    @pl.when(near_fault)
    def _():
        sent = trac.at[:, pl.ds(0, (ny - 1) * own_rows), :]
        remote(sent, sent, fs_sem.at[0], fr_sem.at[0], partner).wait_send()


def combine(w0, w1, w2, coef, fault_sum, prestress, state, normal, u, slip, buf, sem):
    c0, c1, c2 = coef[0], coef[1], coef[2]
    step = BX // CHUNKS
    copies = []
    for i in range(CHUNKS):
        def plane(x, carry):
            for t in range(TILES):
                at = pl.ds(spot_of(x, 8 * t), 8)
                buf[x, pl.ds(8 * t, 8), :] = (c0 * w0[at, :] + c1 * w1[at, :]) + c2 * w2[at, :]
            return carry

        lax.fori_loop(i * step, (i + 1) * step, plane, 0)
        part = pl.ds(i * step, step)
        copy = pltpu.make_async_copy(buf.at[part], u.at[part], sem.at[i])
        copy.start()
        copies.append(copy)
    for i in range(slip.shape[0] // 8):
        at = pl.ds(8 * i, 8)
        traction = (c0 * fault_sum[0, at, :] + c1 * fault_sum[1, at, :]) + c2 * fault_sum[2, at, :]
        x = (prestress[at, :] + 2.0 * traction) / normal[at, :]
        half = 0.6931471805599453
        large = jnp.exp(x - half) - jnp.exp(-x - half)
        q = x * x
        small = x * (1.0 + q * (1 / 6 + q * (1 / 120 + q * (1 / 5040 + q * (1 / 362880 + q / 39916800)))))
        sinh = jnp.where(jnp.abs(x) < 1.0, small, large)
        slip[at, :] = jnp.exp(-state[at, :]) * sinh
    for copy in copies:
        copy.wait()


def per_device(load, stiffness, prestress, state_var, normal_a):
    vmem = pl.BlockSpec(memory_space=pltpu.VMEM)
    hbm = pl.BlockSpec(memory_space=pl.ANY)
    ny = lax.axis_size("gy")
    own = BX // ny
    group = ny * lax.axis_size("gz")
    nx = lax.axis_size("gx")
    big = (ROWS, BZ)
    packs = (BX // SLOTS) * TILES
    DMA = pltpu.SemaphoreType.DMA
    outs = pl.pallas_call(
        krylov,
        out_shape=[
            pltpu.VMEM(big, F32), pltpu.VMEM(big, F32), pltpu.VMEM(big, F32),
            pltpu.VMEM((3, 8, BZ), F32), pltpu.VMEM((3, own, BZ), F32),
        ],
        in_specs=[pl.BlockSpec(memory_space=pltpu.HBM)] * 2,
        out_specs=[vmem] * 5,
        scratch_shapes=[
            pltpu.VMEM((2, BX, BY, BZ), F32),
            pltpu.VMEM((BX * BY, BZ), F32),
            pltpu.VMEM((3, 2, 2, BX, BZ), F32),
            pltpu.VMEM((3, packs, 8, BZ), F32),
            pltpu.VMEM((packs, 8, BZ), F32),
            pltpu.VMEM((3, BX, BZ), F32),
            pltpu.VMEM((3, 2, 2, 2, BY // 2, BZ), F32),
            pltpu.VMEM((3, 2, 2, BX, BZ), F32),
            pltpu.VMEM((3, packs, 8, BZ), F32),
            pltpu.VMEM((2, 3, own, BZ), F32),
            pltpu.VMEM((group * nx, 1, BZ), F32),
            pltpu.VMEM((8, BZ), F32),
            pltpu.VMEM((3 * BZ, BZ), BF16),
            pltpu.VMEM((GROUP * PITCH, BZ), F32),
            pltpu.VMEM((GROUP * PITCH, BZ), F32),
            DMA((4 + INNER,)),
            DMA((3, 2)), DMA((3, 2, 2)), DMA((3, 2)), DMA((3, 2)), DMA((1,)), DMA((3,)),
            DMA((1,)), DMA((2,)),
            DMA((1,)), DMA((1,)),
            pltpu.SemaphoreType.REGULAR((3, 2)),
            pltpu.SemaphoreType.REGULAR((1,)),
        ],
        compiler_params=pltpu.CompilerParams(
            collective_id=0, has_side_effects=True, vmem_limit_bytes=55 * 2**20
        ),
        name="krylov",
    )(load, stiffness)
    return pl.pallas_call(
        combine,
        out_shape=[
            jax.ShapeDtypeStruct(load.shape, F32),
            jax.ShapeDtypeStruct(prestress.shape, F32),
        ],
        in_specs=[vmem] * 8,
        out_specs=[hbm, vmem],
        scratch_shapes=[pltpu.VMEM((BX, BY, BZ), F32), DMA((CHUNKS,))],
        compiler_params=pltpu.CompilerParams(vmem_limit_bytes=24 * 2**20),
        name="combine",
    )(*outs, prestress, state_var, normal_a)


def solution(mesh):
    block = P("gx", "gy", "gz")
    fault = P(("gx", "gy"), "gz")
    return jax.shard_map(
        per_device,
        mesh=mesh,
        in_specs=(block, block, fault, fault, fault),
        out_specs=(block, fault),
        check_vma=False,
    )
```

```python
import functools

import jax
import jax.numpy as jnp
from jax import lax
from jax.experimental import pallas as pl
from jax.experimental.pallas import tpu as pltpu
from jax.sharding import PartitionSpec as P

MESH = pl.DeviceIdType.MESH
F32 = jnp.float32
BF16 = jnp.bfloat16
BX, BY, BZ = 64, 64, 128
LOW = 8
PITCH = BY + LOW
ROWS = (BX + 4) * PITCH + LOW
TILES = BY // 8
STRIPS = BX // 8
CHUNKS = 8
INNER = 6
SLOTS = 32
GROUP = 4
UNROLL = 8


def two_sum(a, b):
    s = a + b
    t = s - a
    return s, (a - (s - t)) + (b - t)


def split(a):
    t = a * 4097.0
    high = t - (t - a)
    return high, a - high


def two_prod(a, b):
    p = a * b
    ah, al = split(a)
    bh, bl = split(b)
    return p, ((ah * bh - p) + ah * bl + al * bh) + al * bl


def norm(h, l):
    s = h + l
    return s, l - (s - h)


def dd_sub(a, b):
    s, e = two_sum(a[0], -b[0])
    return norm(s, e + (a[1] - b[1]))


def dd_mul(a, b):
    p, e = two_prod(a[0], b[0])
    return norm(p, e + (a[0] * b[1] + a[1] * b[0]))


def dd_div(a, b):
    q = a[0] / b[0]
    p, e = two_prod(q, b[0])
    r = ((a[0] - p) - e) + (a[1] - q * b[1])
    return norm(q, r / b[0])


def coefficients(mu):
    theta = dd_div(mu[1], mu[0])
    s = [None] + [dd_sub(mu[j + 1], dd_mul(theta, mu[j])) for j in range(1, 5)]
    a1 = dd_sub(dd_div(s[2], s[1]), theta)
    b1 = dd_div(s[1], mu[0])

    def second(j):
        return dd_sub(dd_sub(s[j + 1], dd_mul(a1, s[j])), dd_mul(b1, mu[j]))

    t2, t3 = second(2), second(3)
    a2 = dd_sub(dd_sub(dd_div(t3, t2), a1), theta)
    b2 = dd_div(t2, s[1])
    a0, a1, a2, b1, b2 = theta[0], a1[0], a2[0], b1[0], b2[0]
    d0 = a0
    d1 = a1 - b1 / d0
    d2 = a2 - b2 / d1
    y2 = 1.0 / (d0 * d1 * d2)
    y1 = (-1.0 / d0 - b2 * y2) / d1
    y0 = (1.0 - b1 * y1) / d0
    c2 = y2
    c1 = y1 - (a0 + a1) * y2
    c0 = y0 - a0 * y1 + (a0 * a1 - b1) * y2
    return c0, c1, c2


def spot_of(x, y=0):
    return pl.multiple_of((x + 2) * PITCH + LOW, 8) + y


def zero_edges(w):
    z8 = jnp.zeros((8, BZ), F32)
    for t in range(2 * PITCH // 8):
        w[pl.ds(8 * t, 8), :] = z8
        w[pl.ds(ROWS - LOW - 2 * PITCH + LOW + 8 * t, 8), :] = z8

    def body(x, carry):
        w[pl.ds(pl.multiple_of((x + 2) * PITCH, 8), 8), :] = z8
        return carry

    lax.fori_loop(0, BX + 1, body, 0, unroll=5)


def krylov(
    load, stiff, w0, w1, w2, coef, fault_sum,
    bs, minv, ypack, zpack, edge, trac,
    hx, hy, hz, fault, part_a, cross_sum, band, even, odd,
    in_sem, xs_sem, xr_sem, ys_sem, yr_sem, zs_sem, zr_sem, fs_sem, fr_sem, rs_sem, rr_sem, token,
):
    gx, gy, gz = (lax.axis_index(a) for a in ("gx", "gy", "gz"))
    nx, ny, nz = (lax.axis_size(a) for a in ("gx", "gy", "gz"))
    lane = lax.broadcasted_iota(jnp.int32, (8, BZ), 1)
    row = lax.broadcasted_iota(jnp.int32, (8, BZ), 0)
    place = (lane + 2) & 3
    halo_here = (place >> 1) == (1 - gz)
    packs = (BX // SLOTS) * TILES
    zero = jnp.zeros((8, BZ), F32)

    regions = [
        (0, 2, 0, BY), (BX - 2, BX, 0, BY), (2, BX - 2, 0, 8), (2, BX - 2, BY - 8, BY)
    ]
    cuts = [2 + (BX - 4) * i // INNER for i in range(INNER + 1)]
    regions += [(lo, hi, 8, BY - 8) for lo, hi in zip(cuts, cuts[1:])]
    for n, (xa, xb, ya, yb) in enumerate(regions):
        part = (pl.ds(xa, xb - xa), pl.ds(ya, yb - ya))
        for i, source in enumerate((load, stiff)):
            pltpu.make_async_copy(source.at[part], bs.at[(i,) + part], in_sem.at[n]).start()

    barrier = pltpu.get_barrier_semaphore()
    side_x = 4 if nx % 4 == 0 else nx
    offsets = [
        (dy, dx, dz, dc)
        for dy in range(nx // side_x) for dx in range(side_x) for dz in range(ny) for dc in range(nz)
    ]

    def hops(o):
        sizes = (nx // side_x, side_x, ny)
        return sum(min(d, n - d) for d, n in zip(o, sizes)) + 0.5 * o[3]

    offsets = sorted(offsets, key=hops, reverse=True)[:-1]
    everyone = [
        (
            lax.rem(gx // side_x + dy, nx // side_x) * side_x + lax.rem(gx + dx, side_x),
            lax.rem(gy + dz, ny),
            lax.rem(gz + dc, nz),
        )
        for dy, dx, dz, dc in offsets
    ]
    has_x = (gx > 0, gx < nx - 1)
    has_y = (gy > 0, gy < ny - 1)

    def one(flag):
        return jnp.where(flag, 1, 0)

    def reach(distances):
        return [
            pair
            for n in distances
            for pair in ((gx >= n, gx - n), (gx + n < nx, gx + n))
        ]

    def tell(sem, distances):
        for there, target in reach(distances):
            @pl.when(there)
            def _(target=target):
                pl.semaphore_signal(sem, inc=1, device_id=(target, gy, gz), device_id_type=MESH)

    def hear(sem, distances):
        count = sum(one(there) for there, _ in reach(distances))

        @pl.when(count > 0)
        def _():
            pl.semaphore_wait(sem, count)

    near, far = (1, 2, 3), (4, 8, 12)
    tell(barrier, near + far)
    column = [
        (gx, lax.rem(gy + dz, ny), lax.rem(gz + dc, nz))
        for dz in range(ny) for dc in range(nz) if dz or dc
    ]
    for device in column:
        pl.semaphore_signal(barrier, inc=1, device_id=device, device_id_type=MESH)

    for w in (w0, w1, w2):
        zero_edges(w)

    at_row = lax.rem(lax.broadcasted_iota(jnp.int32, (3 * BZ, BZ), 0), BZ)
    gap = jnp.abs(at_row - lax.broadcasted_iota(jnp.int32, (3 * BZ, BZ), 1))
    band[...] = jnp.where(gap == 1, 16.0, jnp.where(gap == 2, -1.0, 0.0)).astype(BF16)

    def remote(src, dst, send, recv, device):
        return pltpu.make_async_remote_copy(
            src_ref=src, dst_ref=dst, send_sem=send, recv_sem=recv,
            device_id=device, device_id_type=MESH,
        )

    partner = (gx, gy, 1 - gz)
    half = BY // 2

    def x_sent(k, side, h):
        return k < 2 or h == side

    def x_send(w, k, side, h):
        device = (gx - 1 if side == 0 else gx + 1, gy, gz)
        for n in range(2):
            plane = n if side == 0 else BX - 2 + n
            remote(
                w.at[pl.ds(spot_of(plane, h * half), half), :], hx.at[k, 1 - side, h, n],
                xs_sem.at[k, side], xr_sem.at[k, 1 - side, h], device,
            ).start()

    def x_arrived(k, side, h):
        land = hx.at[k, side, h]
        remote(land, land, xs_sem.at[k, side], xr_sem.at[k, side, h], partner).wait_recv()

    def y_copy(k, side):
        strips = pl.ds(0, BX) if k < 2 else pl.ds(side * (BX // 2), BX // 2)
        return remote(
            ypack.at[k, side, :, strips, :], hy.at[k, 1 - side, :, strips, :],
            ys_sem.at[k, side], yr_sem.at[k, 1 - side],
            (gx, gy - 1 if side == 0 else gy + 1, gz),
        )

    def z_copy(k):
        return remote(zpack.at[k], hz.at[k], zs_sem.at[0], zr_sem.at[k], partner)

    near_fault = (gy == ny // 2 - 1) | (gy == ny // 2)
    source = gy - (ny // 2 - 1)
    low_side = jnp.where(gy == ny // 2, 1.0, 0.0)
    high_side = jnp.where(gy == ny // 2 - 1, 1.0, 0.0)
    own_rows = BX // ny

    def send_fault():
        @pl.when(near_fault)
        def _():
            for r in range(1, ny):
                owner = lax.rem(gy + r, ny)
                remote(
                    trac.at[:, pl.ds(pl.multiple_of(owner * own_rows, 8), own_rows), :],
                    fault.at[source], fs_sem.at[0], fr_sem.at[source], (gx, owner, gz),
                ).start()
            for k in range(3):
                for i in range(own_rows // 8):
                    fault[source, k, pl.ds(8 * i, 8), :] = trac[
                        k, pl.ds(pl.multiple_of(gy * own_rows + 8 * i, 8), 8), :
                    ]

    def send_y(w, k):
        for j in range(STRIPS):
            strip = []
            for n, y in enumerate((0, 1, BY - 2, BY - 1)):
                v = w[pl.ds(spot_of(8 * j, y), 8, stride=PITCH), :]
                ypack[k, n // 2, n % 2, pl.ds(8 * j, 8), :] = v
                strip.append(v)
            term = low_side * (27.0 * strip[0] - strip[1]) + high_side * (strip[2] - 27.0 * strip[3])
            trac[k, pl.ds(8 * j, 8), :] = term / 24.0
        for side in range(2):
            @pl.when(has_y[side])
            def _(side=side):
                y_copy(k, side).start()

    def pack(w, k, i):
        for t in range(TILES):
            packed = zero
            for q in range(SLOTS):
                mask = ((lane + 2 - 4 * q) & (BZ - 1)) < 4
                tile = w[pl.ds(spot_of(i * SLOTS + q, 8 * t), 8), :]
                packed = jnp.where(mask, pltpu.roll(tile, 4 * q, 1), packed)
            zpack[k, i * TILES + t] = packed

    mu0 = zero
    for n, (xa, xb, ya, yb) in enumerate(regions):
        part = (slice(None), pl.ds(xa, xb - xa), pl.ds(ya, yb - ya))
        pltpu.make_async_copy(bs.at[part], bs.at[part], in_sem.at[n]).wait()

        def start_plane(x, acc):
            for t in range(ya // 8, yb // 8):
                at = pl.ds(8 * t, 8)
                b = bs[0, x, at, :]
                inverse = 1.0 / (7.5 + bs[1, x, at, :])
                w = b * inverse
                w0[pl.ds(spot_of(x, 8 * t), 8), :] = w
                minv[pl.ds(pl.multiple_of(x * BY, 8) + 8 * t, 8), :] = inverse * (1.0 / 12.0)
                acc = acc + b * w
            return acc

        count = xb - xa
        tiles = (yb - ya) // 8
        unroll = max(u for u in range(1, count + 1) if count % u == 0 and u * tiles <= 60 or u == 1)
        mu0 = lax.fori_loop(xa, xb, start_plane, mu0, unroll=unroll)
        if n == 1:
            pl.semaphore_wait(
                barrier, len(column) + sum(one(there) for there, _ in reach(near + far))
            )
            for side in range(2):
                @pl.when(has_x[side])
                def _(side=side):
                    for h in range(2):
                        x_send(w0, 0, side, h)
            tell(token.at[0], near)
        if n == 3:
            send_y(w0, 0)

    def edge_terms(d):
        near = jnp.where(place == 1, pltpu.roll(d, BZ - 1, 1), pltpu.roll(d, 1, 1))
        near = jnp.where((place == 1) | (place == 2), near, 0.0)
        return 16.0 * near - jnp.where(place < 2, pltpu.roll(d, BZ - 2, 1), pltpu.roll(d, 2, 1))

    def along_z(w, x):
        c = w[pl.ds(spot_of(x), GROUP * PITCH), :]
        high = c.astype(BF16)
        rest = c - high.astype(F32)
        middle = rest.astype(BF16)
        low = (rest - middle.astype(F32)).astype(BF16)
        return jnp.dot(
            jnp.concatenate([high, middle, low], axis=1), band[...], preferred_element_type=F32
        )

    edge_mask = ((lane + 2) & (BZ - 1)) < 4

    def z_term(x, t):
        turn = lax.rem(BZ - 4 * lax.rem(x, SLOTS), BZ)
        return jnp.where(edge_mask, pltpu.roll(edge[(x // SLOTS) * TILES + t], turn, 1), 0.0)

    def bulk(w, out, k, init, z_fix=None):
        def group(g, zz, acc, with_z):
            for t in range(TILES):
                def at(p, dy):
                    return w[pl.ds(spot_of(g * GROUP, 8 * t) + (p * PITCH + dy), 8), :]

                line = [at(p, 0) for p in range(-2, GROUP + 2)]
                for p in range(GROUP):
                    x = g * GROUP + p
                    near = (line[p + 3] + line[p + 1]) + (at(p, 1) + at(p, -1))
                    far = (line[p + 4] + line[p]) + (at(p, 2) + at(p, -2))
                    n = (16.0 * near - far) + zz[pl.ds(p * PITCH + 8 * t, 8), :]
                    if with_z:
                        n = n + z_term(x, t)
                    acc = out(x, t, line[p + 2], n, acc)
            return acc

        groups = BX // GROUP
        even[...] = along_z(w, 0)

        pairs = groups // 2
        ends = BX // SLOTS
        inside = (pairs - ends) * 2 * GROUP // ends

        def pair(i, acc, with_z=False):
            odd[...] = along_z(w, (2 * i + 1) * GROUP)
            acc = group(2 * i, even, acc, with_z)
            even[...] = along_z(w, jnp.minimum(2 * i + 2, groups - 1) * GROUP)
            return group(2 * i + 1, odd, acc, with_z)

        def first_pair(i, acc):
            pack(w, k, i)
            return pair(i, acc)

        def last_pair(i, acc):
            for p in range(inside):
                for t in range(TILES):
                    z_fix((i - (pairs - ends)) * inside + p, t)
            return pair(i, acc, True)

        acc = lax.fori_loop(0, ends, first_pair, init)
        z_copy(k).start()
        acc = lax.fori_loop(ends, pairs - ends, pair, acc)
        z_copy(k).wait_recv()
        if k == 2:
            return lax.fori_loop(pairs - ends, pairs, pair, acc)
        hear(token.at[k], near if k == 0 else far)
        if k == 0:
            tell(token.at[1], far)
        for i in range(packs):
            edge[i] = edge_terms(jnp.where(halo_here, hz[k, i], 0.0))
        return lax.fori_loop(pairs - ends, pairs, last_pair, acc)

    def fixes(k, apply_x, apply_y, then):
        whole = k < 2
        for side in range(2):
            @pl.when(has_y[side])
            def _(side=side):
                y_copy(k, 1 - side).wait_recv()
                inner, outer = (1, 0) if side == 0 else (0, 1)
                first, second = (0, 1) if side == 0 else (BY - 1, BY - 2)
                span = range(STRIPS)
                if not whole:
                    span = range((1 - side) * STRIPS // 2, (2 - side) * STRIPS // 2)
                for j in span:
                    at = pl.ds(8 * j, 8)
                    close = hy[k, side, inner, at, :]
                    apply_y(j, first, 16.0 * close - hy[k, side, outer, at, :])
                    apply_y(j, second, -close)
        for h in range(2):
            for side in range(2):
                if not x_sent(k, 1 - side, h):
                    continue

                @pl.when(has_x[side])
                def _(side=side, h=h):
                    x_arrived(k, side, h)
                    inner, outer = (1, 0) if side == 0 else (0, 1)
                    first, second = (0, 1) if side == 0 else (BX - 1, BX - 2)
                    for u in range(TILES // 2):
                        t = h * (TILES // 2) + u
                        close = hx[k, side, h, inner, pl.ds(8 * u, 8), :]
                        distant = hx[k, side, h, outer, pl.ds(8 * u, 8), :]
                        apply_x(first, t, 16.0 * close - distant)
                        apply_x(second, t, -close)
                    then(side, h)

    def basis_step(w, new, k, moments, init):
        def out(x, t, c, n, acc):
            new[pl.ds(spot_of(x, 8 * t), 8), :] = (
                c - minv[pl.ds(pl.multiple_of(x * BY, 8) + 8 * t, 8), :] * n
            )
            return moments(x, t, c, acc)

        def z_fix(x, t):
            at = pl.ds(spot_of(x, 8 * t), 8)
            m = minv[pl.ds(pl.multiple_of(x * BY, 8) + 8 * t, 8), :]
            new[at, :] = new[at, :] - m * z_term(x, t)

        sums = bulk(w, out, k, init, z_fix)

        def apply_x(x, t, n):
            at = pl.ds(spot_of(x, 8 * t), 8)
            new[at, :] = new[at, :] - minv[pl.ds(x * BY + 8 * t, 8), :] * n

        def apply_y(j, y, n):
            at = pl.ds(spot_of(8 * j, y), 8, stride=PITCH)
            new[at, :] = new[at, :] - minv[pl.ds(8 * j * BY + y, 8, stride=BY), :] * n

        def then(side, h):
            if x_sent(k + 1, side, h):
                x_send(new, k + 1, side, h)

        fixes(k, apply_x, apply_y, then)
        send_y(new, k + 1)
        return sums

    basis_step(w0, w1, 0, lambda x, t, c, acc: acc, 0)

    def first_moments(x, t, c, acc):
        at = pl.ds(8 * t, 8)
        return (acc[0] + bs[0, x, at, :] * c, acc[1] + ((7.5 + bs[1, x, at, :]) * c) * c)

    mu1, mu2 = basis_step(w1, w2, 1, first_moments, (zero, zero))
    send_fault()

    def last(x, t, c, n, acc):
        d = (7.5 + bs[1, x, pl.ds(8 * t, 8), :]) * c
        return (
            acc[0] + d * w1[pl.ds(spot_of(x, 8 * t), 8), :],
            acc[1] + d * c,
            acc[2] + c * (d - n * (1.0 / 12.0)),
        )

    mu3, mu4, mu5 = bulk(w2, last, 2, (zero, zero, zero))
    cross_sum[...] = zero

    def cross_x(x, t, n):
        cross_sum[...] = cross_sum[...] + w2[pl.ds(spot_of(x, 8 * t), 8), :] * n

    def cross_y(j, y, n):
        cross_sum[...] = cross_sum[...] + w2[pl.ds(spot_of(8 * j, y), 8, stride=PITCH), :] * n

    crossing = zero
    for i in range(packs):
        crossing = crossing + zpack[2, i] * edge_terms(jnp.where(halo_here, hz[2, i], 0.0))
    fixes(2, cross_x, cross_y, lambda side, h: None)
    mu5 = mu5 - (2.0 * cross_sum[...] + crossing) * (1.0 / 12.0)

    local = zero
    for j, m in enumerate((mu0, mu1, mu2, mu3, mu4, mu5)):
        local = jnp.where(row == j, jnp.sum(m, axis=0, keepdims=True), local)
    local = jnp.where(lane == row, jnp.sum(local, axis=1, keepdims=True), 0.0)
    local = jnp.sum(local, axis=0, keepdims=True)

    last_slot = len(everyone)
    part_a[last_slot] = local
    for r, device in enumerate(everyone):
        remote(part_a.at[last_slot], part_a.at[r], rs_sem.at[0], rr_sem.at[0], device).start()
    land = part_a.at[pl.ds(0, last_slot)]
    remote(land, land, rs_sem.at[0], rr_sem.at[0], partner).wait_recv()

    def tree(terms):
        while len(terms) > 1:
            pairs = []
            for a, b in zip(terms[::2], terms[1::2]):
                h, e = two_sum(a[0], b[0])
                pairs.append((h, e + (a[1] + b[1])))
            terms = pairs
        return terms[0]

    rows = [
        (part_a[pl.ds(8 * i, 8)].reshape(8, BZ), zero) for i in range((last_slot + 1) // 8)
    ]
    high, low = tree(rows)
    total = tree([(high[i : i + 1], low[i : i + 1]) for i in range(8)])

    mu = []
    for j in range(6):
        mu.append(norm(*(jnp.broadcast_to(v[:, j : j + 1], (8, BZ)) for v in total)))
    for j, c in enumerate(coefficients(mu)):
        coef[j] = c

    for s in range(2):
        @pl.when(gy != ny // 2 - 1 + s)
        def _(s=s):
            land = fault.at[s]
            remote(land, land, fs_sem.at[0], fr_sem.at[s], partner).wait_recv()
    for k in range(3):
        for i in range(own_rows // 8):
            at = pl.ds(8 * i, 8)
            fault_sum[k, at, :] = fault[0, k, at, :] + fault[1, k, at, :]

    remote(land, land, rs_sem.at[0], rr_sem.at[0], partner).wait_send()
    remote(zpack, hz, zs_sem.at[0], zr_sem.at[0], partner).wait_send()
    for k in range(3):
        for side in range(2):
            @pl.when(has_x[side])
            def _(k=k, side=side):
                sent = hx.at[k, side] if k < 2 else hx.at[k, side, 0]
                remote(sent, sent, xs_sem.at[k, side], xr_sem.at[k, side, 0], partner).wait_send()
            @pl.when(has_y[side])
            def _(k=k, side=side):
                y_copy(k, side).wait_send()

    @pl.when(near_fault)
    def _():
        sent = trac.at[:, pl.ds(0, (ny - 1) * own_rows), :]
        remote(sent, sent, fs_sem.at[0], fr_sem.at[0], partner).wait_send()


def combine(w0, w1, w2, coef, fault_sum, prestress, state, normal, u, slip, buf, sem):
    c0, c1, c2 = coef[0], coef[1], coef[2]
    step = BX // CHUNKS
    copies = []
    for i in range(CHUNKS):
        def plane(x, carry):
            for t in range(TILES):
                at = pl.ds(spot_of(x, 8 * t), 8)
                buf[x, pl.ds(8 * t, 8), :] = (c0 * w0[at, :] + c1 * w1[at, :]) + c2 * w2[at, :]
            return carry

        lax.fori_loop(i * step, (i + 1) * step, plane, 0)
        part = pl.ds(i * step, step)
        copy = pltpu.make_async_copy(buf.at[part], u.at[part], sem.at[i])
        copy.start()
        copies.append(copy)
    for i in range(slip.shape[0] // 8):
        at = pl.ds(8 * i, 8)
        traction = (c0 * fault_sum[0, at, :] + c1 * fault_sum[1, at, :]) + c2 * fault_sum[2, at, :]
        x = (prestress[at, :] + 2.0 * traction) / normal[at, :]
        half = 0.6931471805599453
        large = jnp.exp(x - half) - jnp.exp(-x - half)
        q = x * x
        small = x * (1.0 + q * (1 / 6 + q * (1 / 120 + q * (1 / 5040 + q * (1 / 362880 + q / 39916800)))))
        sinh = jnp.where(jnp.abs(x) < 1.0, small, large)
        slip[at, :] = jnp.exp(-state[at, :]) * sinh
    for copy in copies:
        copy.wait()


def per_device(load, stiffness, prestress, state_var, normal_a):
    vmem = pl.BlockSpec(memory_space=pltpu.VMEM)
    hbm = pl.BlockSpec(memory_space=pl.ANY)
    ny = lax.axis_size("gy")
    own = BX // ny
    group = ny * lax.axis_size("gz")
    nx = lax.axis_size("gx")
    big = (ROWS, BZ)
    packs = (BX // SLOTS) * TILES
    DMA = pltpu.SemaphoreType.DMA
    outs = pl.pallas_call(
        krylov,
        out_shape=[
            pltpu.VMEM(big, F32), pltpu.VMEM(big, F32), pltpu.VMEM(big, F32),
            pltpu.VMEM((3, 8, BZ), F32), pltpu.VMEM((3, own, BZ), F32),
        ],
        in_specs=[pl.BlockSpec(memory_space=pltpu.HBM)] * 2,
        out_specs=[vmem] * 5,
        scratch_shapes=[
            pltpu.VMEM((2, BX, BY, BZ), F32),
            pltpu.VMEM((BX * BY, BZ), F32),
            pltpu.VMEM((3, 2, 2, BX, BZ), F32),
            pltpu.VMEM((3, packs, 8, BZ), F32),
            pltpu.VMEM((packs, 8, BZ), F32),
            pltpu.VMEM((3, BX, BZ), F32),
            pltpu.VMEM((3, 2, 2, 2, BY // 2, BZ), F32),
            pltpu.VMEM((3, 2, 2, BX, BZ), F32),
            pltpu.VMEM((3, packs, 8, BZ), F32),
            pltpu.VMEM((2, 3, own, BZ), F32),
            pltpu.VMEM((group * nx, 1, BZ), F32),
            pltpu.VMEM((8, BZ), F32),
            pltpu.VMEM((3 * BZ, BZ), BF16),
            pltpu.VMEM((GROUP * PITCH, BZ), F32),
            pltpu.VMEM((GROUP * PITCH, BZ), F32),
            DMA((4 + INNER,)),
            DMA((3, 2)), DMA((3, 2, 2)), DMA((3, 2)), DMA((3, 2)), DMA((1,)), DMA((3,)),
            DMA((1,)), DMA((2,)),
            DMA((1,)), DMA((1,)),
            pltpu.SemaphoreType.REGULAR((2,)),
        ],
        compiler_params=pltpu.CompilerParams(
            collective_id=0, has_side_effects=True, vmem_limit_bytes=55 * 2**20
        ),
        name="krylov",
    )(load, stiffness)
    return pl.pallas_call(
        combine,
        out_shape=[
            jax.ShapeDtypeStruct(load.shape, F32),
            jax.ShapeDtypeStruct(prestress.shape, F32),
        ],
        in_specs=[vmem] * 8,
        out_specs=[hbm, vmem],
        scratch_shapes=[pltpu.VMEM((BX, BY, BZ), F32), DMA((CHUNKS,))],
        compiler_params=pltpu.CompilerParams(vmem_limit_bytes=24 * 2**20),
        name="combine",
    )(*outs, prestress, state_var, normal_a)


def solution(mesh):
    block = P("gx", "gy", "gz")
    fault = P(("gx", "gy"), "gz")
    return jax.shard_map(
        per_device,
        mesh=mesh,
        in_specs=(block, block, fault, fault, fault),
        out_specs=(block, fault),
        check_vma=False,
    )
```

```python
import functools

import jax
import jax.numpy as jnp
from jax import lax
from jax.experimental import pallas as pl
from jax.experimental.pallas import tpu as pltpu
from jax.sharding import PartitionSpec as P

MESH = pl.DeviceIdType.MESH
F32 = jnp.float32
BF16 = jnp.bfloat16
BX, BY, BZ = 64, 64, 128
LOW = 8
PITCH = BY + LOW
ROWS = (BX + 4) * PITCH + LOW
TILES = BY // 8
STRIPS = BX // 8
CHUNKS = 8
INNER = 3
SLOTS = 32
GROUP = 4
UNROLL = 8


def two_sum(a, b):
    s = a + b
    t = s - a
    return s, (a - (s - t)) + (b - t)


def split(a):
    t = a * 4097.0
    high = t - (t - a)
    return high, a - high


def two_prod(a, b):
    p = a * b
    ah, al = split(a)
    bh, bl = split(b)
    return p, ((ah * bh - p) + ah * bl + al * bh) + al * bl


def norm(h, l):
    s = h + l
    return s, l - (s - h)


def dd_sub(a, b):
    s, e = two_sum(a[0], -b[0])
    return norm(s, e + (a[1] - b[1]))


def dd_mul(a, b):
    p, e = two_prod(a[0], b[0])
    return norm(p, e + (a[0] * b[1] + a[1] * b[0]))


def dd_div(a, b):
    q = a[0] / b[0]
    p, e = two_prod(q, b[0])
    r = ((a[0] - p) - e) + (a[1] - q * b[1])
    return norm(q, r / b[0])


def coefficients(mu):
    theta = dd_div(mu[1], mu[0])
    s = [None] + [dd_sub(mu[j + 1], dd_mul(theta, mu[j])) for j in range(1, 5)]
    a1 = dd_sub(dd_div(s[2], s[1]), theta)
    b1 = dd_div(s[1], mu[0])

    def second(j):
        return dd_sub(dd_sub(s[j + 1], dd_mul(a1, s[j])), dd_mul(b1, mu[j]))

    t2, t3 = second(2), second(3)
    a2 = dd_sub(dd_sub(dd_div(t3, t2), a1), theta)
    b2 = dd_div(t2, s[1])
    a0, a1, a2, b1, b2 = theta[0], a1[0], a2[0], b1[0], b2[0]
    d0 = a0
    d1 = a1 - b1 / d0
    d2 = a2 - b2 / d1
    y2 = 1.0 / (d0 * d1 * d2)
    y1 = (-1.0 / d0 - b2 * y2) / d1
    y0 = (1.0 - b1 * y1) / d0
    c2 = y2
    c1 = y1 - (a0 + a1) * y2
    c0 = y0 - a0 * y1 + (a0 * a1 - b1) * y2
    return c0, c1, c2


def spot_of(x, y=0):
    return pl.multiple_of((x + 2) * PITCH + LOW, 8) + y


def zero_edges(w):
    z8 = jnp.zeros((8, BZ), F32)
    for t in range(2 * PITCH // 8):
        w[pl.ds(8 * t, 8), :] = z8
        w[pl.ds(ROWS - LOW - 2 * PITCH + LOW + 8 * t, 8), :] = z8

    def body(x, carry):
        w[pl.ds(pl.multiple_of((x + 2) * PITCH, 8), 8), :] = z8
        return carry

    lax.fori_loop(0, BX + 1, body, 0, unroll=5)


def krylov(
    load, stiff, w0, w1, w2, coef, fault_sum,
    bs, minv, ypack, zpack, edge, trac,
    hx, hy, hz, fault, part_a, cross_sum, band, even, odd,
    in_sem, xs_sem, xr_sem, ys_sem, yr_sem, zs_sem, zr_sem, fs_sem, fr_sem, rs_sem, rr_sem, token,
):
    gx, gy, gz = (lax.axis_index(a) for a in ("gx", "gy", "gz"))
    nx, ny, nz = (lax.axis_size(a) for a in ("gx", "gy", "gz"))
    lane = lax.broadcasted_iota(jnp.int32, (8, BZ), 1)
    row = lax.broadcasted_iota(jnp.int32, (8, BZ), 0)
    place = (lane + 2) & 3
    halo_here = (place >> 1) == (1 - gz)
    packs = (BX // SLOTS) * TILES
    zero = jnp.zeros((8, BZ), F32)

    regions = [
        (0, 2, 0, BY), (BX - 2, BX, 0, BY), (2, BX - 2, 0, 8), (2, BX - 2, BY - 8, BY)
    ]
    cuts = [2 + (BX - 4) * i // INNER for i in range(INNER + 1)]
    regions += [(lo, hi, 8, BY - 8) for lo, hi in zip(cuts, cuts[1:])]
    for n, (xa, xb, ya, yb) in enumerate(regions):
        part = (pl.ds(xa, xb - xa), pl.ds(ya, yb - ya))
        for i, source in enumerate((load, stiff)):
            pltpu.make_async_copy(source.at[part], bs.at[(i,) + part], in_sem.at[n]).start()

    barrier = pltpu.get_barrier_semaphore()
    side_x = 4 if nx % 4 == 0 else nx
    offsets = [
        (dy, dx, dz, dc)
        for dy in range(nx // side_x) for dx in range(side_x) for dz in range(ny) for dc in range(nz)
    ]

    def hops(o):
        sizes = (nx // side_x, side_x, ny)
        return sum(min(d, n - d) for d, n in zip(o, sizes)) + 0.5 * o[3]

    offsets = sorted(offsets, key=hops, reverse=True)[:-1]
    everyone = [
        (
            lax.rem(gx // side_x + dy, nx // side_x) * side_x + lax.rem(gx + dx, side_x),
            lax.rem(gy + dz, ny),
            lax.rem(gz + dc, nz),
        )
        for dy, dx, dz, dc in offsets
    ]
    has_x = (gx > 0, gx < nx - 1)
    has_y = (gy > 0, gy < ny - 1)

    def one(flag):
        return jnp.where(flag, 1, 0)

    def reach(distances):
        return [
            pair
            for n in distances
            for pair in ((gx >= n, gx - n), (gx + n < nx, gx + n))
        ]

    def tell(sem, distances):
        for there, target in reach(distances):
            @pl.when(there)
            def _(target=target):
                pl.semaphore_signal(sem, inc=1, device_id=(target, gy, gz), device_id_type=MESH)

    def hear(sem, distances):
        count = sum(one(there) for there, _ in reach(distances))

        @pl.when(count > 0)
        def _():
            pl.semaphore_wait(sem, count)

    near, far = (1, 2, 3), (4, 8, 12)
    tell(barrier, near + far)
    column = [
        (gx, lax.rem(gy + dz, ny), lax.rem(gz + dc, nz))
        for dz in range(ny) for dc in range(nz) if dz or dc
    ]
    for device in column:
        pl.semaphore_signal(barrier, inc=1, device_id=device, device_id_type=MESH)

    for w in (w0, w1, w2):
        zero_edges(w)

    at_row = lax.rem(lax.broadcasted_iota(jnp.int32, (3 * BZ, BZ), 0), BZ)
    gap = jnp.abs(at_row - lax.broadcasted_iota(jnp.int32, (3 * BZ, BZ), 1))
    band[...] = jnp.where(gap == 1, 16.0, jnp.where(gap == 2, -1.0, 0.0)).astype(BF16)

    def remote(src, dst, send, recv, device):
        return pltpu.make_async_remote_copy(
            src_ref=src, dst_ref=dst, send_sem=send, recv_sem=recv,
            device_id=device, device_id_type=MESH,
        )

    partner = (gx, gy, 1 - gz)
    half = BY // 2

    def x_sent(k, side, h):
        return k < 2 or h == side

    def x_send(w, k, side, h):
        device = (gx - 1 if side == 0 else gx + 1, gy, gz)
        for n in range(2):
            plane = n if side == 0 else BX - 2 + n
            remote(
                w.at[pl.ds(spot_of(plane, h * half), half), :], hx.at[k, 1 - side, h, n],
                xs_sem.at[k, side], xr_sem.at[k, 1 - side, h], device,
            ).start()

    def x_arrived(k, side, h):
        land = hx.at[k, side, h]
        remote(land, land, xs_sem.at[k, side], xr_sem.at[k, side, h], partner).wait_recv()

    def y_copy(k, side):
        strips = pl.ds(0, BX) if k < 2 else pl.ds(side * (BX // 2), BX // 2)
        return remote(
            ypack.at[k, side, :, strips, :], hy.at[k, 1 - side, :, strips, :],
            ys_sem.at[k, side], yr_sem.at[k, 1 - side],
            (gx, gy - 1 if side == 0 else gy + 1, gz),
        )

    def z_copy(k):
        return remote(zpack.at[k], hz.at[k], zs_sem.at[0], zr_sem.at[k], partner)

    near_fault = (gy == ny // 2 - 1) | (gy == ny // 2)
    source = gy - (ny // 2 - 1)
    low_side = jnp.where(gy == ny // 2, 1.0, 0.0)
    high_side = jnp.where(gy == ny // 2 - 1, 1.0, 0.0)
    own_rows = BX // ny

    def send_fault():
        @pl.when(near_fault)
        def _():
            for r in range(1, ny):
                owner = lax.rem(gy + r, ny)
                remote(
                    trac.at[:, pl.ds(pl.multiple_of(owner * own_rows, 8), own_rows), :],
                    fault.at[source], fs_sem.at[0], fr_sem.at[source], (gx, owner, gz),
                ).start()
            for k in range(3):
                for i in range(own_rows // 8):
                    fault[source, k, pl.ds(8 * i, 8), :] = trac[
                        k, pl.ds(pl.multiple_of(gy * own_rows + 8 * i, 8), 8), :
                    ]

    def send_y(w, k):
        for j in range(STRIPS):
            strip = []
            for n, y in enumerate((0, 1, BY - 2, BY - 1)):
                v = w[pl.ds(spot_of(8 * j, y), 8, stride=PITCH), :]
                ypack[k, n // 2, n % 2, pl.ds(8 * j, 8), :] = v
                strip.append(v)
            term = low_side * (27.0 * strip[0] - strip[1]) + high_side * (strip[2] - 27.0 * strip[3])
            trac[k, pl.ds(8 * j, 8), :] = term / 24.0
        for side in range(2):
            @pl.when(has_y[side])
            def _(side=side):
                y_copy(k, side).start()

    def pack(w, k, i):
        for t in range(TILES):
            packed = zero
            for q in range(SLOTS):
                mask = ((lane + 2 - 4 * q) & (BZ - 1)) < 4
                tile = w[pl.ds(spot_of(i * SLOTS + q, 8 * t), 8), :]
                packed = jnp.where(mask, pltpu.roll(tile, 4 * q, 1), packed)
            zpack[k, i * TILES + t] = packed

    mu0 = zero
    for n, (xa, xb, ya, yb) in enumerate(regions):
        part = (slice(None), pl.ds(xa, xb - xa), pl.ds(ya, yb - ya))
        pltpu.make_async_copy(bs.at[part], bs.at[part], in_sem.at[n]).wait()

        def start_plane(x, acc):
            for t in range(ya // 8, yb // 8):
                at = pl.ds(8 * t, 8)
                b = bs[0, x, at, :]
                inverse = 1.0 / (7.5 + bs[1, x, at, :])
                w = b * inverse
                w0[pl.ds(spot_of(x, 8 * t), 8), :] = w
                minv[pl.ds(pl.multiple_of(x * BY, 8) + 8 * t, 8), :] = inverse * (1.0 / 12.0)
                acc = acc + b * w
            return acc

        count = xb - xa
        tiles = (yb - ya) // 8
        unroll = max(u for u in range(1, count + 1) if count % u == 0 and u * tiles <= 60 or u == 1)
        mu0 = lax.fori_loop(xa, xb, start_plane, mu0, unroll=unroll)
        if n == 1:
            pl.semaphore_wait(
                barrier, len(column) + sum(one(there) for there, _ in reach(near + far))
            )
            for side in range(2):
                @pl.when(has_x[side])
                def _(side=side):
                    for h in range(2):
                        x_send(w0, 0, side, h)
            tell(token.at[0], near)
        if n == 3:
            send_y(w0, 0)

    def edge_terms(d):
        near = jnp.where(place == 1, pltpu.roll(d, BZ - 1, 1), pltpu.roll(d, 1, 1))
        near = jnp.where((place == 1) | (place == 2), near, 0.0)
        return 16.0 * near - jnp.where(place < 2, pltpu.roll(d, BZ - 2, 1), pltpu.roll(d, 2, 1))

    def along_z(w, x):
        c = w[pl.ds(spot_of(x), GROUP * PITCH), :]
        high = c.astype(BF16)
        rest = c - high.astype(F32)
        middle = rest.astype(BF16)
        low = (rest - middle.astype(F32)).astype(BF16)
        return jnp.dot(
            jnp.concatenate([high, middle, low], axis=1), band[...], preferred_element_type=F32
        )

    edge_mask = ((lane + 2) & (BZ - 1)) < 4

    def z_term(x, t):
        turn = lax.rem(BZ - 4 * lax.rem(x, SLOTS), BZ)
        return jnp.where(edge_mask, pltpu.roll(edge[(x // SLOTS) * TILES + t], turn, 1), 0.0)

    def bulk(w, out, k, init, z_fix=None):
        def group(g, zz, acc, with_z):
            for t in range(TILES):
                def at(p, dy):
                    return w[pl.ds(spot_of(g * GROUP, 8 * t) + (p * PITCH + dy), 8), :]

                line = [at(p, 0) for p in range(-2, GROUP + 2)]
                for p in range(GROUP):
                    x = g * GROUP + p
                    near = (line[p + 3] + line[p + 1]) + (at(p, 1) + at(p, -1))
                    far = (line[p + 4] + line[p]) + (at(p, 2) + at(p, -2))
                    n = (16.0 * near - far) + zz[pl.ds(p * PITCH + 8 * t, 8), :]
                    if with_z:
                        n = n + z_term(x, t)
                    acc = out(x, t, line[p + 2], n, acc)
            return acc

        groups = BX // GROUP
        even[...] = along_z(w, 0)

        pairs = groups // 2
        ends = BX // SLOTS
        inside = (pairs - ends) * 2 * GROUP // ends

        def pair(i, acc, with_z=False):
            odd[...] = along_z(w, (2 * i + 1) * GROUP)
            acc = group(2 * i, even, acc, with_z)
            even[...] = along_z(w, jnp.minimum(2 * i + 2, groups - 1) * GROUP)
            return group(2 * i + 1, odd, acc, with_z)

        def first_pair(i, acc):
            pack(w, k, i)
            return pair(i, acc)

        def last_pair(i, acc):
            for p in range(inside):
                for t in range(TILES):
                    z_fix((i - (pairs - ends)) * inside + p, t)
            return pair(i, acc, True)

        acc = lax.fori_loop(0, ends, first_pair, init)
        z_copy(k).start()
        acc = lax.fori_loop(ends, pairs - ends, pair, acc)
        z_copy(k).wait_recv()
        if k == 2:
            return lax.fori_loop(pairs - ends, pairs, pair, acc)
        hear(token.at[k], near if k == 0 else far)
        if k == 0:
            tell(token.at[1], far)
        for i in range(packs):
            edge[i] = edge_terms(jnp.where(halo_here, hz[k, i], 0.0))
        return lax.fori_loop(pairs - ends, pairs, last_pair, acc)

    def fixes(k, apply_x, apply_y, then):
        whole = k < 2
        for side in range(2):
            @pl.when(has_y[side])
            def _(side=side):
                y_copy(k, 1 - side).wait_recv()
                inner, outer = (1, 0) if side == 0 else (0, 1)
                first, second = (0, 1) if side == 0 else (BY - 1, BY - 2)
                span = range(STRIPS)
                if not whole:
                    span = range((1 - side) * STRIPS // 2, (2 - side) * STRIPS // 2)
                for j in span:
                    at = pl.ds(8 * j, 8)
                    close = hy[k, side, inner, at, :]
                    apply_y(j, first, 16.0 * close - hy[k, side, outer, at, :])
                    apply_y(j, second, -close)
        for h in range(2):
            for side in range(2):
                if not x_sent(k, 1 - side, h):
                    continue

                @pl.when(has_x[side])
                def _(side=side, h=h):
                    x_arrived(k, side, h)
                    inner, outer = (1, 0) if side == 0 else (0, 1)
                    first, second = (0, 1) if side == 0 else (BX - 1, BX - 2)
                    for u in range(TILES // 2):
                        t = h * (TILES // 2) + u
                        close = hx[k, side, h, inner, pl.ds(8 * u, 8), :]
                        distant = hx[k, side, h, outer, pl.ds(8 * u, 8), :]
                        apply_x(first, t, 16.0 * close - distant)
                        apply_x(second, t, -close)
                    then(side, h)

    def basis_step(w, new, k, moments, init):
        def out(x, t, c, n, acc):
            new[pl.ds(spot_of(x, 8 * t), 8), :] = (
                c - minv[pl.ds(pl.multiple_of(x * BY, 8) + 8 * t, 8), :] * n
            )
            return moments(x, t, c, acc)

        def z_fix(x, t):
            at = pl.ds(spot_of(x, 8 * t), 8)
            m = minv[pl.ds(pl.multiple_of(x * BY, 8) + 8 * t, 8), :]
            new[at, :] = new[at, :] - m * z_term(x, t)

        sums = bulk(w, out, k, init, z_fix)

        def apply_x(x, t, n):
            at = pl.ds(spot_of(x, 8 * t), 8)
            new[at, :] = new[at, :] - minv[pl.ds(x * BY + 8 * t, 8), :] * n

        def apply_y(j, y, n):
            at = pl.ds(spot_of(8 * j, y), 8, stride=PITCH)
            new[at, :] = new[at, :] - minv[pl.ds(8 * j * BY + y, 8, stride=BY), :] * n

        def then(side, h):
            if x_sent(k + 1, side, h):
                x_send(new, k + 1, side, h)

        fixes(k, apply_x, apply_y, then)
        send_y(new, k + 1)
        return sums

    basis_step(w0, w1, 0, lambda x, t, c, acc: acc, 0)

    def first_moments(x, t, c, acc):
        at = pl.ds(8 * t, 8)
        return (acc[0] + bs[0, x, at, :] * c, acc[1] + ((7.5 + bs[1, x, at, :]) * c) * c)

    mu1, mu2 = basis_step(w1, w2, 1, first_moments, (zero, zero))
    send_fault()

    def last(x, t, c, n, acc):
        d = (7.5 + bs[1, x, pl.ds(8 * t, 8), :]) * c
        return (
            acc[0] + d * w1[pl.ds(spot_of(x, 8 * t), 8), :],
            acc[1] + d * c,
            acc[2] + c * (d - n * (1.0 / 12.0)),
        )

    mu3, mu4, mu5 = bulk(w2, last, 2, (zero, zero, zero))
    cross_sum[...] = zero

    def cross_x(x, t, n):
        cross_sum[...] = cross_sum[...] + w2[pl.ds(spot_of(x, 8 * t), 8), :] * n

    def cross_y(j, y, n):
        cross_sum[...] = cross_sum[...] + w2[pl.ds(spot_of(8 * j, y), 8, stride=PITCH), :] * n

    crossing = zero
    for i in range(packs):
        crossing = crossing + zpack[2, i] * edge_terms(jnp.where(halo_here, hz[2, i], 0.0))
    fixes(2, cross_x, cross_y, lambda side, h: None)
    mu5 = mu5 - (2.0 * cross_sum[...] + crossing) * (1.0 / 12.0)

    local = zero
    for j, m in enumerate((mu0, mu1, mu2, mu3, mu4, mu5)):
        local = jnp.where(row == j, jnp.sum(m, axis=0, keepdims=True), local)
    local = jnp.where(lane == row, jnp.sum(local, axis=1, keepdims=True), 0.0)
    local = jnp.sum(local, axis=0, keepdims=True)

    last_slot = len(everyone)
    part_a[last_slot] = local
    for r, device in enumerate(everyone):
        remote(part_a.at[last_slot], part_a.at[r], rs_sem.at[0], rr_sem.at[0], device).start()
    land = part_a.at[pl.ds(0, last_slot)]
    remote(land, land, rs_sem.at[0], rr_sem.at[0], partner).wait_recv()

    def tree(terms):
        while len(terms) > 1:
            pairs = []
            for a, b in zip(terms[::2], terms[1::2]):
                h, e = two_sum(a[0], b[0])
                pairs.append((h, e + (a[1] + b[1])))
            terms = pairs
        return terms[0]

    rows = [
        (part_a[pl.ds(8 * i, 8)].reshape(8, BZ), zero) for i in range((last_slot + 1) // 8)
    ]
    high, low = tree(rows)
    total = tree([(high[i : i + 1], low[i : i + 1]) for i in range(8)])

    mu = []
    for j in range(6):
        mu.append(norm(*(jnp.broadcast_to(v[:, j : j + 1], (8, BZ)) for v in total)))
    for j, c in enumerate(coefficients(mu)):
        coef[j] = c

    for s in range(2):
        @pl.when(gy != ny // 2 - 1 + s)
        def _(s=s):
            land = fault.at[s]
            remote(land, land, fs_sem.at[0], fr_sem.at[s], partner).wait_recv()
    for k in range(3):
        for i in range(own_rows // 8):
            at = pl.ds(8 * i, 8)
            fault_sum[k, at, :] = fault[0, k, at, :] + fault[1, k, at, :]

    remote(land, land, rs_sem.at[0], rr_sem.at[0], partner).wait_send()
    remote(zpack, hz, zs_sem.at[0], zr_sem.at[0], partner).wait_send()
    for k in range(3):
        for side in range(2):
            @pl.when(has_x[side])
            def _(k=k, side=side):
                sent = hx.at[k, side] if k < 2 else hx.at[k, side, 0]
                remote(sent, sent, xs_sem.at[k, side], xr_sem.at[k, side, 0], partner).wait_send()
            @pl.when(has_y[side])
            def _(k=k, side=side):
                y_copy(k, side).wait_send()

    @pl.when(near_fault)
    def _():
        sent = trac.at[:, pl.ds(0, (ny - 1) * own_rows), :]
        remote(sent, sent, fs_sem.at[0], fr_sem.at[0], partner).wait_send()


def combine(w0, w1, w2, coef, fault_sum, prestress, state, normal, u, slip, buf, sem):
    c0, c1, c2 = coef[0], coef[1], coef[2]
    step = BX // CHUNKS
    copies = []
    for i in range(CHUNKS):
        def plane(x, carry):
            for t in range(TILES):
                at = pl.ds(spot_of(x, 8 * t), 8)
                buf[x, pl.ds(8 * t, 8), :] = (c0 * w0[at, :] + c1 * w1[at, :]) + c2 * w2[at, :]
            return carry

        lax.fori_loop(i * step, (i + 1) * step, plane, 0)
        part = pl.ds(i * step, step)
        copy = pltpu.make_async_copy(buf.at[part], u.at[part], sem.at[i])
        copy.start()
        copies.append(copy)
    for i in range(slip.shape[0] // 8):
        at = pl.ds(8 * i, 8)
        traction = (c0 * fault_sum[0, at, :] + c1 * fault_sum[1, at, :]) + c2 * fault_sum[2, at, :]
        x = (prestress[at, :] + 2.0 * traction) / normal[at, :]
        half = 0.6931471805599453
        large = jnp.exp(x - half) - jnp.exp(-x - half)
        q = x * x
        small = x * (1.0 + q * (1 / 6 + q * (1 / 120 + q * (1 / 5040 + q * (1 / 362880 + q / 39916800)))))
        sinh = jnp.where(jnp.abs(x) < 1.0, small, large)
        slip[at, :] = jnp.exp(-state[at, :]) * sinh
    for copy in copies:
        copy.wait()


def per_device(load, stiffness, prestress, state_var, normal_a):
    vmem = pl.BlockSpec(memory_space=pltpu.VMEM)
    hbm = pl.BlockSpec(memory_space=pl.ANY)
    ny = lax.axis_size("gy")
    own = BX // ny
    group = ny * lax.axis_size("gz")
    nx = lax.axis_size("gx")
    big = (ROWS, BZ)
    packs = (BX // SLOTS) * TILES
    DMA = pltpu.SemaphoreType.DMA
    outs = pl.pallas_call(
        krylov,
        out_shape=[
            pltpu.VMEM(big, F32), pltpu.VMEM(big, F32), pltpu.VMEM(big, F32),
            pltpu.VMEM((3, 8, BZ), F32), pltpu.VMEM((3, own, BZ), F32),
        ],
        in_specs=[pl.BlockSpec(memory_space=pltpu.HBM)] * 2,
        out_specs=[vmem] * 5,
        scratch_shapes=[
            pltpu.VMEM((2, BX, BY, BZ), F32),
            pltpu.VMEM((BX * BY, BZ), F32),
            pltpu.VMEM((3, 2, 2, BX, BZ), F32),
            pltpu.VMEM((3, packs, 8, BZ), F32),
            pltpu.VMEM((packs, 8, BZ), F32),
            pltpu.VMEM((3, BX, BZ), F32),
            pltpu.VMEM((3, 2, 2, 2, BY // 2, BZ), F32),
            pltpu.VMEM((3, 2, 2, BX, BZ), F32),
            pltpu.VMEM((3, packs, 8, BZ), F32),
            pltpu.VMEM((2, 3, own, BZ), F32),
            pltpu.VMEM((group * nx, 1, BZ), F32),
            pltpu.VMEM((8, BZ), F32),
            pltpu.VMEM((3 * BZ, BZ), BF16),
            pltpu.VMEM((GROUP * PITCH, BZ), F32),
            pltpu.VMEM((GROUP * PITCH, BZ), F32),
            DMA((4 + INNER,)),
            DMA((3, 2)), DMA((3, 2, 2)), DMA((3, 2)), DMA((3, 2)), DMA((1,)), DMA((3,)),
            DMA((1,)), DMA((2,)),
            DMA((1,)), DMA((1,)),
            pltpu.SemaphoreType.REGULAR((2,)),
        ],
        compiler_params=pltpu.CompilerParams(
            collective_id=0, has_side_effects=True, vmem_limit_bytes=55 * 2**20
        ),
        name="krylov",
    )(load, stiffness)
    return pl.pallas_call(
        combine,
        out_shape=[
            jax.ShapeDtypeStruct(load.shape, F32),
            jax.ShapeDtypeStruct(prestress.shape, F32),
        ],
        in_specs=[vmem] * 8,
        out_specs=[hbm, vmem],
        scratch_shapes=[pltpu.VMEM((BX, BY, BZ), F32), DMA((CHUNKS,))],
        compiler_params=pltpu.CompilerParams(vmem_limit_bytes=24 * 2**20),
        name="combine",
    )(*outs, prestress, state_var, normal_a)


def solution(mesh):
    block = P("gx", "gy", "gz")
    fault = P(("gx", "gy"), "gz")
    return jax.shard_map(
        per_device,
        mesh=mesh,
        in_specs=(block, block, fault, fault, fault),
        out_specs=(block, fault),
        check_vma=False,
    )
```
